32 devices in a mesh: tok: 16 (over z, y, x), head: 2 (over core).
Axes of the slice: x: 2, y: 2, z: 4, core: 2. Of those that a mesh axis runs over, the one named last changes fastest.
Arguments:
- query_rows: bfloat16 [6144, 2048], P('tok', 'head'), may hold values from -6 to 6
- key_rows: bfloat16 [6144, 1024], P('tok', 'head'), may hold values from -6 to 6
- value_rows: bfloat16 [6144, 1024], P('tok', 'head'), may hold values from -6 to 6
- out_grad: bfloat16 [6144, 2048], P('tok', 'head'), may hold values from -96 to 96
- log_norm: float32 [6144, 16], P('tok', 'head'), may hold values from 6.5 to 8
- delta_rows: float32 [6144, 16], P('tok', 'head'), may hold values from -48 to 48
- window_len: int32 [16], P('head'), may hold values from 896 to 1024, as said below
- activations: bfloat16 [6144, 5376], P('tok'), may hold values from -6 to 6
- value_weight: bfloat16 [5376, 1024], P('tok', 'head')
- row_state: float32 [2, 5376], P('head', 'tok'), as said below
- col_state: float32 [16, 1024], P('tok', 'head'), as said below
Outputs:
- query_grad: bfloat16 [6144, 2048], P('tok', 'head')
- key_grad: bfloat16 [6144, 1024], P('tok', 'head')
- value_grad: bfloat16 [6144, 1024], P('tok', 'head')
- new_weight: bfloat16 [5376, 1024], P('tok', 'head')
- update_dir: float32 [5376, 1024], P('tok', 'head')
The draws below stay inside these ranges and needn't reach their ends.
Inputs may be any that keep to these rules, and one draw needn't show every extreme that they name: `window_len`: every head's window is one of the integers from 896 to 1024, and some head has exactly 1024. `row_state`: positive. `col_state`: positive.
All inputs are finite; a program needn't handle non-finite values.
Results may differ from the reference program's by a relative error of at most 0.005.
Values may be sent and summed in bfloat16 or wider, within the bound.
A program may use at most 128 MiB of HBM per device.

```python
import jax
import jax.numpy as jnp
from jax import lax

D = 5376
HD = 128
Q_HEADS = 16
KV_HEADS = 8
WINDOW = 1024
TOK_DEV = 384
GROUP = 2
QD = 2048
KVD = 1024
SPAN = 1408
TOKENS = 6144
N_TOK = 16
N_HEAD = 2


def draw_window_len(key, part):
    shorter = jax.random.randint(key, (Q_HEADS,), 0, WINDOW // 8 + 1)
    picked = jax.random.randint(jax.random.fold_in(key, 7), (), 0, Q_HEADS)
    shorter = jnp.where(jnp.arange(Q_HEADS) == picked, 0, shorter)
    return (WINDOW - shorter).astype(jnp.int32)


def draw_row_state(key, part):
    spread = jax.random.uniform(key, (N_HEAD, D), jnp.float32, 0.0, 1.0)
    return TOKENS * 0.2 * 10.0 ** spread


def draw_col_state(key, part):
    shard = jnp.arange(N_TOK, dtype=jnp.float32)[:, None] / max(N_TOK - 1, 1)
    jitter = jax.random.uniform(key, (N_TOK, KVD), jnp.float32, -0.3, 0.3)
    power = 1.5 - 3.0 * shard + jitter
    return TOKENS * 0.64 * 10.0 ** power


def draw_value_weight(key, part):
    key_base = jax.random.fold_in(key, 11)
    key_rows = jax.random.fold_in(key, 12)
    key_cols = jax.random.fold_in(key, 13)
    base = jnp.clip(jax.random.normal(key_base, (D, KVD), jnp.float32), -4.0, 4.0)
    row_pos = jnp.arange(D, dtype=jnp.float32) / D
    row_jitter = jax.random.uniform(key_rows, (D,), jnp.float32, 0.7, 1.4)
    col_scale = 10.0 ** jax.random.uniform(key_cols, (KVD,), jnp.float32, 0.0, 1.0)
    row_scale = 10.0 ** row_pos * row_jitter
    return (base * row_scale[:, None] * col_scale[None, :] / jnp.sqrt(jnp.float32(D))).astype(jnp.bfloat16)


def raised(drawn, stream_key, source, target, blocks, factor):
    owner, partner = [(jnp.arange(drawn.shape[position]) // (drawn.shape[position] // blocks)).reshape([-1 if axis == position else 1 for axis in range(drawn.ndim)]) for position in (source, target)]
    chosen = jax.random.permutation(stream_key, blocks)[partner]
    strong = (owner == chosen) | (owner == (partner + blocks // 2) % blocks)
    return jnp.where(strong, factor * drawn, drawn)


def block_scale(stream_key, extent, shards, least, largest):
    factor_of, own = 1.0, jax.random.fold_in(stream_key, 6)
    for dim, parts in shards:
        draws = jnp.exp(jax.random.uniform(jax.random.fold_in(own, dim), (parts,), jnp.float32, least / len(shards), largest / len(shards)))
        factor_of = factor_of * jnp.repeat(draws, extent[dim] // parts).reshape([-1 if axis == dim else 1 for axis in range(len(extent))])
    return factor_of


def centred(stream_key, extent, scale, most, pieces=(), kind=jnp.bfloat16):
    entries = scale * jax.random.normal(stream_key, extent, jnp.float32)
    if pieces:
        entries = entries * block_scale(stream_key, extent, pieces, -0.22, 0.18)
    return jnp.clip(entries, -most, most).astype(kind)


def bell_draw_with(key, shape, scale, most, pieces, heavy, held_as=jnp.bfloat16):
    entries = scale * jax.random.normal(key, shape, jnp.float32)
    if pieces:
        entries = entries * block_scale(key, shape, pieces, -0.22, 0.18)
    return jnp.clip(raised(entries, jax.random.fold_in(key, 3), *heavy), -most, most).astype(held_as)


def setup_inputs(seed: int = 0) -> dict:
    seeds = jax.random.split(jax.random.key(seed), 12)
    return {
        "query_rows": centred(seeds[0], (TOKENS, QD), 1.0, 6.0, ((0, 16), (1, 2))),
        "key_rows": centred(seeds[1], (TOKENS, KVD), 1.0, 6.0, ((0, 16), (1, 2))),
        "value_rows": centred(seeds[2], (TOKENS, KVD), 1.0, 6.0, ((0, 16), (1, 2))),
        "out_grad": centred(seeds[3], (TOKENS, QD), 16.0, 96.0, ((0, 16), (1, 2))),
        "log_norm": jnp.clip(6.5 + 1.5 * jax.random.uniform(seeds[4], (TOKENS, Q_HEADS), jnp.float32) ** block_scale(seeds[4], (TOKENS, Q_HEADS), ((0, 16), (1, 2)), -0.2, 0.2), 6.5, 8.0),
        "delta_rows": centred(seeds[5], (TOKENS, Q_HEADS), 8.0, 48.0, ((0, 16), (1, 2)), jnp.float32),
        "window_len": draw_window_len(jax.random.fold_in(seeds[11], 71), 0),
        "activations": bell_draw_with(seeds[7], (TOKENS, D), 1.0, 6.0, ((0, 16),), (0, 1, 16, 2.0)),
        "value_weight": draw_value_weight(jax.random.fold_in(seeds[11], 71), 0),
        "row_state": draw_row_state(jax.random.fold_in(seeds[11], 71), 0),
        "col_state": draw_col_state(jax.random.fold_in(seeds[11], 71), 0),
    }


QUERY_SCALE = 1.0 / 12.0
DECAY_RATE = 0.9
LEARN_RATE = 0.05

def attend_block(query_blk, key_blk, value_blk, grad_blk, norm_blk, delta_blk, window_len, first_query, first_key):
    query_f = query_blk.astype(jnp.float32)
    key_f = key_blk.astype(jnp.float32)
    value_f = value_blk.astype(jnp.float32)
    grad_f = grad_blk.astype(jnp.float32)
    scores = jnp.einsum('tkgd,skd->kgts', query_f, key_f) * QUERY_SCALE
    query_pos = first_query + jnp.arange(TOK_DEV, dtype=jnp.int32)
    key_pos = first_key + jnp.arange(SPAN, dtype=jnp.int32)
    distance = query_pos[:, None] - key_pos[None, :]
    limits = window_len.reshape(KV_HEADS, GROUP)[:, :, None, None]
    visible = (distance[None, None] >= 0) & (distance[None, None] < limits) & (key_pos >= 0)[None, None, None, :]
    norm_t = jnp.transpose(norm_blk.reshape(TOK_DEV, KV_HEADS, GROUP), (1, 2, 0))
    delta_t = jnp.transpose(delta_blk.reshape(TOK_DEV, KV_HEADS, GROUP), (1, 2, 0))
    prob_full = jnp.where(visible, jnp.exp(scores - norm_t[..., None]), 0.0)
    prob_low = lax.optimization_barrier(prob_full.astype(jnp.bfloat16)).astype(jnp.float32)
    value_part = jnp.einsum('kgts,tkgd->skd', prob_low, grad_f)
    prob_grad = jnp.einsum('tkgd,skd->kgts', grad_f, value_f)
    score_grad = QUERY_SCALE * prob_full * (prob_grad - delta_t[..., None])
    score_grad = lax.optimization_barrier(score_grad.astype(jnp.bfloat16)).astype(jnp.float32)
    query_part = jnp.einsum('kgts,skd->tkgd', score_grad, key_f)
    key_part = jnp.einsum('kgts,tkgd->skd', score_grad, query_f)
    return (query_part, key_part, value_part)

def reference(query_rows, key_rows, value_rows, out_grad, log_norm, delta_rows, window_len, activations, value_weight, row_state, col_state):
    pad_rows = WINDOW
    query4 = query_rows.reshape(TOKENS, KV_HEADS, GROUP, HD)
    grad4 = out_grad.reshape(TOKENS, KV_HEADS, GROUP, HD)
    key_pad = jnp.concatenate([jnp.zeros((pad_rows, KVD), jnp.bfloat16), key_rows], axis=0).reshape(pad_rows + TOKENS, KV_HEADS, HD)
    value_pad = jnp.concatenate([jnp.zeros((pad_rows, KVD), jnp.bfloat16), value_rows], axis=0).reshape(pad_rows + TOKENS, KV_HEADS, HD)
    zeros_acc = jnp.zeros((pad_rows + TOKENS, KV_HEADS, HD), jnp.float32)

    def step_block(carry, index):
        key_acc, value_acc = carry
        start = (index * TOK_DEV).astype(jnp.int32)
        query_blk = lax.dynamic_slice_in_dim(query4, start, TOK_DEV, 0)
        grad_blk = lax.dynamic_slice_in_dim(grad4, start, TOK_DEV, 0)
        norm_blk = lax.dynamic_slice_in_dim(log_norm, start, TOK_DEV, 0)
        delta_blk = lax.dynamic_slice_in_dim(delta_rows, start, TOK_DEV, 0)
        key_blk = lax.dynamic_slice_in_dim(key_pad, start, SPAN, 0)
        value_blk = lax.dynamic_slice_in_dim(value_pad, start, SPAN, 0)
        query_part, key_part, value_part = attend_block(query_blk, key_blk, value_blk, grad_blk, norm_blk, delta_blk, window_len, start, start - pad_rows)
        key_acc = lax.dynamic_update_slice_in_dim(key_acc, lax.dynamic_slice_in_dim(key_acc, start, SPAN, 0) + key_part, start, 0)
        value_acc = lax.dynamic_update_slice_in_dim(value_acc, lax.dynamic_slice_in_dim(value_acc, start, SPAN, 0) + value_part, start, 0)
        return ((key_acc, value_acc), query_part)
    (key_acc, value_acc), query_parts = lax.scan(step_block, (zeros_acc, zeros_acc), jnp.arange(N_TOK, dtype=jnp.int32))
    query_grad = query_parts.reshape(TOKENS, QD).astype(jnp.bfloat16)
    key_grad = key_acc[pad_rows:].reshape(TOKENS, KVD).astype(jnp.bfloat16)
    value_grad = value_acc[pad_rows:].reshape(TOKENS, KVD).astype(jnp.bfloat16)
    weight_grad = lax.dot_general(activations, value_grad, (((0,), (0,)), ((), ())), preferred_element_type=jnp.float32)
    row_blk = D // N_TOK
    col_blk = KVD // N_HEAD
    blocks = weight_grad.reshape(N_TOK, row_blk, N_HEAD, col_blk)
    squares = blocks * blocks
    row_new = lax.optimization_barrier(jnp.mean(squares, axis=3))
    col_new = lax.optimization_barrier(jnp.mean(squares, axis=1))
    row_old = jnp.transpose(row_state.reshape(N_HEAD, N_TOK, row_blk), (1, 2, 0))
    col_old = col_state.reshape(N_TOK, N_HEAD, col_blk)
    row_mix = DECAY_RATE * row_old + (1.0 - DECAY_RATE) * row_new
    col_mix = DECAY_RATE * col_old + (1.0 - DECAY_RATE) * col_new
    row_mean = lax.optimization_barrier(jnp.mean(row_mix, axis=1))
    second = row_mix[:, :, :, None] * col_mix[:, None, :, :] / row_mean[:, None, :, None]
    scaled = blocks / jnp.sqrt(second)
    weight_f = value_weight.astype(jnp.float32)
    rms_scaled = jnp.sqrt(jnp.sum(scaled * scaled) / (D * KVD))
    rms_weight = jnp.sqrt(jnp.sum(weight_f * weight_f) / (D * KVD))
    update_dir = (rms_weight * scaled / jnp.maximum(1.0, rms_scaled)).reshape(D, KVD)
    new_weight = (weight_f - LEARN_RATE * update_dir).astype(jnp.bfloat16)
    return (query_grad, key_grad, value_grad, new_weight, update_dir)
```

```python
import functools
import math

import jax
import jax.numpy as jnp
from jax import lax
from jax.experimental import pallas as pl
from jax.experimental.pallas import tpu as pltpu
from jax.sharding import PartitionSpec as P

HD = 128
WINDOW = 1024
WINDOW_MIN = 896
SUB = 128
QUERY_SCALE = 1.0 / 12.0
LOG2E = math.log2(math.e)
DECAY_RATE = 0.9
LEARN_RATE = 0.05
F32 = jnp.float32
BF16 = jnp.bfloat16
MESH = pl.DeviceIdType.MESH


def xor(index, j):
    k = 0
    while (1 << k) <= j:
        if (j >> k) & 1:
            index = index + (1 << k) * (1 - 2 * lax.rem(index // (1 << k), 2))
        k += 1
    return index


class Plan:
    def __init__(self, n, n_head, tok_len, kv_local, group, width, rows):
        self.n, self.n_head, self.tok_len = n, n_head, tok_len
        self.kv_local, self.group = kv_local, group
        self.width, self.rows = width, rows
        self.gather = 4 if n % 4 == 0 else 1
        self.upper = n // self.gather
        self.split = self.gather if kv_local % self.gather == 0 else 1
        self.kv = kv_local // self.split
        self.tokens = self.split * tok_len
        self.blocks = n // self.split
        self.reach = min(-(-WINDOW // self.tokens), self.blocks - 1)
        self.subs = tok_len // SUB
        self.streams = self.split
        self.part = width // self.streams
        self.bits = int(math.log2(self.upper))
        self.share = 2 if n_head % 2 == 0 and self.upper % 2 == 0 else 1

    def halo_count(self, o):
        return min(self.tokens, WINDOW - (o - 1) * self.tokens)

    def halo_first(self, o):
        return max(0, WINDOW - o * self.tokens)


def fused_kernel(
    pn,
    lim_ref, q_ref, g_ref, k_ref, v_ref, st_ref, at_ref, w_ref, rs_ref, cs_ref,
    dq_ref, dk_ref, dv_ref, sc_ref, fac_ref,
    qb, gb, kb, vb, stb, dva, dka, dqb, dkb, hsv, hsk, hrv, hrk, act, vga, acc, sbuf, rbuf,
    xs, xr,
    own_sem, in_s, in_r, halo_s, halo_r, back_s, back_r, act_own, act_s, act_r, fwd_s, fwd_r,
    vg_s, vg_r, dq_s, dq_r, dk_s, dk_r, out_sem, rs_s, rs_r, x_s, x_r,
):
    n, n_head, gather, upper = pn.n, pn.n_head, pn.gather, pn.upper
    split, kv, length, tokens = pn.split, pn.kv, pn.tok_len, pn.tokens
    group, subs = pn.group, pn.subs
    me, hd = lax.axis_index("tok"), lax.axis_index("head")
    c, u = lax.rem(me, gather), me // gather
    place, block = lax.rem(me, split), me // split
    kw, qw = kv * HD, kv * group * HD

    def at_plane(j):
        return {"tok": me - c + xor(c, j)}

    near = [(j, h) for j in range(gather) for h in range(n_head) if j or h]
    far = list(range(1, upper))
    near_ids = [{"tok": me - c + xor(c, j), "head": xor(hd, h)} for j, h in near]
    far_ids = [{"tok": xor(u, i) * gather + c} for i in far]
    barrier = pltpu.get_barrier_semaphore()
    for partner in near_ids + far_ids:
        pl.semaphore_signal(barrier, inc=1, device_id=partner, device_id_type=MESH)
    lone = []
    if split == 1:
        for o in range(1, pn.reach + 1):
            lone.append(o)
            @pl.when(block + o < pn.blocks)
            def _(o=o):
                pl.semaphore_signal(barrier, inc=1, device_id={"tok": me + o}, device_id_type=MESH)

            @pl.when(block >= o)
            def _(o=o):
                pl.semaphore_signal(barrier, inc=1, device_id={"tok": me - o}, device_id_type=MESH)

    def cols(index, size):
        return pl.ds(pl.multiple_of(index * size, 128), size)

    own = [
        pltpu.make_async_copy(k_ref.at[:, cols(place, kw)], kb.at[pl.ds(WINDOW + place * length, length)], own_sem.at[0]),
        pltpu.make_async_copy(v_ref.at[:, cols(place, kw)], vb.at[pl.ds(WINDOW + place * length, length)], own_sem.at[1]),
        pltpu.make_async_copy(q_ref.at[:, cols(place, qw)], qb.at[pl.ds(place * length, length)], own_sem.at[2]),
        pltpu.make_async_copy(g_ref.at[:, cols(place, qw)], gb.at[pl.ds(place * length, length)], own_sem.at[3]),
        pltpu.make_async_copy(st_ref.at[pl.ds(place * kv, kv)], stb.at[place], own_sem.at[4]),
    ]
    for copy in own:
        copy.start()
    half = upper // pn.share
    low = lax.rem(hd, pn.share) * half

    act_mine = [
        pltpu.make_async_copy(
            at_ref.at[i * gather + c], act.at[i, :, cols(c, length)], act_own.at[i]
        )
        for i in range(upper)
    ]
    for copy in act_mine:
        copy.start()
    dva[...] = jnp.zeros_like(dva)
    dka[...] = jnp.zeros_like(dka)

    pl.semaphore_wait(barrier, len(near_ids) + len(far_ids))
    for o in lone:
        @pl.when(block + o < pn.blocks)
        def _():
            pl.semaphore_wait(barrier, 1)

        @pl.when(block >= o)
        def _():
            pl.semaphore_wait(barrier, 1)

    def exchange(a, j):
        other = xor(place, j)
        src, dst = [
            (k_ref.at[:, cols(other, kw)], kb.at[pl.ds(WINDOW + place * length, length)]),
            (v_ref.at[:, cols(other, kw)], vb.at[pl.ds(WINDOW + place * length, length)]),
            (q_ref.at[:, cols(other, qw)], qb.at[pl.ds(place * length, length)]),
            (g_ref.at[:, cols(other, qw)], gb.at[pl.ds(place * length, length)]),
            (st_ref.at[pl.ds(other * kv, kv)], stb.at[place]),
        ][a]
        return pltpu.make_async_remote_copy(
            src_ref=src, dst_ref=dst, send_sem=in_s.at[a, j], recv_sem=in_r.at[a, j],
            device_id=at_plane(j), device_id_type=MESH,
        )

    for a in (0, 1, 4, 2, 3):
        for j in range(1, split):
            exchange(a, j).start()

    def halo(a, o):
        count, first = pn.halo_count(o), pn.halo_first(o)
        buf = (kb, vb)[a]
        return pltpu.make_async_remote_copy(
            src_ref=buf.at[pl.ds(WINDOW + tokens - count, count)],
            dst_ref=buf.at[pl.ds(first, count)],
            send_sem=halo_s.at[a, o - 1], recv_sem=halo_r.at[a, o - 1],
            device_id={"tok": me + o * split}, device_id_type=MESH,
        )

    for a in (0, 1):
        own[a].wait()
        for j in range(1, split):
            exchange(a, j).wait_recv()
        for o in range(1, pn.reach + 1):
            @pl.when(block + o < pn.blocks)
            def _(a=a, o=o):
                halo(a, o).start()

            @pl.when(block < o)
            def _(a=a, o=o):
                buf = (kb, vb)[a]
                here = pl.ds(pn.halo_first(o), pn.halo_count(o))
                buf[here] = jnp.zeros((pn.halo_count(o), kw), BF16)
    if pn.reach * tokens < WINDOW:
        rest = WINDOW - pn.reach * tokens
        for buf in (kb, vb):
            buf[pl.ds(0, rest)] = jnp.zeros((rest, kw), BF16)

    def act_send(j, i):
        other = xor(c, j)
        return pltpu.make_async_remote_copy(
            src_ref=at_ref.at[(low + i) * gather + other],
            dst_ref=act.at[low + i, :, cols(c, length)],
            send_sem=act_s.at[j, i], recv_sem=act_r.at[j, i],
            device_id=at_plane(j), device_id_type=MESH,
        )

    def act_forward(j):
        piece = act.at[pl.ds(low, half), :, cols(xor(c, j), length)]
        return pltpu.make_async_remote_copy(
            src_ref=piece, dst_ref=piece, send_sem=fwd_s.at[j], recv_sem=fwd_r.at[j],
            device_id={"head": xor(hd, 1)}, device_id_type=MESH,
        )

    for a in (0, 1):
        for o in range(1, pn.reach + 1):
            @pl.when(block >= o)
            def _(a=a, o=o):
                halo(a, o).wait_recv()

    seen = WINDOW + SUB
    chunk = seen // 3
    lanes = group * SUB

    def unit(b, kh, sub):
        start = pl.multiple_of(b * length + sub * SUB, SUB)
        rows_q = pl.ds(start, SUB)
        head = kh * group * HD
        query = jnp.concatenate(
            [qb[rows_q, head + m * HD : head + (m + 1) * HD] for m in range(group)], axis=0
        )
        grad = jnp.concatenate(
            [gb[rows_q, head + m * HD : head + (m + 1) * HD] for m in range(group)], axis=0
        )
        norm = stb[b, kh, pl.ds(sub, 1), :]
        delta = stb[b, kh, pl.ds(subs + sub, 1), :]
        total = jnp.zeros((lanes, HD), F32)
        for piece in range(3):
            here = pl.ds(pl.multiple_of(start + piece * chunk, SUB), chunk)
            keys = kb[here, kh * HD : (kh + 1) * HD]
            values = vb[here, kh * HD : (kh + 1) * HD]
            scores = lax.dot_general(
                keys, query, (((1,), (1,)), ((), ())), preferred_element_type=F32
            )
            prob = jnp.exp2(scores * (QUERY_SCALE * LOG2E) - norm)
            if piece == 0:
                edge = WINDOW - WINDOW_MIN + SUB
                row = lax.broadcasted_iota(jnp.int32, (edge, lanes), 0)
                lane = lax.broadcasted_iota(jnp.int32, (edge, lanes), 1)
                limit = jnp.full((edge, lanes), 0, jnp.int32)
                for m in range(group):
                    limit = jnp.where(
                        lane // SUB == m, lim_ref[(place * kv + kh) * group + m], limit
                    )
                visible = WINDOW + lax.rem(lane, SUB) - row < limit
                prob = jnp.concatenate(
                    [jnp.where(visible, prob[:edge], 0.0), prob[edge:]], axis=0
                )
            if piece == 2:
                row = lax.broadcasted_iota(jnp.int32, (SUB, lanes), 0)
                lane = lax.broadcasted_iota(jnp.int32, (SUB, lanes), 1)
                visible = row <= lax.rem(lane, SUB)
                prob = jnp.concatenate(
                    [prob[: chunk - SUB], jnp.where(visible, prob[chunk - SUB :], 0.0)], axis=0
                )
            dva[here, kh * HD : (kh + 1) * HD] += jnp.dot(
                prob.astype(BF16), grad, preferred_element_type=F32
            )
            dprob = lax.dot_general(
                values, grad, (((1,), (1,)), ((), ())), preferred_element_type=F32
            )
            dscore = (QUERY_SCALE * prob * (dprob - delta)).astype(BF16)
            dka[here, kh * HD : (kh + 1) * HD] += jnp.dot(
                dscore, query, preferred_element_type=F32
            )
            total = total + lax.dot_general(
                dscore, keys, (((0,), (0,)), ((), ())), preferred_element_type=F32
            )
        low_q = total.astype(BF16)
        for m in range(group):
            dqb[rows_q, head + m * HD : head + (m + 1) * HD] = low_q[m * SUB : (m + 1) * SUB]

    def dq_send(j):
        other = xor(place, j)
        src = dqb.at[pl.ds(other * length, length)]
        return pltpu.make_async_remote_copy(
            src_ref=src, dst_ref=dq_ref.at[:, cols(place, qw)],
            send_sem=dq_s.at[j], recv_sem=dq_r.at[j],
            device_id=at_plane(j), device_id_type=MESH,
        )

    def local_out(src, dst, i):
        return pltpu.make_async_copy(src, dst, out_sem.at[i])

    for j in range(split):
        b = xor(place, j)
        for a in (2, 3, 4):
            if j:
                exchange(a, j).wait_recv()
            else:
                own[a].wait()
        for kh in range(kv):
            @pl.loop(0, subs)
            def _(sub, b=b, kh=kh):
                unit(b, kh, sub)

        if j == 0:
            for jj in range(1, gather):
                for i in range(half):
                    act_send(jj, i).start()

    def back(a, o):
        count, first = pn.halo_count(o), pn.halo_first(o)
        return pltpu.make_async_remote_copy(
            src_ref=(hsv, hsk)[a].at[pl.ds(first, count)],
            dst_ref=(hrv, hrk)[a].at[o - 1, pl.ds(0, count)],
            send_sem=back_s.at[a, o - 1], recv_sem=back_r.at[a, o - 1],
            device_id={"tok": me - o * split}, device_id_type=MESH,
        )

    for a in (0, 1):
        (hsv, hsk)[a][...] = (dva, dka)[a][pl.ds(0, WINDOW)].astype(BF16)
        for o in range(1, pn.reach + 1):
            @pl.when(block >= o)
            def _(a=a, o=o):
                back(a, o).start()

    def add_back(a):
        for o in range(1, pn.reach + 1):
            @pl.when(block + o < pn.blocks)
            def _(o=o):
                count = pn.halo_count(o)
                back(a, o).wait_recv()
                here = pl.ds(WINDOW + tokens - count, count)
                total = (dva, dka)[a]
                total[here] = total[here] + (hrv, hrk)[a][o - 1, pl.ds(0, count)].astype(F32)

    def vg_send(j):
        return pltpu.make_async_remote_copy(
            src_ref=vga.at[c], dst_ref=vga.at[c], send_sem=vg_s.at[j], recv_sem=vg_r.at[j],
            device_id=at_plane(j), device_id_type=MESH,
        )

    add_back(0)
    vga[c] = dva[pl.ds(WINDOW, tokens)].astype(BF16)
    for j in range(1, gather):
        vg_send(j).start()

    local = 0
    outs = []
    outs.append(local_out(dqb.at[pl.ds(place * length, length)], dq_ref.at[:, cols(place, qw)], 0))
    outs[-1].start()
    for j in range(1, split):
        dq_send(j).start()

    add_back(1)
    dkb[...] = dka[pl.ds(WINDOW, tokens)].astype(BF16)

    def dk_send(j):
        other = xor(place, j)
        return pltpu.make_async_remote_copy(
            src_ref=dkb.at[pl.ds(other * length, length)], dst_ref=dk_ref.at[:, cols(place, kw)],
            send_sem=dk_s.at[j], recv_sem=dk_r.at[j],
            device_id=at_plane(j), device_id_type=MESH,
        )

    outs.append(local_out(dkb.at[pl.ds(place * length, length)], dk_ref.at[:, cols(place, kw)], 1))
    outs[-1].start()
    for j in range(1, split):
        dk_send(j).start()

    for copy in act_mine:
        copy.wait()
    for j in range(1, gather):
        for i in range(half):
            act_send(j, i).wait_recv()
        if pn.share == 2:
            act_forward(j).start()
    if pn.share == 2:
        for j in range(1, gather):
            piece_in = act.at[pl.ds(half - low, half), :, cols(xor(c, j), length)]
            pltpu.make_async_remote_copy(
                src_ref=piece_in, dst_ref=piece_in, send_sem=fwd_s.at[j], recv_sem=fwd_r.at[j],
                device_id={"head": xor(hd, 1)}, device_id_type=MESH,
            ).wait_recv()

    bits, part, rows = pn.bits, pn.part, pn.rows
    counts = [upper >> (p + 1) for p in range(bits)]
    starts = [sum(counts[:p]) for p in range(bits)]
    partners = [{"tok": xor(u, 1 << p) * gather + c} for p in range(bits)]

    def bit_of(index, k):
        return lax.rem(index // (1 << k), 2)

    def block_at(phase, j, other):
        index = 0
        for k in range(phase):
            index = index + (1 << k) * bit_of(u, k)
        mine = bit_of(u, phase)
        index = index + (1 << phase) * ((1 - mine) if other else mine)
        return index + (1 << (phase + 1)) * j

    def copy_of(s, p):
        here = pl.ds(starts[p], counts[p])
        return pltpu.make_async_remote_copy(
            src_ref=sbuf.at[s, here], dst_ref=rbuf.at[s, here],
            send_sem=rs_s.at[s, p], recv_sem=rs_r.at[s, p],
            device_id=partners[p], device_id_type=MESH,
        )

    def product(s, index):
        if split == gather:
            return jnp.dot(act[index], vga[xor(c, s)], preferred_element_type=F32)
        whole = vga[...].reshape(gather * length, part)
        return jnp.dot(act[index], whole, preferred_element_type=F32)

    def wait_vg(j):
        vg_in = vga.at[xor(c, j)]
        pltpu.make_async_remote_copy(
            src_ref=vg_in, dst_ref=vg_in, send_sem=vg_s.at[j], recv_sem=vg_r.at[j],
            device_id=at_plane(j), device_id_type=MESH,
        ).wait_recv()

    if split == 1:
        for j in range(1, gather):
            wait_vg(j)
    for s in range(pn.streams):
        if s:
            wait_vg(s)

        @pl.loop(0, counts[0])
        def _(j, s=s):
            sbuf[s, j] = product(s, block_at(0, j, True)).astype(BF16)

        copy_of(s, 0).start()

        @pl.loop(0, counts[0])
        def _(j, s=s):
            index = block_at(0, j, False)
            acc[s, index] = product(s, index)

    if split == gather:
        for j in range(gather):
            src = xor(c, j)
            outs.append(local_out(
                vga.at[src, pl.ds(c * length, length)], dv_ref.at[:, cols(src, kw)], 2 + j))
            outs[-1].start()
    else:
        outs.append(local_out(vga.at[c], dv_ref, 2))
        outs[-1].start()

    weight_f = w_ref[...].astype(F32)
    weight_sum = jnp.sum(weight_f * weight_f)

    for p in range(bits):
        for s in range(pn.streams):
            copy_of(s, p).wait_recv()

            @pl.loop(0, counts[p])
            def _(j, s=s, p=p):
                index = block_at(p, j, False)
                acc[s, index] = acc[s, index] + rbuf[s, starts[p] + j].astype(F32)

            if p + 1 < bits:
                @pl.loop(0, counts[p + 1])
                def _(j, s=s, p=p):
                    index = block_at(p + 1, j, True)
                    sbuf[s, starts[p + 1] + j] = acc[s, index].astype(BF16)

                copy_of(s, p + 1).start()

    row_sum = jnp.zeros((rows, 1), F32)
    for s in range(pn.streams):
        wg = acc[s, u]
        row_sum = row_sum + jnp.sum(wg * wg, axis=1, keepdims=True)
    row_mix = DECAY_RATE * rs_ref[...] + (1.0 - DECAY_RATE) * (row_sum / pn.width)
    row_mean = jnp.sum(row_mix) / rows
    scaled_sum = jnp.float32(0.0)
    for s in range(pn.streams):
        wg = acc[s, u]
        here = cols(xor(c, s), part) if split == gather else slice(0, part)
        col_new = jnp.sum(wg * wg, axis=0, keepdims=True) / rows
        col_mix = DECAY_RATE * cs_ref[:, here] + (1.0 - DECAY_RATE) * col_new
        scaled = wg / jnp.sqrt(row_mix * col_mix / row_mean)
        sc_ref[:, here] = scaled
        scaled_sum = scaled_sum + jnp.sum(scaled * scaled)

    row = lax.broadcasted_iota(jnp.int32, (8, 128), 0)
    xs[0] = jnp.where(row < 4, scaled_sum, weight_sum)

    def share(level, i, partner):
        slot = i + (len(near) if level else 0)
        return pltpu.make_async_remote_copy(
            src_ref=xs.at[level], dst_ref=xr.at[slot], send_sem=x_s.at[slot],
            recv_sem=x_r.at[slot], device_id=partner, device_id_type=MESH,
        )

    for level, ids in enumerate((near_ids, far_ids)):
        for i, partner in enumerate(ids):
            share(level, i, partner).start()
        total = xs[level]
        for i, partner in enumerate(ids):
            share(level, i, partner).wait_recv()
            total = total + xr[i + (len(near) if level else 0)]
        xs[level + 1] = total
    sums = xs[2]
    size = float(rows * n * pn.width * n_head)
    rms_scaled = jnp.sqrt(sums[0:1] / size)
    rms_weight = jnp.sqrt(sums[4:5] / size)
    fac_ref[...] = jnp.broadcast_to(rms_weight / jnp.maximum(1.0, rms_scaled), fac_ref.shape)

    for a in range(5):
        for j in range(1, split):
            exchange(a, j).wait_send()
    for a in (0, 1):
        for o in range(1, pn.reach + 1):
            @pl.when(block + o < pn.blocks)
            def _(a=a, o=o):
                halo(a, o).wait_send()

            @pl.when(block >= o)
            def _(a=a, o=o):
                back(a, o).wait_send()
    for j in range(1, gather):
        for i in range(half):
            act_send(j, i).wait_send()
        if pn.share == 2:
            act_forward(j).wait_send()
        vg_send(j).wait_send()
    for j in range(1, split):
        dq_send(j).wait()
        dk_send(j).wait()
    for copy in outs:
        copy.wait()
    for p in range(bits):
        for s in range(pn.streams):
            copy_of(s, p).wait_send()
    for level, ids in enumerate((near_ids, far_ids)):
        for i, partner in enumerate(ids):
            share(level, i, partner).wait_send()


def fused(pn, limits, query, grad, keys, values, stats, act_t, weight, row_state, col_state):
    kw, qw = pn.kv * HD, pn.kv * pn.group * HD
    whole = WINDOW + pn.tokens
    smem = pl.BlockSpec(memory_space=pltpu.SMEM)
    vmem = pl.BlockSpec(memory_space=pltpu.VMEM)
    hbm = pl.BlockSpec(memory_space=pl.ANY)
    dma = pltpu.SemaphoreType.DMA
    half = pn.upper // pn.share
    peers = pn.gather * pn.n_head - 1 + pn.upper - 1
    reach, gather, split = pn.reach, pn.gather, pn.split
    piece = (pn.tokens, kw) if split == gather else (pn.tok_len, kw)
    return pl.pallas_call(
        functools.partial(fused_kernel, pn),
        out_shape=[
            jax.ShapeDtypeStruct(query.shape, BF16),
            jax.ShapeDtypeStruct(keys.shape, BF16),
            jax.ShapeDtypeStruct(keys.shape, BF16),
            jax.ShapeDtypeStruct((pn.rows, pn.width), F32),
            jax.ShapeDtypeStruct((8, 128), F32),
        ],
        in_specs=[smem, vmem, vmem, vmem, vmem, vmem, hbm, vmem, vmem, vmem],
        out_specs=[hbm, hbm, hbm, vmem, vmem],
        scratch_shapes=[
            pltpu.VMEM((pn.tokens, qw), BF16),
            pltpu.VMEM((pn.tokens, qw), BF16),
            pltpu.VMEM((whole, kw), BF16),
            pltpu.VMEM((whole, kw), BF16),
            pltpu.VMEM((split, pn.kv, 2 * pn.subs, pn.group * SUB), F32),
            pltpu.VMEM((whole, kw), F32),
            pltpu.VMEM((whole, kw), F32),
            pltpu.VMEM((pn.tokens, qw), BF16),
            pltpu.VMEM((pn.tokens, kw), BF16),
            pltpu.VMEM((WINDOW, kw), BF16),
            pltpu.VMEM((WINDOW, kw), BF16),
            pltpu.VMEM((reach, min(pn.tokens, WINDOW), kw), BF16),
            pltpu.VMEM((reach, min(pn.tokens, WINDOW), kw), BF16),
            pltpu.VMEM((pn.upper, pn.rows, gather * pn.tok_len), BF16),
            pltpu.VMEM((gather,) + piece, BF16),
            pltpu.VMEM((pn.streams, pn.upper, pn.rows, pn.part), F32),
            pltpu.VMEM((pn.streams, pn.upper - 1, pn.rows, pn.part), BF16),
            pltpu.VMEM((pn.streams, pn.upper - 1, pn.rows, pn.part), BF16),
            pltpu.VMEM((3, 8, 128), F32),
            pltpu.VMEM((peers, 8, 128), F32),
            dma((5,)), dma((5, split)), dma((5, split)), dma((2, reach)), dma((2, reach)),
            dma((2, reach)), dma((2, reach)), dma((pn.upper,)),
            dma((gather, half)), dma((gather, half)), dma((gather,)), dma((gather,)),
            dma((gather,)), dma((gather,)), dma((split,)), dma((split,)),
            dma((split,)), dma((split,)), dma((2 + gather,)),
            dma((pn.streams, pn.bits)), dma((pn.streams, pn.bits)), dma((peers,)), dma((peers,)),
        ],
        compiler_params=pltpu.CompilerParams(
            collective_id=0, has_side_effects=True, vmem_limit_bytes=56 * 1024 * 1024
        ),
        name="fused",
    )(limits, query, grad, keys, values, stats, act_t, weight, row_state, col_state)


def shards(
    query_rows, key_rows, value_rows, out_grad, log_norm, delta_rows, window_len,
    activations, value_weight, row_state, col_state, *, n, n_head,
):
    tok_len = query_rows.shape[0]
    kv_local = key_rows.shape[1] // HD
    group = query_rows.shape[1] // key_rows.shape[1]
    rows, width = value_weight.shape
    pn = Plan(n, n_head, tok_len, kv_local, group, width, rows)

    def arranged(x):
        x = x.reshape(pn.subs, SUB, kv_local, group)
        return jnp.transpose(x, (2, 0, 3, 1)).reshape(kv_local, pn.subs, group * SUB)

    stats = jnp.concatenate([arranged(log_norm * LOG2E), arranged(delta_rows)], axis=1)
    act_t = activations.T.reshape(n, rows, tok_len)
    query_grad, key_grad, value_grad, scaled, factor = fused(
        pn, window_len, query_rows, out_grad, key_rows, value_rows, stats, act_t,
        value_weight, row_state.reshape(-1, 1), col_state,
    )
    update_dir = scaled * factor[0, 0]
    new_weight = (value_weight.astype(F32) - LEARN_RATE * update_dir).astype(BF16)
    return (query_grad, key_grad, value_grad, new_weight, update_dir)


def solution(mesh):
    both = P("tok", "head")
    return jax.shard_map(
        functools.partial(shards, n=mesh.shape["tok"], n_head=mesh.shape["head"]),
        mesh=mesh,
        in_specs=(
            both, both, both, both, both, both, P("head"), P("tok", None),
            both, P("head", "tok"), both,
        ),
        out_specs=(both,) * 5,
        check_vma=False,
    )
```

```python
import functools
import math

import jax
import jax.numpy as jnp
from jax import lax
from jax.experimental import pallas as pl
from jax.experimental.pallas import tpu as pltpu
from jax.sharding import PartitionSpec as P

HD = 128
WINDOW = 1024
WINDOW_MIN = 896
SUB = 128
QUERY_SCALE = 1.0 / 12.0
LOG2E = math.log2(math.e)
DECAY_RATE = 0.9
LEARN_RATE = 0.05
F32 = jnp.float32
BF16 = jnp.bfloat16
MESH = pl.DeviceIdType.MESH


def xor(index, j):
    k = 0
    while (1 << k) <= j:
        if (j >> k) & 1:
            index = index + (1 << k) * (1 - 2 * lax.rem(index // (1 << k), 2))
        k += 1
    return index


class Plan:
    def __init__(self, n, n_head, tok_len, kv_local, group, width, rows):
        self.n, self.n_head, self.tok_len = n, n_head, tok_len
        self.kv_local, self.group = kv_local, group
        self.width, self.rows = width, rows
        self.gather = 4 if n % 4 == 0 else 1
        self.upper = n // self.gather
        self.split = self.gather if kv_local % self.gather == 0 else 1
        self.kv = kv_local // self.split
        self.tokens = self.split * tok_len
        self.blocks = n // self.split
        self.reach = min(-(-WINDOW // self.tokens), self.blocks - 1)
        self.subs = tok_len // SUB
        self.streams = self.split
        self.part = width // self.streams
        self.bits = int(math.log2(self.upper))
        self.share = 2 if n_head % 2 == 0 and self.upper % 2 == 0 else 1
        self.half = self.upper // self.share
        self.wide = self.half * self.gather * rows
        self.inside = rows % 16 == 0 and self.wide % SUB == 0

    def halo_count(self, o):
        return min(self.tokens, WINDOW - (o - 1) * self.tokens)

    def halo_first(self, o):
        return max(0, WINDOW - o * self.tokens)


class Link:
    def __init__(self, ledger, key, src, dst, sems, at, device, send_if=None, recv_if=None):
        self.ledger, self.key = ledger, key
        self.send_if, self.recv_if = send_if, recv_if
        self.copy = pltpu.make_async_remote_copy(
            src_ref=src, dst_ref=dst, send_sem=sems[0].at[at], recv_sem=sems[1].at[at],
            device_id=device, device_id_type=MESH,
        )

    def guarded(self, condition, action):
        if condition is None:
            action()
        else:
            pl.when(condition)(action)

    def start(self):
        self.guarded(self.send_if, self.copy.start)
        self.ledger[self.key + ("send",)] = lambda: self.guarded(self.send_if, self.copy.wait_send)
        self.ledger[self.key + ("recv",)] = lambda: self.guarded(self.recv_if, self.copy.wait_recv)

    def wait_recv(self):
        self.ledger.pop(self.key + ("recv",))
        self.guarded(self.recv_if, self.copy.wait_recv)


def fused_kernel(
    pn,
    lim_ref, q_ref, g_ref, k_ref, v_ref, ln_ref, de_ref, at_ref, w_ref, rs_ref, cs_ref,
    dq_ref, dk_ref, dv_ref, sc_ref, fac_ref,
    st, wv, abuf, turned, qb, gb, kb, vb, stb, dva, dka, dqb, dkb, hsv, hsk, hrv, hrk, act, vga, acc, sbuf, rbuf,
    xs, xr,
    own_sem, in_s, in_r, halo_s, halo_r, back_s, back_r, act_own, act_s, act_r, fwd_s, fwd_r,
    vg_s, vg_r, dq_s, dq_r, dk_s, dk_r, out_sem, rs_s, rs_r, x_s, x_r,
):
    n, n_head, gather, upper = pn.n, pn.n_head, pn.gather, pn.upper
    split, kv, length, tokens = pn.split, pn.kv, pn.tok_len, pn.tokens
    group, subs = pn.group, pn.subs
    me, hd = lax.axis_index("tok"), lax.axis_index("head")
    c, u = lax.rem(me, gather), me // gather
    place, block = lax.rem(me, split), me // split
    kw, qw = kv * HD, kv * group * HD
    rows = pn.rows
    ledger = {}

    def at_plane(j):
        return {"tok": me - c + xor(c, j)}

    near = [(j, h) for j in range(gather) for h in range(n_head) if j or h]
    far = list(range(1, upper))
    near_ids = [{"tok": me - c + xor(c, j), "head": xor(hd, h)} for j, h in near]
    far_ids = [{"tok": xor(u, i) * gather + c} for i in far]
    barrier = pltpu.get_barrier_semaphore()
    for partner in near_ids + far_ids:
        pl.semaphore_signal(barrier, inc=1, device_id=partner, device_id_type=MESH)
    lone = []
    if split == 1:
        for o in range(1, pn.reach + 1):
            lone.append(o)
            @pl.when(block + o < pn.blocks)
            def _(o=o):
                pl.semaphore_signal(barrier, inc=1, device_id={"tok": me + o}, device_id_type=MESH)

            @pl.when(block >= o)
            def _(o=o):
                pl.semaphore_signal(barrier, inc=1, device_id={"tok": me - o}, device_id_type=MESH)

    def cols(index, size):
        return pl.ds(pl.multiple_of(index * size, 128), size)

    own = [
        pltpu.make_async_copy(k_ref.at[:, cols(place, kw)], kb.at[pl.ds(WINDOW + place * length, length)], own_sem.at[0]),
        pltpu.make_async_copy(v_ref.at[:, cols(place, kw)], vb.at[pl.ds(WINDOW + place * length, length)], own_sem.at[1]),
        pltpu.make_async_copy(q_ref.at[:, cols(place, qw)], qb.at[pl.ds(place * length, length)], own_sem.at[2]),
        pltpu.make_async_copy(g_ref.at[:, cols(place, qw)], gb.at[pl.ds(place * length, length)], own_sem.at[3]),
        pltpu.make_async_copy(st.at[pl.ds(place * kv, kv)], stb.at[place], own_sem.at[4]),
    ]
    half = pn.half
    low = lax.rem(hd, pn.share) * half
    if pn.inside:
        load = pltpu.make_async_copy(
            at_ref.at[:, cols(lax.rem(hd, pn.share), pn.wide)], abuf, own_sem.at[5]
        )
        load.start()
    for copy in own[:4]:
        copy.start()
    weight_in = pltpu.make_async_copy(w_ref, wv, own_sem.at[6])
    weight_in.start()

    pl.semaphore_wait(barrier, len(near_ids) + len(far_ids))
    for o in lone:
        @pl.when(block + o < pn.blocks)
        def _():
            pl.semaphore_wait(barrier, 1)

        @pl.when(block >= o)
        def _():
            pl.semaphore_wait(barrier, 1)

    def exchange(a, j):
        other = xor(place, j)
        src, dst = [
            (k_ref.at[:, cols(other, kw)], kb.at[pl.ds(WINDOW + place * length, length)]),
            (v_ref.at[:, cols(other, kw)], vb.at[pl.ds(WINDOW + place * length, length)]),
            (q_ref.at[:, cols(other, qw)], qb.at[pl.ds(place * length, length)]),
            (g_ref.at[:, cols(other, qw)], gb.at[pl.ds(place * length, length)]),
            (st.at[pl.ds(other * kv, kv)], stb.at[place]),
        ][a]
        return Link(ledger, ("in", a, j), src, dst, (in_s, in_r), (a, j), at_plane(j))

    for a in (0, 1, 2, 3):
        for j in range(1, split):
            exchange(a, j).start()
    for i, ref in enumerate((ln_ref, de_ref)):
        stat = ref[...]
        if i == 0:
            stat = stat * LOG2E
        for k in range(pn.kv_local):
            st[k, i * group : (i + 1) * group] = stat[k * group : (k + 1) * group]
    own[4].start()
    for j in range(1, split):
        exchange(4, j).start()
    dva[...] = jnp.zeros_like(dva)
    dka[...] = jnp.zeros_like(dka)

    def turn(first, last):
        @pl.loop(first, last)
        def _(i):
            here = pl.ds(pl.multiple_of(i * SUB, SUB), SUB)
            turned[here, :] = abuf[:, here].T

    steps = pn.wide // SUB
    if pn.inside:
        load.wait()

    def halo(a, o):
        count, first = pn.halo_count(o), pn.halo_first(o)
        buf = (kb, vb)[a]
        return Link(
            ledger, ("halo", a, o), buf.at[pl.ds(WINDOW + tokens - count, count)],
            buf.at[pl.ds(first, count)], (halo_s, halo_r), (a, o - 1), {"tok": me + o * split},
            block + o < pn.blocks, block >= o,
        )

    for a in (0, 1):
        own[a].wait()
        for j in range(1, split):
            exchange(a, j).wait_recv()
        for o in range(1, pn.reach + 1):
            halo(a, o).start()

            @pl.when(block < o)
            def _(a=a, o=o):
                buf = (kb, vb)[a]
                here = pl.ds(pn.halo_first(o), pn.halo_count(o))
                buf[here] = jnp.zeros((pn.halo_count(o), kw), BF16)
    if pn.reach * tokens < WINDOW:
        rest = WINDOW - pn.reach * tokens
        for buf in (kb, vb):
            buf[pl.ds(0, rest)] = jnp.zeros((rest, kw), BF16)

    if pn.inside:
        turn(0, steps)

    def act_piece(i, owner):
        if pn.inside:
            return turned.at[pl.ds(pl.multiple_of((i * gather + owner) * rows, 16), rows)]
        return at_ref.at[(low + i) * gather + owner]

    act_mine = [
        pltpu.make_async_copy(act_piece(i, c), act.at[low + i, :, cols(c, length)], act_own.at[i])
        for i in range(half)
    ]
    for copy in act_mine:
        copy.start()

    def act_send(j, i):
        return Link(
            ledger, ("act", j, i), act_piece(i, xor(c, j)), act.at[low + i, :, cols(c, length)],
            (act_s, act_r), (j, i), at_plane(j),
        )

    def act_forward(j):
        piece = act.at[pl.ds(low, half), :, cols(xor(c, j), length)]
        return Link(ledger, ("forward", j), piece, piece, (fwd_s, fwd_r), (j,), {"head": xor(hd, 1)})

    for i in range(half):
        for j in range(1, gather):
            act_send(j, i).start()
    for a in (0, 1):
        for o in range(1, pn.reach + 1):
            halo(a, o).wait_recv()

    seen = WINDOW + SUB
    chunk = seen // 3
    lanes = group * SUB

    def unit(b, kh, sub):
        start = pl.multiple_of(b * length + sub * SUB, SUB)
        rows_q = pl.ds(start, SUB)
        head = kh * group * HD
        query = jnp.concatenate(
            [qb[rows_q, head + m * HD : head + (m + 1) * HD] for m in range(group)], axis=0
        )
        grad = jnp.concatenate(
            [gb[rows_q, head + m * HD : head + (m + 1) * HD] for m in range(group)], axis=0
        )
        lane_q = pl.ds(pl.multiple_of(sub * SUB, SUB), SUB)
        norm, delta = [
            jnp.concatenate([stb[b, kh, i * group + m : i * group + m + 1, lane_q] for m in range(group)], axis=1)
            for i in range(2)
        ]
        total = jnp.zeros((lanes, HD), F32)
        for piece in range(3):
            here = pl.ds(pl.multiple_of(start + piece * chunk, SUB), chunk)
            keys = kb[here, kh * HD : (kh + 1) * HD]
            values = vb[here, kh * HD : (kh + 1) * HD]
            scores = lax.dot_general(
                keys, query, (((1,), (1,)), ((), ())), preferred_element_type=F32
            )
            prob = jnp.exp2(scores * (QUERY_SCALE * LOG2E) - norm)
            if piece == 0:
                edge = WINDOW - WINDOW_MIN + SUB
                row = lax.broadcasted_iota(jnp.int32, (edge, lanes), 0)
                lane = lax.broadcasted_iota(jnp.int32, (edge, lanes), 1)
                limit = jnp.full((edge, lanes), 0, jnp.int32)
                for m in range(group):
                    limit = jnp.where(
                        lane // SUB == m, lim_ref[(place * kv + kh) * group + m], limit
                    )
                visible = WINDOW + lax.rem(lane, SUB) - row < limit
                prob = jnp.concatenate(
                    [jnp.where(visible, prob[:edge], 0.0), prob[edge:]], axis=0
                )
            if piece == 2:
                row = lax.broadcasted_iota(jnp.int32, (SUB, lanes), 0)
                lane = lax.broadcasted_iota(jnp.int32, (SUB, lanes), 1)
                visible = row <= lax.rem(lane, SUB)
                prob = jnp.concatenate(
                    [prob[: chunk - SUB], jnp.where(visible, prob[chunk - SUB :], 0.0)], axis=0
                )
            dva[here, kh * HD : (kh + 1) * HD] += jnp.dot(
                prob.astype(BF16), grad, preferred_element_type=F32
            )
            dprob = lax.dot_general(
                values, grad, (((1,), (1,)), ((), ())), preferred_element_type=F32
            )
            dscore = (QUERY_SCALE * prob * (dprob - delta)).astype(BF16)
            dka[here, kh * HD : (kh + 1) * HD] += jnp.dot(
                dscore, query, preferred_element_type=F32
            )
            total = total + lax.dot_general(
                dscore, keys, (((0,), (0,)), ((), ())), preferred_element_type=F32
            )
        low_q = total.astype(BF16)
        for m in range(group):
            dqb[rows_q, head + m * HD : head + (m + 1) * HD] = low_q[m * SUB : (m + 1) * SUB]

    def dq_send(j):
        other = xor(place, j)
        src = dqb.at[pl.ds(other * length, length)]
        return Link(
            ledger, ("dq", j), src, dq_ref.at[:, cols(place, qw)], (dq_s, dq_r), (j,), at_plane(j))

    def local_out(src, dst, i):
        return pltpu.make_async_copy(src, dst, out_sem.at[i])

    for j in range(split):
        b = xor(place, j)
        for a in (2, 3, 4):
            if j:
                exchange(a, j).wait_recv()
            else:
                own[a].wait()
        for kh in range(kv):
            @pl.loop(0, subs)
            def _(sub, b=b, kh=kh):
                unit(b, kh, sub)

        if j == 0:
            for copy in act_mine:
                copy.wait()
            if pn.share == 2:
                act_forward(0).start()

    def back(a, o):
        count, first = pn.halo_count(o), pn.halo_first(o)
        return Link(
            ledger, ("back", a, o), (hsv, hsk)[a].at[pl.ds(first, count)],
            (hrv, hrk)[a].at[o - 1, pl.ds(0, count)], (back_s, back_r), (a, o - 1),
            {"tok": me - o * split}, block >= o, block + o < pn.blocks,
        )

    for a in (0, 1):
        (hsv, hsk)[a][...] = (dva, dka)[a][pl.ds(0, WINDOW)].astype(BF16)
        for o in range(1, pn.reach + 1):
            back(a, o).start()

    def add_back(a):
        for o in range(1, pn.reach + 1):
            back(a, o).wait_recv()

            @pl.when(block + o < pn.blocks)
            def _(o=o):
                count = pn.halo_count(o)
                here = pl.ds(WINDOW + tokens - count, count)
                total = (dva, dka)[a]
                total[here] = total[here] + (hrv, hrk)[a][o - 1, pl.ds(0, count)].astype(F32)

    cut = vga.shape[1] // 2

    def vg_copy(j, owner, part_of):
        piece = vga.at[owner, pl.ds(part_of * cut, cut)]
        return Link(
            ledger, ("vg", j, part_of), piece, piece, (vg_s, vg_r), (j, part_of),
            at_plane(j if j < 3 else (2, 1)[part_of]),
        )

    def vg_send(j, h):
        return vg_copy(j, c if j < 3 else xor(c, (1, 2)[h]), h)

    def vg_wait(j, h):
        vg_copy(j, xor(c, j), h).wait_recv()

    add_back(0)
    vga[c] = dva[pl.ds(WINDOW, tokens)].astype(BF16)
    if gather > 1:
        for h in (0, 1):
            vg_send(1, h).start()
            vg_send(2, 1 - h).start()
    for j in range(1, gather):
        for i in range(half):
            act_send(j, i).wait_recv()
        if pn.share == 2:
            act_forward(j).start()

    if pn.share == 2:
        for j in range(gather):
            piece_in = act.at[pl.ds(half - low, half), :, cols(xor(c, j), length)]
            Link(
                ledger, ("forward", j), piece_in, piece_in, (fwd_s, fwd_r), (j,),
                {"head": xor(hd, 1)},
            ).wait_recv()

    bits, part = pn.bits, pn.part
    counts = [upper >> (p + 1) for p in range(bits)]
    starts = [sum(counts[:p]) for p in range(bits)]
    partners = [{"tok": xor(u, 1 << p) * gather + c} for p in range(bits)]

    def bit_of(index, k):
        return lax.rem(index // (1 << k), 2)

    def block_at(phase, j, other):
        index = 0
        for k in range(phase):
            index = index + (1 << k) * bit_of(u, k)
        mine = bit_of(u, phase)
        index = index + (1 << phase) * ((1 - mine) if other else mine)
        return index + (1 << (phase + 1)) * j

    def copy_of(s, p):
        here = pl.ds(starts[p], counts[p])
        return Link(
            ledger, ("sum", s, p), sbuf.at[s, here], rbuf.at[s, here], (rs_s, rs_r), (s, p), partners[p])

    def product(s, index):
        if split == gather:
            return jnp.dot(act[index], vga[xor(c, s)], preferred_element_type=F32)
        whole = vga[...].reshape(gather * length, part)
        return jnp.dot(act[index], whole, preferred_element_type=F32)

    def pass_on():
        vg_wait(1, 0)
        vg_send(3, 0).start()
        vg_wait(2, 1)
        vg_send(3, 1).start()

    if split == 1 and gather > 1:
        pass_on()
        vg_wait(1, 1)
        vg_wait(2, 0)
        vg_wait(3, 0)
        vg_wait(3, 1)
    for s in range(pn.streams):
        if s == 1:
            pass_on()
        if s == 3:
            vg_wait(3, 0)
            vg_wait(3, 1)
        elif s:
            vg_wait(s, s % 2)

        @pl.loop(0, counts[0])
        def _(j, s=s):
            sbuf[s, j] = product(s, block_at(0, j, True)).astype(BF16)

        copy_of(s, 0).start()

        @pl.loop(0, counts[0])
        def _(j, s=s):
            index = block_at(0, j, False)
            acc[s, index] = product(s, index)

    outs = []
    outs.append(local_out(dqb.at[pl.ds(place * length, length)], dq_ref.at[:, cols(place, qw)], 0))
    outs[-1].start()
    for j in range(1, split):
        dq_send(j).start()

    add_back(1)
    dkb[...] = dka[pl.ds(WINDOW, tokens)].astype(BF16)

    def dk_send(j):
        other = xor(place, j)
        return Link(
            ledger, ("dk", j), dkb.at[pl.ds(other * length, length)], dk_ref.at[:, cols(place, kw)],
            (dk_s, dk_r), (j,), at_plane(j),
        )

    outs.append(local_out(dkb.at[pl.ds(place * length, length)], dk_ref.at[:, cols(place, kw)], 1))
    outs[-1].start()
    for j in range(1, split):
        dk_send(j).start()
    if split == gather:
        for j in range(gather):
            src = xor(c, j)
            outs.append(local_out(
                vga.at[src, pl.ds(c * length, length)], dv_ref.at[:, cols(src, kw)], 2 + j))
            outs[-1].start()
    else:
        outs.append(local_out(vga.at[c], dv_ref, 2))
        outs[-1].start()

    weight_in.wait()
    weight_f = wv[...].astype(F32)
    weight_sum = jnp.sum(weight_f * weight_f)

    for p in range(bits):
        for s in range(pn.streams):
            copy_of(s, p).wait_recv()

            @pl.loop(0, counts[p])
            def _(j, s=s, p=p):
                index = block_at(p, j, False)
                acc[s, index] = acc[s, index] + rbuf[s, starts[p] + j].astype(F32)

            if p + 1 < bits:
                @pl.loop(0, counts[p + 1])
                def _(j, s=s, p=p):
                    index = block_at(p + 1, j, True)
                    sbuf[s, starts[p + 1] + j] = acc[s, index].astype(BF16)

                copy_of(s, p + 1).start()

    row_sum = jnp.zeros((rows, 1), F32)
    for s in range(pn.streams):
        wg = acc[s, u]
        row_sum = row_sum + jnp.sum(wg * wg, axis=1, keepdims=True)
    diag = lax.broadcasted_iota(jnp.int32, (rows, rows), 0) == lax.broadcasted_iota(
        jnp.int32, (rows, rows), 1)
    row_old = jnp.sum(jnp.where(diag, rs_ref[...], 0.0), axis=1, keepdims=True)
    row_mix = DECAY_RATE * row_old + (1.0 - DECAY_RATE) * (row_sum / pn.width)
    row_mean = jnp.sum(row_mix) / rows
    scaled_sum = jnp.float32(0.0)
    for s in range(pn.streams):
        wg = acc[s, u]
        here = cols(xor(c, s), part) if split == gather else slice(0, part)
        col_new = jnp.sum(wg * wg, axis=0, keepdims=True) / rows
        col_mix = DECAY_RATE * cs_ref[:, here] + (1.0 - DECAY_RATE) * col_new
        scaled = wg / jnp.sqrt(row_mix * col_mix / row_mean)
        sc_ref[:, here] = scaled
        scaled_sum = scaled_sum + jnp.sum(scaled * scaled)

    row = lax.broadcasted_iota(jnp.int32, (8, 128), 0)
    xs[0] = jnp.where(row < 4, scaled_sum, weight_sum)

    def share(level, i, partner):
        slot = i + (len(near) if level else 0)
        return Link(ledger, ("share", slot), xs.at[level], xr.at[slot], (x_s, x_r), (slot,), partner)

    for level, ids in enumerate((near_ids, far_ids)):
        for i, partner in enumerate(ids):
            share(level, i, partner).start()
        total = xs[level]
        for i, partner in enumerate(ids):
            share(level, i, partner).wait_recv()
            total = total + xr[i + (len(near) if level else 0)]
        xs[level + 1] = total
    sums = xs[2]
    size = float(rows * n * pn.width * n_head)
    rms_scaled = jnp.sqrt(sums[0:1] / size)
    rms_weight = jnp.sqrt(sums[4:5] / size)
    fac_ref[...] = jnp.broadcast_to(rms_weight / jnp.maximum(1.0, rms_scaled), fac_ref.shape)

    for copy in outs:
        copy.wait()
    for wait in ledger.values():
        wait()


def fused(pn, limits, query, grad, keys, values, norm, delta, act, weight, row_state, col_state):
    kw, qw = pn.kv * HD, pn.kv * pn.group * HD
    whole = WINDOW + pn.tokens
    smem = pl.BlockSpec(memory_space=pltpu.SMEM)
    vmem = pl.BlockSpec(memory_space=pltpu.VMEM)
    hbm = pl.BlockSpec(memory_space=pl.ANY)
    dma = pltpu.SemaphoreType.DMA
    half = pn.half
    peers = pn.gather * pn.n_head - 1 + pn.upper - 1
    reach, gather, split = pn.reach, pn.gather, pn.split
    piece = (pn.tokens, kw) if split == gather else (pn.tok_len, kw)
    return pl.pallas_call(
        functools.partial(fused_kernel, pn),
        out_shape=[
            jax.ShapeDtypeStruct(query.shape, BF16),
            jax.ShapeDtypeStruct(keys.shape, BF16),
            jax.ShapeDtypeStruct(keys.shape, BF16),
            jax.ShapeDtypeStruct((pn.rows, pn.width), F32),
            jax.ShapeDtypeStruct((8, 128), F32),
        ],
        in_specs=[smem, hbm, hbm, hbm, hbm, vmem, vmem, hbm, hbm, vmem, vmem],
        out_specs=[hbm, hbm, hbm, vmem, vmem],
        scratch_shapes=[
            pltpu.VMEM((pn.kv_local, 2 * pn.group, pn.tok_len), F32),
            pltpu.VMEM((pn.rows, pn.width), BF16),
            pltpu.VMEM((pn.tok_len, pn.wide) if pn.inside else act.shape[1:], BF16),
            pltpu.VMEM((pn.wide, pn.tok_len) if pn.inside else (16, 128), BF16),
            pltpu.VMEM((pn.tokens, qw), BF16),
            pltpu.VMEM((pn.tokens, qw), BF16),
            pltpu.VMEM((whole, kw), BF16),
            pltpu.VMEM((whole, kw), BF16),
            pltpu.VMEM((split, pn.kv, 2 * pn.group, pn.tok_len), F32),
            pltpu.VMEM((whole, kw), F32),
            pltpu.VMEM((whole, kw), F32),
            pltpu.VMEM((pn.tokens, qw), BF16),
            pltpu.VMEM((pn.tokens, kw), BF16),
            pltpu.VMEM((WINDOW, kw), BF16),
            pltpu.VMEM((WINDOW, kw), BF16),
            pltpu.VMEM((reach, min(pn.tokens, WINDOW), kw), BF16),
            pltpu.VMEM((reach, min(pn.tokens, WINDOW), kw), BF16),
            pltpu.VMEM((pn.upper, pn.rows, gather * pn.tok_len), BF16),
            pltpu.VMEM((gather,) + piece, BF16),
            pltpu.VMEM((pn.streams, pn.upper, pn.rows, pn.part), F32),
            pltpu.VMEM((pn.streams, pn.upper - 1, pn.rows, pn.part), BF16),
            pltpu.VMEM((pn.streams, pn.upper - 1, pn.rows, pn.part), BF16),
            pltpu.VMEM((3, 8, 128), F32),
            pltpu.VMEM((peers, 8, 128), F32),
            dma((7,)), dma((5, split)), dma((5, split)), dma((2, reach)), dma((2, reach)),
            dma((2, reach)), dma((2, reach)), dma((half,)),
            dma((gather, half)), dma((gather, half)), dma((gather,)), dma((gather,)),
            dma((gather, 2)), dma((gather, 2)), dma((split,)), dma((split,)),
            dma((split,)), dma((split,)), dma((2 + gather,)),
            dma((pn.streams, pn.bits)), dma((pn.streams, pn.bits)), dma((peers,)), dma((peers,)),
        ],
        compiler_params=pltpu.CompilerParams(
            collective_id=0, has_side_effects=True, vmem_limit_bytes=56 * 1024 * 1024
        ),
        name="fused",
    )(limits, query, grad, keys, values, norm, delta, act, weight, row_state, col_state)


def finish_kernel(
    dq_in, dk_in, dv_in, w_in, sc_in, fac_ref, dq, dk, dv, new, upd,
    dq_v, dk_v, dv_v, w_v, sc_v, new_v, upd_v, in_sem, out_sem,
):
    pairs = [(dq_in, dq_v, dq), (dk_in, dk_v, dk), (dv_in, dv_v, dv)]
    loads = [pltpu.make_async_copy(sc_in, sc_v, in_sem.at[3]), pltpu.make_async_copy(w_in, w_v, in_sem.at[4])]
    for copy in loads:
        copy.start()
    ins = [pltpu.make_async_copy(a, b, in_sem.at[i]) for i, (a, b, _) in enumerate(pairs)]
    outs = [pltpu.make_async_copy(b, d, out_sem.at[i]) for i, (_, b, d) in enumerate(pairs)]
    outs += [pltpu.make_async_copy(new_v, new, out_sem.at[3]), pltpu.make_async_copy(upd_v, upd, out_sem.at[4])]
    for copy in ins:
        copy.start()
    for copy in loads:
        copy.wait()
    update = sc_v[...] * fac_ref[0:1, 0:1]
    upd_v[...] = update
    outs[4].start()
    new_v[...] = (w_v[...].astype(F32) - LEARN_RATE * update).astype(BF16)
    outs[3].start()
    for i in range(3):
        ins[i].wait()
        outs[i].start()
    for copy in outs:
        copy.wait()


def finish(dq, dk, dv, weight, scaled, factor):
    hbm = pl.BlockSpec(memory_space=pl.ANY)
    vmem = pl.BlockSpec(memory_space=pltpu.VMEM)
    arrays = [dq, dk, dv, weight, scaled]
    outs = [dq, dk, dv, weight, scaled]
    return pl.pallas_call(
        finish_kernel,
        out_shape=[jax.ShapeDtypeStruct(x.shape, x.dtype) for x in outs],
        in_specs=[hbm] * 5 + [vmem],
        out_specs=[hbm] * 5,
        scratch_shapes=[pltpu.VMEM(x.shape, x.dtype) for x in arrays + [weight, scaled]]
        + [pltpu.SemaphoreType.DMA((5,)), pltpu.SemaphoreType.DMA((5,))],
        name="finish",
    )(*arrays, factor)


def shards(
    query_rows, key_rows, value_rows, out_grad, log_norm, delta_rows, window_len,
    activations, value_weight, row_state, col_state, *, n, n_head,
):
    tok_len = query_rows.shape[0]
    kv_local = key_rows.shape[1] // HD
    group = query_rows.shape[1] // key_rows.shape[1]
    rows, width = value_weight.shape
    pn = Plan(n, n_head, tok_len, kv_local, group, width, rows)

    act = activations if pn.inside else activations.T.reshape(n, rows, tok_len)
    query_grad, key_grad, value_grad, scaled, factor = fused(
        pn, window_len, query_rows, out_grad, key_rows, value_rows, log_norm.T, delta_rows.T, act,
        value_weight, row_state, col_state,
    )
    return finish(query_grad, key_grad, value_grad, value_weight, scaled, factor)


def solution(mesh):
    both = P("tok", "head")
    return jax.shard_map(
        functools.partial(shards, n=mesh.shape["tok"], n_head=mesh.shape["head"]),
        mesh=mesh,
        in_specs=(
            both, both, both, both, both, both, P("head"), P("tok", None),
            both, P("head", "tok"), both,
        ),
        out_specs=(both,) * 5,
        check_vma=False,
    )
```

```python
import functools
import math

import jax
import jax.numpy as jnp
from jax import lax
from jax.experimental import pallas as pl
from jax.experimental.pallas import tpu as pltpu
from jax.sharding import PartitionSpec as P

HD = 128
WINDOW = 1024
WINDOW_MIN = 896
SUB = 128
QUERY_SCALE = 1.0 / 12.0
LOG2E = math.log2(math.e)
DECAY_RATE = 0.9
LEARN_RATE = 0.05
F32 = jnp.float32
BF16 = jnp.bfloat16
MESH = pl.DeviceIdType.MESH


def xor(index, j):
    k = 0
    while (1 << k) <= j:
        if (j >> k) & 1:
            index = index + (1 << k) * (1 - 2 * lax.rem(index // (1 << k), 2))
        k += 1
    return index


class Plan:
    def __init__(self, n, n_head, tok_len, kv_local, group, width, rows):
        self.n, self.n_head, self.tok_len = n, n_head, tok_len
        self.kv_local, self.group = kv_local, group
        self.width, self.rows = width, rows
        self.gather = 4 if n % 4 == 0 else 1
        self.upper = n // self.gather
        self.split = self.gather if kv_local % self.gather == 0 else 1
        self.kv = kv_local // self.split
        self.tokens = self.split * tok_len
        self.blocks = n // self.split
        self.reach = min(-(-WINDOW // self.tokens), self.blocks - 1)
        self.subs = tok_len // SUB
        self.streams = self.split
        self.part = width // self.streams
        self.bits = int(math.log2(self.upper))
        self.share = 2 if n_head % 2 == 0 and self.upper % 2 == 0 else 1
        self.half = self.upper // self.share
        self.wide = self.half * self.gather * rows
        self.inside = rows % 16 == 0 and self.wide % SUB == 0
        first = rows * 5 // 6 // 16 * 16
        cut = self.inside and self.split == self.gather and first
        self.parts = [(0, first), (first, rows - first)] if cut else [(0, rows)]
        self.flat = n * n_head <= 64

    def halo_count(self, o):
        return min(self.tokens, WINDOW - (o - 1) * self.tokens)

    def halo_first(self, o):
        return max(0, WINDOW - o * self.tokens)


class Link:
    def __init__(self, ledger, key, src, dst, sems, at, device, send_if=None, recv_if=None):
        self.ledger, self.key = ledger, key
        self.send_if, self.recv_if = send_if, recv_if
        self.copy = pltpu.make_async_remote_copy(
            src_ref=src, dst_ref=dst, send_sem=sems[0].at[at], recv_sem=sems[1].at[at],
            device_id=device, device_id_type=MESH,
        )

    def guarded(self, condition, action):
        if condition is None:
            action()
        else:
            pl.when(condition)(action)

    def start(self):
        self.guarded(self.send_if, self.copy.start)
        self.ledger[self.key + ("send",)] = lambda: self.guarded(self.send_if, self.copy.wait_send)
        self.ledger[self.key + ("recv",)] = lambda: self.guarded(self.recv_if, self.copy.wait_recv)

    def wait_recv(self):
        self.ledger.pop(self.key + ("recv",))
        self.guarded(self.recv_if, self.copy.wait_recv)


def fused_kernel(
    pn,
    lim_in, q_ref, g_ref, k_ref, v_ref, ln_in, de_in, at_ref, w_ref, rs_in, cs_in,
    dq_ref, dk_ref, dv_ref, sc_out, fac_out,
    lim_ref, ln_ref, de_ref, rs_ref, cs_ref, sc_ref, fac_ref, st, wv, abuf, turned, qb, gb, kb, vb, stb, dva, dka, dqb, dkb, hsv, hsk, hrv, hrk, act, vga, acc, sbuf, rbuf,
    xs, xr,
    own_sem, small_sem, in_s, in_r, halo_s, halo_r, back_s, back_r, act_own, act_s, act_r, fwd_s, fwd_r,
    vg_s, vg_r, dq_s, dq_r, dk_s, dk_r, out_sem, rs_s, rs_r, x_s, x_r,
):
    n, n_head, gather, upper = pn.n, pn.n_head, pn.gather, pn.upper
    split, kv, length, tokens = pn.split, pn.kv, pn.tok_len, pn.tokens
    group, subs = pn.group, pn.subs
    me, hd = lax.axis_index("tok"), lax.axis_index("head")
    c, u = lax.rem(me, gather), me // gather
    place, block = lax.rem(me, split), me // split
    kw, qw = kv * HD, kv * group * HD
    rows = pn.rows
    ledger = {}

    def at_plane(j):
        return {"tok": me - c + xor(c, j)}

    near = [(j, h) for j in range(gather) for h in range(n_head) if j or h]
    far = list(range(1, upper))
    near_ids = [{"tok": me - c + xor(c, j), "head": xor(hd, h)} for j, h in near]
    far_ids = [{"tok": xor(u, i) * gather + c} for i in far]
    barrier = pltpu.get_barrier_semaphore()
    for partner in near_ids + far_ids:
        pl.semaphore_signal(barrier, inc=1, device_id=partner, device_id_type=MESH)
    lone = []
    if split == 1:
        for o in range(1, pn.reach + 1):
            lone.append(o)
            @pl.when(block + o < pn.blocks)
            def _(o=o):
                pl.semaphore_signal(barrier, inc=1, device_id={"tok": me + o}, device_id_type=MESH)

            @pl.when(block >= o)
            def _(o=o):
                pl.semaphore_signal(barrier, inc=1, device_id={"tok": me - o}, device_id_type=MESH)

    def cols(index, size):
        return pl.ds(pl.multiple_of(index * size, 128), size)

    own = [
        pltpu.make_async_copy(k_ref.at[:, cols(place, kw)], kb.at[pl.ds(WINDOW + place * length, length)], own_sem.at[0]),
        pltpu.make_async_copy(v_ref.at[:, cols(place, kw)], vb.at[pl.ds(WINDOW + place * length, length)], own_sem.at[1]),
        pltpu.make_async_copy(q_ref.at[:, cols(place, qw)], qb.at[pl.ds(place * length, length)], own_sem.at[2]),
        pltpu.make_async_copy(g_ref.at[:, cols(place, qw)], gb.at[pl.ds(place * length, length)], own_sem.at[3]),
        pltpu.make_async_copy(st.at[pl.ds(place * kv, kv)], stb.at[place], own_sem.at[4]),
    ]
    half = pn.half
    low = lax.rem(hd, pn.share) * half
    if pn.inside:
        load = pltpu.make_async_copy(
            at_ref.at[:, cols(lax.rem(hd, pn.share), pn.wide)], abuf, own_sem.at[5]
        )
        load.start()
    for copy in own[:4]:
        copy.start()
    small = [
        pltpu.make_async_copy(src, dst, small_sem.at[i])
        for i, (src, dst) in enumerate(
            [(ln_in, ln_ref), (de_in, de_ref), (lim_in, lim_ref), (rs_in, rs_ref), (cs_in, cs_ref)])
    ]
    for copy in small:
        copy.start()
    weight_in = pltpu.make_async_copy(w_ref, wv, own_sem.at[6])
    weight_in.start()

    pl.semaphore_wait(barrier, len(near_ids) + len(far_ids))
    for o in lone:
        @pl.when(block + o < pn.blocks)
        def _():
            pl.semaphore_wait(barrier, 1)

        @pl.when(block >= o)
        def _():
            pl.semaphore_wait(barrier, 1)

    def exchange(a, j):
        other = xor(place, j)
        src, dst = [
            (k_ref.at[:, cols(other, kw)], kb.at[pl.ds(WINDOW + place * length, length)]),
            (v_ref.at[:, cols(other, kw)], vb.at[pl.ds(WINDOW + place * length, length)]),
            (q_ref.at[:, cols(other, qw)], qb.at[pl.ds(place * length, length)]),
            (g_ref.at[:, cols(other, qw)], gb.at[pl.ds(place * length, length)]),
            (st.at[pl.ds(other * kv, kv)], stb.at[place]),
        ][a]
        return Link(ledger, ("in", a, j), src, dst, (in_s, in_r), (a, j), at_plane(j))

    for a in (0, 1, 2, 3):
        for j in range(1, split):
            exchange(a, j).start()
    for copy in small:
        copy.wait()
    for i, ref in enumerate((ln_ref, de_ref)):
        stat = ref[...]
        if i == 0:
            stat = stat * LOG2E
        for k in range(pn.kv_local):
            st[k, i * group : (i + 1) * group] = stat[k * group : (k + 1) * group]
    own[4].start()
    for j in range(1, split):
        exchange(4, j).start()
    dva[...] = jnp.zeros_like(dva)
    dka[...] = jnp.zeros_like(dka)

    def turn(first, last):
        @pl.loop(first, last)
        def _(i):
            here = pl.ds(pl.multiple_of(i * SUB, SUB), SUB)
            turned[here, :] = abuf[:, here].T

    steps = pn.wide // SUB
    if pn.inside:
        load.wait()

    def halo(a, o):
        count, first = pn.halo_count(o), pn.halo_first(o)
        buf = (kb, vb)[a]
        return Link(
            ledger, ("halo", a, o), buf.at[pl.ds(WINDOW + tokens - count, count)],
            buf.at[pl.ds(first, count)], (halo_s, halo_r), (a, o - 1), {"tok": me + o * split},
            block + o < pn.blocks, block >= o,
        )

    for a in (0, 1):
        own[a].wait()
        for j in range(1, split):
            exchange(a, j).wait_recv()
        for o in range(1, pn.reach + 1):
            halo(a, o).start()

            @pl.when(block < o)
            def _(a=a, o=o):
                buf = (kb, vb)[a]
                here = pl.ds(pn.halo_first(o), pn.halo_count(o))
                buf[here] = jnp.zeros((pn.halo_count(o), kw), BF16)
    if pn.reach * tokens < WINDOW:
        rest = WINDOW - pn.reach * tokens
        for buf in (kb, vb):
            buf[pl.ds(0, rest)] = jnp.zeros((rest, kw), BF16)

    if pn.inside:
        turn(0, steps)

    parts = pn.parts

    def act_piece(i, owner, r):
        first, size = parts[r]
        if pn.inside:
            here = pl.multiple_of((i * gather + owner) * rows + first, 16)
            return turned.at[pl.ds(here, size)]
        return at_ref.at[(low + i) * gather + owner]

    act_mine = [
        pltpu.make_async_copy(
            act_piece(i, c, r), act.at[low + i, pl.ds(*parts[r]), cols(c, length)], act_own.at[i, r])
        for i in range(half) for r in range(len(parts))
    ]
    for copy in act_mine:
        copy.start()

    def act_send(j, i, r):
        return Link(
            ledger, ("act", j, i, r), act_piece(i, xor(c, j), r),
            act.at[low + i, pl.ds(*parts[r]), cols(c, length)],
            (act_s, act_r), (j, i, r), at_plane(j),
        )

    def act_forward(j, i, r, start=low):
        piece = act.at[start + i, pl.ds(*parts[r]), cols(xor(c, j), length)]
        return Link(
            ledger, ("forward", j, i, r), piece, piece, (fwd_s, fwd_r), (j, i, r),
            {"head": xor(hd, 1)})

    order = [(j, i) for i in range(half) for j in (1, 2, 3)]
    if gather == 1:
        order = []

    def act_out(r):
        for j, i in order:
            act_send(j, i, r).start()

    def act_pass(r):
        for j, i in order:
            act_send(j, i, r).wait_recv()
            if pn.share == 2:
                act_forward(j, i, r).start()

    def act_ready(r):
        if pn.share == 2:
            for j, i in [(0, i) for i in range(half)] + order:
                act_forward(j, i, r, half - low).wait_recv()

    act_out(0)
    for a in (0, 1):
        for o in range(1, pn.reach + 1):
            halo(a, o).wait_recv()

    seen = WINDOW + SUB
    chunk = seen // 3
    lanes = group * SUB

    def unit(b, kh, sub):
        start = pl.multiple_of(b * length + sub * SUB, SUB)
        rows_q = pl.ds(start, SUB)
        head = kh * group * HD
        query = jnp.concatenate(
            [qb[rows_q, head + m * HD : head + (m + 1) * HD] for m in range(group)], axis=0
        )
        grad = jnp.concatenate(
            [gb[rows_q, head + m * HD : head + (m + 1) * HD] for m in range(group)], axis=0
        )
        lane_q = pl.ds(pl.multiple_of(sub * SUB, SUB), SUB)
        norm, delta = [
            jnp.concatenate([stb[b, kh, i * group + m : i * group + m + 1, lane_q] for m in range(group)], axis=1)
            for i in range(2)
        ]
        total = jnp.zeros((lanes, HD), F32)
        for piece in range(3):
            here = pl.ds(pl.multiple_of(start + piece * chunk, SUB), chunk)
            keys = kb[here, kh * HD : (kh + 1) * HD]
            values = vb[here, kh * HD : (kh + 1) * HD]
            scores = lax.dot_general(
                keys, query, (((1,), (1,)), ((), ())), preferred_element_type=F32
            )
            prob = jnp.exp2(scores * (QUERY_SCALE * LOG2E) - norm)
            if piece == 0:
                edge = WINDOW - WINDOW_MIN + SUB
                row = lax.broadcasted_iota(jnp.int32, (edge, lanes), 0)
                lane = lax.broadcasted_iota(jnp.int32, (edge, lanes), 1)
                limit = jnp.full((edge, lanes), 0, jnp.int32)
                for m in range(group):
                    limit = jnp.where(
                        lane // SUB == m, lim_ref[(place * kv + kh) * group + m], limit
                    )
                visible = WINDOW + lax.rem(lane, SUB) - row < limit
                prob = jnp.concatenate(
                    [jnp.where(visible, prob[:edge], 0.0), prob[edge:]], axis=0
                )
            if piece == 2:
                row = lax.broadcasted_iota(jnp.int32, (SUB, lanes), 0)
                lane = lax.broadcasted_iota(jnp.int32, (SUB, lanes), 1)
                visible = row <= lax.rem(lane, SUB)
                prob = jnp.concatenate(
                    [prob[: chunk - SUB], jnp.where(visible, prob[chunk - SUB :], 0.0)], axis=0
                )
            dva[here, kh * HD : (kh + 1) * HD] += jnp.dot(
                prob.astype(BF16), grad, preferred_element_type=F32
            )
            dprob = lax.dot_general(
                values, grad, (((1,), (1,)), ((), ())), preferred_element_type=F32
            )
            dscore = (QUERY_SCALE * prob * (dprob - delta)).astype(BF16)
            dka[here, kh * HD : (kh + 1) * HD] += jnp.dot(
                dscore, query, preferred_element_type=F32
            )
            total = total + lax.dot_general(
                dscore, keys, (((0,), (0,)), ((), ())), preferred_element_type=F32
            )
        low_q = total.astype(BF16)
        for m in range(group):
            dqb[rows_q, head + m * HD : head + (m + 1) * HD] = low_q[m * SUB : (m + 1) * SUB]

    def dq_send(j):
        other = xor(place, j)
        src = dqb.at[pl.ds(other * length, length)]
        return Link(
            ledger, ("dq", j), src, dq_ref.at[:, cols(place, qw)], (dq_s, dq_r), (j,), at_plane(j))

    def local_out(src, dst, i):
        return pltpu.make_async_copy(src, dst, out_sem.at[i])

    for j in range(split):
        b = xor(place, j)
        for a in (2, 3, 4):
            if j:
                exchange(a, j).wait_recv()
            else:
                own[a].wait()
        for kh in range(kv):
            @pl.loop(0, subs)
            def _(sub, b=b, kh=kh):
                unit(b, kh, sub)

        if j == 0:
            for copy in act_mine:
                copy.wait()
            if pn.share == 2:
                for r in range(len(parts)):
                    for i in range(half):
                        act_forward(0, i, r).start()

    def back(a, o):
        count, first = pn.halo_count(o), pn.halo_first(o)
        return Link(
            ledger, ("back", a, o), (hsv, hsk)[a].at[pl.ds(first, count)],
            (hrv, hrk)[a].at[o - 1, pl.ds(0, count)], (back_s, back_r), (a, o - 1),
            {"tok": me - o * split}, block >= o, block + o < pn.blocks,
        )

    for a in (0, 1):
        (hsv, hsk)[a][...] = (dva, dka)[a][pl.ds(0, WINDOW)].astype(BF16)
        for o in range(1, pn.reach + 1):
            back(a, o).start()

    def add_back(a):
        for o in range(1, pn.reach + 1):
            back(a, o).wait_recv()

            @pl.when(block + o < pn.blocks)
            def _(o=o):
                count = pn.halo_count(o)
                here = pl.ds(WINDOW + tokens - count, count)
                total = (dva, dka)[a]
                total[here] = total[here] + (hrv, hrk)[a][o - 1, pl.ds(0, count)].astype(F32)

    cut = vga.shape[1] // 2

    def vg_copy(j, owner, part_of):
        piece = vga.at[owner, pl.ds(part_of * cut, cut)]
        return Link(
            ledger, ("vg", j, part_of), piece, piece, (vg_s, vg_r), (j, part_of),
            at_plane(j if j < 3 else (2, 1)[part_of]),
        )

    def vg_send(j, h):
        return vg_copy(j, c if j < 3 else xor(c, (1, 2)[h]), h)

    def vg_wait(j, h):
        vg_copy(j, xor(c, j), h).wait_recv()

    act_pass(0)
    add_back(0)
    vga[c] = dva[pl.ds(WINDOW, tokens)].astype(BF16)
    if gather > 1:
        for h in (0, 1):
            vg_send(1, h).start()
            vg_send(2, 1 - h).start()
    act_ready(0)
    bits, part = pn.bits, pn.part
    counts = [upper >> (p + 1) for p in range(bits)]
    starts = [sum(counts[:p]) for p in range(bits)]
    partners = [{"tok": xor(u, 1 << p) * gather + c} for p in range(bits)]

    def bit_of(index, k):
        return lax.rem(index // (1 << k), 2)

    def block_at(phase, j, other):
        index = 0
        for k in range(phase):
            index = index + (1 << k) * bit_of(u, k)
        mine = bit_of(u, phase)
        index = index + (1 << phase) * ((1 - mine) if other else mine)
        return index + (1 << (phase + 1)) * j

    def copy_of(s, p, r):
        here, there = pl.ds(starts[p], counts[p]), pl.ds(*parts[r])
        return Link(
            ledger, ("sum", s, p, r), sbuf.at[s, here, there], rbuf.at[s, here, there],
            (rs_s, rs_r), (s, p, r), partners[p],
        )

    def product(s, index, r):
        left = act[index, pl.ds(*parts[r]), :]
        if split == gather:
            return jnp.dot(left, vga[xor(c, s)], preferred_element_type=F32)
        whole = vga[...].reshape(gather * length, part)
        return jnp.dot(left, whole, preferred_element_type=F32)

    def products(s, r):
        there = pl.ds(*parts[r])

        @pl.loop(0, counts[0])
        def _(j):
            sbuf[s, j, there] = product(s, block_at(0, j, True), r).astype(BF16)

        copy_of(s, 0, r).start()

        @pl.loop(0, counts[0])
        def _(j):
            index = block_at(0, j, False)
            acc[s, index, there] = product(s, index, r)

    def arrived(s, p, r):
        there = pl.ds(*parts[r])
        copy_of(s, p, r).wait_recv()

        @pl.loop(0, counts[p])
        def _(j):
            index = block_at(p, j, False)
            acc[s, index, there] = acc[s, index, there] + rbuf[s, starts[p] + j, there].astype(F32)

        if p + 1 < bits:
            @pl.loop(0, counts[p + 1])
            def _(j):
                index = block_at(p + 1, j, True)
                sbuf[s, starts[p + 1] + j, there] = acc[s, index, there].astype(BF16)

            copy_of(s, p + 1, r).start()

    def pass_on():
        vg_wait(1, 0)
        vg_send(3, 0).start()
        vg_wait(2, 1)
        vg_send(3, 1).start()

    last = len(parts) - 1
    if split == 1 and gather > 1:
        pass_on()
        vg_wait(1, 1)
        vg_wait(2, 0)
        vg_wait(3, 0)
        vg_wait(3, 1)
    products(0, 0)
    if split > 1:
        pass_on()
        if last:
            act_out(1)
            arrived(0, 0, 0)
        for s in (1, 2):
            vg_wait(s, s % 2)
            products(s, 0)

    outs = []
    outs.append(local_out(dqb.at[pl.ds(place * length, length)], dq_ref.at[:, cols(place, qw)], 0))
    outs[-1].start()
    for j in range(1, split):
        dq_send(j).start()

    add_back(1)
    dkb[...] = dka[pl.ds(WINDOW, tokens)].astype(BF16)

    def dk_send(j):
        other = xor(place, j)
        return Link(
            ledger, ("dk", j), dkb.at[pl.ds(other * length, length)], dk_ref.at[:, cols(place, kw)],
            (dk_s, dk_r), (j,), at_plane(j),
        )

    outs.append(local_out(dkb.at[pl.ds(place * length, length)], dk_ref.at[:, cols(place, kw)], 1))
    outs[-1].start()
    for j in range(1, split):
        dk_send(j).start()
    if last:
        vg_wait(3, 0)
        vg_wait(3, 1)
        products(3, 0)
        arrived(1, 0, 0)
        arrived(2, 0, 0)
        act_pass(1)
        act_ready(1)
        for s in range(4):
            products(s, 1)
    elif split > 1:
        vg_wait(3, 0)
        vg_wait(3, 1)
        products(3, 0)
    if split == gather:
        for j in range(gather):
            src = xor(c, j)
            outs.append(local_out(
                vga.at[src, pl.ds(c * length, length)], dv_ref.at[:, cols(src, kw)], 2 + j))
            outs[-1].start()
    else:
        outs.append(local_out(vga.at[c], dv_ref, 2))
        outs[-1].start()

    weight_in.wait()
    weight_f = wv[...].astype(F32)
    weight_sum = jnp.sum(weight_f * weight_f)

    early, late = list(range(min(3, pn.streams))), list(range(3, pn.streams))
    steps = [(s, 0, last) for s in early]
    if last:
        steps += [(s, 1, 0) for s in early] if bits > 1 else []
    steps = ([(s, 0, 0) for s in late] if last else []) + steps + [(s, 0, last) for s in late]
    for p in range(1, bits):
        steps += [(s, p, r) for r in range(len(parts)) for s in early if p > 1 or r == last]
        steps += [(s, p, r) for r in range(len(parts)) for s in late]
    for s, p, r in steps:
        arrived(s, p, r)

    row_sum = jnp.zeros((rows, 1), F32)
    for s in range(pn.streams):
        wg = acc[s, u]
        row_sum = row_sum + jnp.sum(wg * wg, axis=1, keepdims=True)
    diag = lax.broadcasted_iota(jnp.int32, (rows, rows), 0) == lax.broadcasted_iota(
        jnp.int32, (rows, rows), 1)
    row_old = jnp.sum(jnp.where(diag, rs_ref[...], 0.0), axis=1, keepdims=True)
    row_mix = DECAY_RATE * row_old + (1.0 - DECAY_RATE) * (row_sum / pn.width)
    row_mean = jnp.sum(row_mix) / rows
    scaled_sum = jnp.float32(0.0)
    for s in range(pn.streams):
        wg = acc[s, u]
        here = cols(xor(c, s), part) if split == gather else slice(0, part)
        col_new = jnp.sum(wg * wg, axis=0, keepdims=True) / rows
        col_mix = DECAY_RATE * cs_ref[:, here] + (1.0 - DECAY_RATE) * col_new
        scaled = wg / jnp.sqrt(row_mix * col_mix / row_mean)
        sc_ref[:, here] = scaled
        scaled_sum = scaled_sum + jnp.sum(scaled * scaled)

    outs.append(local_out(sc_ref, sc_out, 2 + gather))
    outs[-1].start()
    row = lax.broadcasted_iota(jnp.int32, (8, 128), 0)
    xs[0] = jnp.where(row < 4, scaled_sum, weight_sum)

    if pn.flat:
        levels = [[
            {"tok": xor(u, i) * gather + xor(c, j), "head": xor(hd, h)}
            for i in range(upper) for j in range(gather) for h in range(n_head) if i or j or h
        ]]
    else:
        levels = [near_ids, far_ids]

    def share(level, i, partner):
        slot = i + (len(near) if level else 0)
        return Link(ledger, ("share", slot), xs.at[level], xr.at[slot], (x_s, x_r), (slot,), partner)

    for level, ids in enumerate(levels):
        for i, partner in enumerate(ids):
            share(level, i, partner).start()
        total = xs[level]
        for i, partner in enumerate(ids):
            share(level, i, partner).wait_recv()
            total = total + xr[i + (len(near) if level else 0)]
        xs[level + 1] = total
    sums = xs[len(levels)]
    size = float(rows * n * pn.width * n_head)
    rms_scaled = jnp.sqrt(sums[0:1] / size)
    rms_weight = jnp.sqrt(sums[4:5] / size)
    fac_ref[...] = jnp.broadcast_to(rms_weight / jnp.maximum(1.0, rms_scaled), fac_ref.shape)

    outs.append(local_out(fac_ref, fac_out, 3 + gather))
    outs[-1].start()
    for copy in outs:
        copy.wait()
    for wait in ledger.values():
        wait()


def fused(pn, limits, query, grad, keys, values, norm, delta, act, weight, row_state, col_state):
    kw, qw = pn.kv * HD, pn.kv * pn.group * HD
    whole = WINDOW + pn.tokens
    hbm = pl.BlockSpec(memory_space=pl.ANY)
    dma = pltpu.SemaphoreType.DMA
    half, cuts = pn.half, len(pn.parts)
    peers = pn.n * pn.n_head - 1 if pn.flat else pn.gather * pn.n_head - 1 + pn.upper - 1
    reach, gather, split = pn.reach, pn.gather, pn.split
    piece = (pn.tokens, kw) if split == gather else (pn.tok_len, kw)
    return pl.pallas_call(
        functools.partial(fused_kernel, pn),
        out_shape=[
            jax.ShapeDtypeStruct(query.shape, BF16),
            jax.ShapeDtypeStruct(keys.shape, BF16),
            jax.ShapeDtypeStruct(keys.shape, BF16),
            jax.ShapeDtypeStruct((pn.rows, pn.width), F32),
            jax.ShapeDtypeStruct((8, 128), F32),
        ],
        in_specs=[hbm] * 11,
        out_specs=[hbm] * 5,
        scratch_shapes=[
            pltpu.SMEM(limits.shape, jnp.int32),
            pltpu.VMEM(norm.shape, F32),
            pltpu.VMEM(delta.shape, F32),
            pltpu.VMEM(row_state.shape, F32),
            pltpu.VMEM(col_state.shape, F32),
            pltpu.VMEM((pn.rows, pn.width), F32),
            pltpu.VMEM((8, 128), F32),
            pltpu.VMEM((pn.kv_local, 2 * pn.group, pn.tok_len), F32),
            pltpu.VMEM((pn.rows, pn.width), BF16),
            pltpu.VMEM((pn.tok_len, pn.wide) if pn.inside else act.shape[1:], BF16),
            pltpu.VMEM((pn.wide, pn.tok_len) if pn.inside else (16, 128), BF16),
            pltpu.VMEM((pn.tokens, qw), BF16),
            pltpu.VMEM((pn.tokens, qw), BF16),
            pltpu.VMEM((whole, kw), BF16),
            pltpu.VMEM((whole, kw), BF16),
            pltpu.VMEM((split, pn.kv, 2 * pn.group, pn.tok_len), F32),
            pltpu.VMEM((whole, kw), F32),
            pltpu.VMEM((whole, kw), F32),
            pltpu.VMEM((pn.tokens, qw), BF16),
            pltpu.VMEM((pn.tokens, kw), BF16),
            pltpu.VMEM((WINDOW, kw), BF16),
            pltpu.VMEM((WINDOW, kw), BF16),
            pltpu.VMEM((reach, min(pn.tokens, WINDOW), kw), BF16),
            pltpu.VMEM((reach, min(pn.tokens, WINDOW), kw), BF16),
            pltpu.VMEM((pn.upper, pn.rows, gather * pn.tok_len), BF16),
            pltpu.VMEM((gather,) + piece, BF16),
            pltpu.VMEM((pn.streams, pn.upper, pn.rows, pn.part), F32),
            pltpu.VMEM((pn.streams, pn.upper - 1, pn.rows, pn.part), BF16),
            pltpu.VMEM((pn.streams, pn.upper - 1, pn.rows, pn.part), BF16),
            pltpu.VMEM((3, 8, 128), F32),
            pltpu.VMEM((peers, 8, 128), F32),
            dma((7,)), dma((5,)), dma((5, split)), dma((5, split)), dma((2, reach)), dma((2, reach)),
            dma((2, reach)), dma((2, reach)), dma((half, cuts)),
            dma((gather, half, cuts)), dma((gather, half, cuts)),
            dma((gather, half, cuts)), dma((gather, half, cuts)),
            dma((gather, 2)), dma((gather, 2)), dma((split,)), dma((split,)),
            dma((split,)), dma((split,)), dma((4 + gather,)),
            dma((pn.streams, pn.bits, cuts)), dma((pn.streams, pn.bits, cuts)), dma((peers,)), dma((peers,)),
        ],
        compiler_params=pltpu.CompilerParams(
            collective_id=0, has_side_effects=True, vmem_limit_bytes=56 * 1024 * 1024
        ),
        name="fused",
    )(limits, query, grad, keys, values, norm, delta, act, weight, row_state, col_state)


def finish_kernel(
    dq_in, dk_in, dv_in, w_in, sc_in, fac_in, dq, dk, dv, new, upd,
    dq_v, dk_v, dv_v, w_v, sc_v, new_v, upd_v, fac_ref, in_sem, out_sem,
):
    pairs = [(dq_in, dq_v, dq), (dk_in, dk_v, dk), (dv_in, dv_v, dv)]
    loads = [pltpu.make_async_copy(fac_in, fac_ref, in_sem.at[5]), pltpu.make_async_copy(sc_in, sc_v, in_sem.at[3]), pltpu.make_async_copy(w_in, w_v, in_sem.at[4])]
    for copy in loads:
        copy.start()
    ins = [pltpu.make_async_copy(a, b, in_sem.at[i]) for i, (a, b, _) in enumerate(pairs)]
    outs = [pltpu.make_async_copy(b, d, out_sem.at[i]) for i, (_, b, d) in enumerate(pairs)]
    outs += [pltpu.make_async_copy(new_v, new, out_sem.at[3]), pltpu.make_async_copy(upd_v, upd, out_sem.at[4])]
    for copy in ins:
        copy.start()
    for copy in loads:
        copy.wait()
    update = sc_v[...] * fac_ref[0:1, 0:1]
    upd_v[...] = update
    outs[4].start()
    new_v[...] = (w_v[...].astype(F32) - LEARN_RATE * update).astype(BF16)
    outs[3].start()
    for i in range(3):
        ins[i].wait()
        outs[i].start()
    for copy in outs:
        copy.wait()


def finish(dq, dk, dv, weight, scaled, factor):
    hbm = pl.BlockSpec(memory_space=pl.ANY)
    arrays = [dq, dk, dv, weight, scaled]
    outs = [dq, dk, dv, weight, scaled]
    return pl.pallas_call(
        finish_kernel,
        out_shape=[jax.ShapeDtypeStruct(x.shape, x.dtype) for x in outs],
        in_specs=[hbm] * 6,
        out_specs=[hbm] * 5,
        scratch_shapes=[pltpu.VMEM(x.shape, x.dtype) for x in arrays + [weight, scaled, factor]]
        + [pltpu.SemaphoreType.DMA((6,)), pltpu.SemaphoreType.DMA((5,))],
        name="finish",
    )(*arrays, factor)


def shards(
    query_rows, key_rows, value_rows, out_grad, log_norm, delta_rows, window_len,
    activations, value_weight, row_state, col_state, *, n, n_head,
):
    tok_len = query_rows.shape[0]
    kv_local = key_rows.shape[1] // HD
    group = query_rows.shape[1] // key_rows.shape[1]
    rows, width = value_weight.shape
    pn = Plan(n, n_head, tok_len, kv_local, group, width, rows)

    act = activations if pn.inside else activations.T.reshape(n, rows, tok_len)
    query_grad, key_grad, value_grad, scaled, factor = fused(
        pn, window_len, query_rows, out_grad, key_rows, value_rows, log_norm.T, delta_rows.T, act,
        value_weight, row_state, col_state,
    )
    return finish(query_grad, key_grad, value_grad, value_weight, scaled, factor)


def solution(mesh):
    both = P("tok", "head")
    return jax.shard_map(
        functools.partial(shards, n=mesh.shape["tok"], n_head=mesh.shape["head"]),
        mesh=mesh,
        in_specs=(
            both, both, both, both, both, both, P("head"), P("tok", None),
            both, P("head", "tok"), both,
        ),
        out_specs=(both,) * 5,
        check_vma=False,
    )
```

```python
import functools
import math

import jax
import jax.numpy as jnp
from jax import lax
from jax.experimental import pallas as pl
from jax.experimental.pallas import tpu as pltpu
from jax.sharding import PartitionSpec as P

HD = 128
WINDOW = 1024
WINDOW_MIN = 896
SUB = 128
QUERY_SCALE = 1.0 / 12.0
LOG2E = math.log2(math.e)
DECAY_RATE = 0.9
LEARN_RATE = 0.05
F32 = jnp.float32
BF16 = jnp.bfloat16
MESH = pl.DeviceIdType.MESH


def xor(index, j):
    k = 0
    while (1 << k) <= j:
        if (j >> k) & 1:
            index = index + (1 << k) * (1 - 2 * lax.rem(index // (1 << k), 2))
        k += 1
    return index


class Plan:
    def __init__(self, n, n_head, tok_len, kv_local, group, width, rows):
        self.n, self.n_head, self.tok_len = n, n_head, tok_len
        self.kv_local, self.group = kv_local, group
        self.width, self.rows = width, rows
        self.gather = 4 if n % 4 == 0 else 1
        self.upper = n // self.gather
        self.split = self.gather if kv_local % self.gather == 0 else 1
        self.kv = kv_local // self.split
        self.tokens = self.split * tok_len
        self.blocks = n // self.split
        self.reach = min(-(-WINDOW // self.tokens), self.blocks - 1)
        self.subs = tok_len // SUB
        self.streams = self.split
        self.part = width // self.streams
        self.bits = int(math.log2(self.upper))
        self.share = 2 if n_head % 2 == 0 and self.upper % 2 == 0 else 1
        self.half = self.upper // self.share
        self.wide = self.half * self.gather * rows
        self.inside = rows % 16 == 0 and self.wide % SUB == 0
        first = rows * 5 // 7 // 16 * 16
        cut = self.inside and self.split == self.gather and first
        self.parts = [(0, first), (first, rows - first)] if cut else [(0, rows)]
        self.flat = n * n_head <= 64
        length = self.tokens if self.split == self.gather else tok_len
        first, middle = self.tokens - WINDOW, length // 2
        self.ahead = self.split == self.gather and 0 < first < middle and first % 16 == 0
        if self.ahead:
            self.pieces = [(0, first), (first, middle - first), (middle, length - middle)]
        else:
            self.pieces = [(0, middle), (middle, length - middle)]
        self.tail = len(self.pieces) - 1

    def halo_count(self, o):
        return min(self.tokens, WINDOW - (o - 1) * self.tokens)

    def halo_first(self, o):
        return max(0, WINDOW - o * self.tokens)


class Link:
    def __init__(self, ledger, key, src, dst, sems, at, device, send_if=None, recv_if=None):
        self.ledger, self.key = ledger, key
        self.send_if, self.recv_if = send_if, recv_if
        self.copy = pltpu.make_async_remote_copy(
            src_ref=src, dst_ref=dst, send_sem=sems[0].at[at], recv_sem=sems[1].at[at],
            device_id=device, device_id_type=MESH,
        )

    def guarded(self, condition, action):
        if condition is None:
            action()
        else:
            pl.when(condition)(action)

    def start(self):
        self.guarded(self.send_if, self.copy.start)
        self.ledger[self.key + ("send",)] = lambda: self.guarded(self.send_if, self.copy.wait_send)
        self.ledger[self.key + ("recv",)] = lambda: self.guarded(self.recv_if, self.copy.wait_recv)

    def wait_recv(self):
        self.ledger.pop(self.key + ("recv",))
        self.guarded(self.recv_if, self.copy.wait_recv)


def fused_kernel(
    pn,
    lim_in, q_ref, g_ref, k_ref, v_ref, ln_in, de_in, at_ref, w_ref, rs_in, cs_in,
    dq_ref, dk_ref, dv_ref, sc_out, fac_out,
    lim_ref, ln_ref, de_ref, rs_ref, cs_ref, sc_ref, fac_ref, st, wv, abuf, turned, qb, gb, kb, vb, stb, dva, dka, dqb, dkb, hsv, hsk, hrv, hrk, act, vga, acc, sbuf, rbuf,
    xs, xr,
    own_sem, small_sem, in_s, in_r, halo_s, halo_r, back_s, back_r, act_own, act_s, act_r, fwd_s, fwd_r,
    vg_s, vg_r, dq_s, dq_r, dk_s, dk_r, out_sem, rs_s, rs_r, x_s, x_r,
):
    n, n_head, gather, upper = pn.n, pn.n_head, pn.gather, pn.upper
    split, kv, length, tokens = pn.split, pn.kv, pn.tok_len, pn.tokens
    group, subs = pn.group, pn.subs
    me, hd = lax.axis_index("tok"), lax.axis_index("head")
    c, u = lax.rem(me, gather), me // gather
    place, block = lax.rem(me, split), me // split
    kw, qw = kv * HD, kv * group * HD
    rows = pn.rows
    ledger = {}

    def at_plane(j):
        return {"tok": me - c + xor(c, j)}

    near = [(j, h) for j in range(gather) for h in range(n_head) if j or h]
    far = list(range(1, upper))
    near_ids = [{"tok": me - c + xor(c, j), "head": xor(hd, h)} for j, h in near]
    far_ids = [{"tok": xor(u, i) * gather + c} for i in far]
    barrier = pltpu.get_barrier_semaphore()
    for partner in near_ids + far_ids:
        pl.semaphore_signal(barrier, inc=1, device_id=partner, device_id_type=MESH)
    lone = []
    if split == 1:
        for o in range(1, pn.reach + 1):
            lone.append(o)
            @pl.when(block + o < pn.blocks)
            def _(o=o):
                pl.semaphore_signal(barrier, inc=1, device_id={"tok": me + o}, device_id_type=MESH)

            @pl.when(block >= o)
            def _(o=o):
                pl.semaphore_signal(barrier, inc=1, device_id={"tok": me - o}, device_id_type=MESH)

    def cols(index, size):
        return pl.ds(pl.multiple_of(index * size, 128), size)

    own = [
        pltpu.make_async_copy(k_ref.at[:, cols(place, kw)], kb.at[pl.ds(WINDOW + place * length, length)], own_sem.at[0]),
        pltpu.make_async_copy(v_ref.at[:, cols(place, kw)], vb.at[pl.ds(WINDOW + place * length, length)], own_sem.at[1]),
        pltpu.make_async_copy(q_ref.at[:, cols(place, qw)], qb.at[pl.ds(place * length, length)], own_sem.at[2]),
        pltpu.make_async_copy(g_ref.at[:, cols(place, qw)], gb.at[pl.ds(place * length, length)], own_sem.at[3]),
        pltpu.make_async_copy(st.at[pl.ds(place * kv, kv)], stb.at[place], own_sem.at[4]),
    ]
    half = pn.half
    low = lax.rem(hd, pn.share) * half
    if pn.inside:
        load = pltpu.make_async_copy(
            at_ref.at[:, cols(lax.rem(hd, pn.share), pn.wide)], abuf, own_sem.at[5]
        )
        load.start()
    for copy in own[:4]:
        copy.start()
    small = [
        pltpu.make_async_copy(src, dst, small_sem.at[i])
        for i, (src, dst) in enumerate(
            [(ln_in, ln_ref), (de_in, de_ref), (lim_in, lim_ref), (rs_in, rs_ref), (cs_in, cs_ref)])
    ]
    for copy in small:
        copy.start()
    weight_in = pltpu.make_async_copy(w_ref, wv, own_sem.at[6])
    weight_in.start()

    pl.semaphore_wait(barrier, len(near_ids) + len(far_ids))
    for o in lone:
        @pl.when(block + o < pn.blocks)
        def _():
            pl.semaphore_wait(barrier, 1)

        @pl.when(block >= o)
        def _():
            pl.semaphore_wait(barrier, 1)

    def exchange(a, j):
        other = xor(place, j)
        src, dst = [
            (k_ref.at[:, cols(other, kw)], kb.at[pl.ds(WINDOW + place * length, length)]),
            (v_ref.at[:, cols(other, kw)], vb.at[pl.ds(WINDOW + place * length, length)]),
            (q_ref.at[:, cols(other, qw)], qb.at[pl.ds(place * length, length)]),
            (g_ref.at[:, cols(other, qw)], gb.at[pl.ds(place * length, length)]),
            (st.at[pl.ds(other * kv, kv)], stb.at[place]),
        ][a]
        return Link(ledger, ("in", a, j), src, dst, (in_s, in_r), (a, j), at_plane(j))

    for a in (0, 1, 2, 3):
        for j in range(1, split):
            exchange(a, j).start()
    for copy in small:
        copy.wait()
    for i, ref in enumerate((ln_ref, de_ref)):
        stat = ref[...]
        if i == 0:
            stat = stat * LOG2E
        for k in range(pn.kv_local):
            st[k, i * group : (i + 1) * group] = stat[k * group : (k + 1) * group]
    own[4].start()
    for j in range(1, split):
        exchange(4, j).start()
    dva[...] = jnp.zeros_like(dva)
    dka[...] = jnp.zeros_like(dka)

    def turn(first, last):
        @pl.loop(first, last)
        def _(i):
            here = pl.ds(pl.multiple_of(i * SUB, SUB), SUB)
            turned[here, :] = abuf[:, here].T

    steps = pn.wide // SUB
    if pn.inside:
        load.wait()

    def halo(a, o):
        count, first = pn.halo_count(o), pn.halo_first(o)
        buf = (kb, vb)[a]
        return Link(
            ledger, ("halo", a, o), buf.at[pl.ds(WINDOW + tokens - count, count)],
            buf.at[pl.ds(first, count)], (halo_s, halo_r), (a, o - 1), {"tok": me + o * split},
            block + o < pn.blocks, block >= o,
        )

    for a in (0, 1):
        own[a].wait()
        for j in range(1, split):
            exchange(a, j).wait_recv()
        for o in range(1, pn.reach + 1):
            halo(a, o).start()

            @pl.when(block < o)
            def _(a=a, o=o):
                buf = (kb, vb)[a]
                here = pl.ds(pn.halo_first(o), pn.halo_count(o))
                buf[here] = jnp.zeros((pn.halo_count(o), kw), BF16)
    if pn.reach * tokens < WINDOW:
        rest = WINDOW - pn.reach * tokens
        for buf in (kb, vb):
            buf[pl.ds(0, rest)] = jnp.zeros((rest, kw), BF16)

    if pn.inside:
        turn(0, steps)

    parts = pn.parts

    def act_piece(i, owner, r):
        first, size = parts[r]
        if pn.inside:
            here = pl.multiple_of((i * gather + owner) * rows + first, 16)
            return turned.at[pl.ds(here, size)]
        return at_ref.at[(low + i) * gather + owner]

    act_mine = [
        pltpu.make_async_copy(
            act_piece(i, c, r), act.at[low + i, pl.ds(*parts[r]), cols(c, length)], act_own.at[i, r])
        for i in range(half) for r in range(len(parts))
    ]
    for copy in act_mine:
        copy.start()

    def act_send(j, i, r):
        return Link(
            ledger, ("act", j, i, r), act_piece(i, xor(c, j), r),
            act.at[low + i, pl.ds(*parts[r]), cols(c, length)],
            (act_s, act_r), (j, i, r), at_plane(j),
        )

    def act_forward(j, i, r, start=low):
        piece = act.at[start + i, pl.ds(*parts[r]), cols(xor(c, j), length)]
        return Link(
            ledger, ("forward", j, i, r), piece, piece, (fwd_s, fwd_r), (j, i, r),
            {"head": xor(hd, 1)})

    order = [(j, i) for i in range(half) for j in (1, 2, 3)]
    if gather == 1:
        order = []

    def act_out(r):
        for j, i in order:
            act_send(j, i, r).start()

    def act_pass(r):
        for j, i in order:
            act_send(j, i, r).wait_recv()
            if pn.share == 2:
                act_forward(j, i, r).start()

    def act_ready(r):
        if pn.share == 2:
            for j, i in [(0, i) for i in range(half)] + order:
                act_forward(j, i, r, half - low).wait_recv()

    act_out(0)
    for a in (0, 1):
        for o in range(1, pn.reach + 1):
            halo(a, o).wait_recv()

    seen = WINDOW + SUB
    chunk = seen // 3
    lanes = group * SUB

    def unit(b, kh, sub):
        start = pl.multiple_of(b * length + sub * SUB, SUB)
        rows_q = pl.ds(start, SUB)
        head = kh * group * HD
        query = jnp.concatenate(
            [qb[rows_q, head + m * HD : head + (m + 1) * HD] for m in range(group)], axis=0
        )
        grad = jnp.concatenate(
            [gb[rows_q, head + m * HD : head + (m + 1) * HD] for m in range(group)], axis=0
        )
        lane_q = pl.ds(pl.multiple_of(sub * SUB, SUB), SUB)
        norm, delta = [
            jnp.concatenate([stb[b, kh, i * group + m : i * group + m + 1, lane_q] for m in range(group)], axis=1)
            for i in range(2)
        ]
        total = jnp.zeros((lanes, HD), F32)
        for piece in range(3):
            here = pl.ds(pl.multiple_of(start + piece * chunk, SUB), chunk)
            keys = kb[here, kh * HD : (kh + 1) * HD]
            values = vb[here, kh * HD : (kh + 1) * HD]
            scores = lax.dot_general(
                keys, query, (((1,), (1,)), ((), ())), preferred_element_type=F32
            )
            prob = jnp.exp2(scores * (QUERY_SCALE * LOG2E) - norm)
            if piece == 0:
                edge = WINDOW - WINDOW_MIN + SUB
                row = lax.broadcasted_iota(jnp.int32, (edge, lanes), 0)
                lane = lax.broadcasted_iota(jnp.int32, (edge, lanes), 1)
                limit = jnp.full((edge, lanes), 0, jnp.int32)
                for m in range(group):
                    limit = jnp.where(
                        lane // SUB == m, lim_ref[(place * kv + kh) * group + m], limit
                    )
                visible = WINDOW + lax.rem(lane, SUB) - row < limit
                prob = jnp.concatenate(
                    [jnp.where(visible, prob[:edge], 0.0), prob[edge:]], axis=0
                )
            if piece == 2:
                row = lax.broadcasted_iota(jnp.int32, (SUB, lanes), 0)
                lane = lax.broadcasted_iota(jnp.int32, (SUB, lanes), 1)
                visible = row <= lax.rem(lane, SUB)
                prob = jnp.concatenate(
                    [prob[: chunk - SUB], jnp.where(visible, prob[chunk - SUB :], 0.0)], axis=0
                )
            dva[here, kh * HD : (kh + 1) * HD] += jnp.dot(
                prob.astype(BF16), grad, preferred_element_type=F32
            )
            dprob = lax.dot_general(
                values, grad, (((1,), (1,)), ((), ())), preferred_element_type=F32
            )
            dscore = (QUERY_SCALE * prob * (dprob - delta)).astype(BF16)
            dka[here, kh * HD : (kh + 1) * HD] += jnp.dot(
                dscore, query, preferred_element_type=F32
            )
            total = total + lax.dot_general(
                dscore, keys, (((0,), (0,)), ((), ())), preferred_element_type=F32
            )
        low_q = total.astype(BF16)
        for m in range(group):
            dqb[rows_q, head + m * HD : head + (m + 1) * HD] = low_q[m * SUB : (m + 1) * SUB]

    def dq_send(j):
        other = xor(place, j)
        src = dqb.at[pl.ds(other * length, length)]
        return Link(
            ledger, ("dq", j), src, dq_ref.at[:, cols(place, qw)], (dq_s, dq_r), (j,), at_plane(j))

    def local_out(src, dst, i):
        return pltpu.make_async_copy(src, dst, out_sem.at[i])

    for j in range(split):
        b = xor(place, j)
        for a in (2, 3, 4):
            if j:
                exchange(a, j).wait_recv()
            else:
                own[a].wait()
        for kh in range(kv):
            @pl.loop(0, subs)
            def _(sub, b=b, kh=kh):
                unit(b, kh, sub)

        if j == 0:
            for copy in act_mine:
                copy.wait()
            if pn.share == 2:
                for r in range(len(parts)):
                    for i in range(half):
                        act_forward(0, i, r).start()

    def back(a, o):
        count, first = pn.halo_count(o), pn.halo_first(o)
        return Link(
            ledger, ("back", a, o), (hsv, hsk)[a].at[pl.ds(first, count)],
            (hrv, hrk)[a].at[o - 1, pl.ds(0, count)], (back_s, back_r), (a, o - 1),
            {"tok": me - o * split}, block >= o, block + o < pn.blocks,
        )

    tail = pn.tail

    def vg_copy(j, owner, h):
        piece = vga.at[owner, pl.ds(*pn.pieces[h])]
        return Link(
            ledger, ("vg", j, h), piece, piece, (vg_s, vg_r), (j, h),
            at_plane(j if j < 3 else (1 if h == tail else 2)),
        )

    def vg_send(j, h):
        return vg_copy(j, c if j < 3 else xor(c, 2 if h == tail else 1), h)

    def vg_wait(j, h):
        vg_copy(j, xor(c, j), h).wait_recv()

    for a in (0, 1):
        (hsv, hsk)[a][...] = (dva, dka)[a][pl.ds(0, WINDOW)].astype(BF16)
        for o in range(1, pn.reach + 1):
            back(a, o).start()
        if a == 0 and pn.ahead:
            first = pn.pieces[0][1]
            vga[c, pl.ds(0, first)] = dva[pl.ds(WINDOW, first)].astype(BF16)
            for j in (1, 2):
                vg_send(j, 0).start()

    def add_back(a):
        for o in range(1, pn.reach + 1):
            back(a, o).wait_recv()

            @pl.when(block + o < pn.blocks)
            def _(o=o):
                count = pn.halo_count(o)
                here = pl.ds(WINDOW + tokens - count, count)
                total = (dva, dka)[a]
                total[here] = total[here] + (hrv, hrk)[a][o - 1, pl.ds(0, count)].astype(F32)

    act_pass(0)
    add_back(0)
    ready = pn.pieces[0][1] if pn.ahead else 0
    vga[c, pl.ds(ready, tokens - ready)] = dva[pl.ds(WINDOW + ready, tokens - ready)].astype(BF16)
    rest = list(range(1 if pn.ahead else 0, len(pn.pieces)))
    if gather > 1:
        for h, g in zip(rest, rest[::-1]):
            vg_send(1, h).start()
            vg_send(2, g).start()
    act_ready(0)
    bits, part = pn.bits, pn.part
    counts = [upper >> (p + 1) for p in range(bits)]
    starts = [sum(counts[:p]) for p in range(bits)]
    partners = [{"tok": xor(u, 1 << p) * gather + c} for p in range(bits)]

    def bit_of(index, k):
        return lax.rem(index // (1 << k), 2)

    def block_at(phase, j, other):
        index = 0
        for k in range(phase):
            index = index + (1 << k) * bit_of(u, k)
        mine = bit_of(u, phase)
        index = index + (1 << phase) * ((1 - mine) if other else mine)
        return index + (1 << (phase + 1)) * j

    def copy_of(s, p, r):
        here, there = pl.ds(starts[p], counts[p]), pl.ds(*parts[r])
        return Link(
            ledger, ("sum", s, p, r), sbuf.at[s, here, there], rbuf.at[s, here, there],
            (rs_s, rs_r), (s, p, r), partners[p],
        )

    def product(s, index, r):
        left = act[index, pl.ds(*parts[r]), :]
        if split == gather:
            return jnp.dot(left, vga[xor(c, s)], preferred_element_type=F32)
        whole = vga[...].reshape(gather * length, part)
        return jnp.dot(left, whole, preferred_element_type=F32)

    def products(s, r):
        there = pl.ds(*parts[r])

        @pl.loop(0, counts[0])
        def _(j):
            sbuf[s, j, there] = product(s, block_at(0, j, True), r).astype(BF16)

        copy_of(s, 0, r).start()

        @pl.loop(0, counts[0])
        def _(j):
            index = block_at(0, j, False)
            acc[s, index, there] = product(s, index, r)

    def arrived(s, p, r):
        there = pl.ds(*parts[r])
        copy_of(s, p, r).wait_recv()

        @pl.loop(0, counts[p])
        def _(j):
            index = block_at(p, j, False)
            acc[s, index, there] = acc[s, index, there] + rbuf[s, starts[p] + j, there].astype(F32)

        if p + 1 < bits:
            @pl.loop(0, counts[p + 1])
            def _(j):
                index = block_at(p + 1, j, True)
                sbuf[s, starts[p + 1] + j, there] = acc[s, index, there].astype(BF16)

            copy_of(s, p + 1, r).start()

    def pass_on():
        for h in range(tail - 1):
            vg_wait(1, h)
            vg_send(3, h).start()
        vg_wait(2, tail)
        vg_send(3, tail).start()
        vg_wait(1, tail - 1)
        vg_send(3, tail - 1).start()

    def vg_rest(j):
        for h in range(tail + 1):
            if j == 3 or (j == 1 and h == tail) or (j == 2 and h != tail):
                vg_wait(j, h)

    last = len(parts) - 1
    if split == 1 and gather > 1:
        pass_on()
        for j in (1, 2, 3):
            vg_rest(j)
    products(0, 0)
    if split > 1:
        pass_on()
        if last:
            act_out(1)
            arrived(0, 0, 0)
        for s in (1, 2):
            vg_rest(s)
            products(s, 0)

    outs = []
    outs.append(local_out(dqb.at[pl.ds(place * length, length)], dq_ref.at[:, cols(place, qw)], 0))
    outs[-1].start()

    add_back(1)
    dkb[...] = dka[pl.ds(WINDOW, tokens)].astype(BF16)

    def dk_send(j):
        other = xor(place, j)
        return Link(
            ledger, ("dk", j), dkb.at[pl.ds(other * length, length)], dk_ref.at[:, cols(place, kw)],
            (dk_s, dk_r), (j,), at_plane(j),
        )

    outs.append(local_out(dkb.at[pl.ds(place * length, length)], dk_ref.at[:, cols(place, kw)], 1))
    outs[-1].start()
    if last:
        vg_rest(3)
        products(3, 0)
        arrived(1, 0, 0)
        arrived(2, 0, 0)
        act_pass(1)
        act_ready(1)
        for s in range(4):
            products(s, 1)
    elif split > 1:
        vg_rest(3)
        products(3, 0)
    for j in range(1, split):
        dq_send(j).start()
    for j in range(1, split):
        dk_send(j).start()
    if split == gather:
        for j in range(gather):
            src = xor(c, j)
            outs.append(local_out(
                vga.at[src, pl.ds(c * length, length)], dv_ref.at[:, cols(src, kw)], 2 + j))
            outs[-1].start()
    else:
        outs.append(local_out(vga.at[c], dv_ref, 2))
        outs[-1].start()

    weight_in.wait()
    weight_f = wv[...].astype(F32)
    weight_sum = jnp.sum(weight_f * weight_f)

    early, late = list(range(min(3, pn.streams))), list(range(3, pn.streams))
    steps = [(s, 0, last) for s in early]
    if last:
        steps += [(s, 1, 0) for s in early] if bits > 1 else []
    steps = ([(s, 0, 0) for s in late] if last else []) + steps + [(s, 0, last) for s in late]
    for p in range(1, bits):
        steps += [(s, p, r) for r in range(len(parts)) for s in early if p > 1 or r == last]
        steps += [(s, p, r) for r in range(len(parts)) for s in late]
    for s, p, r in steps:
        arrived(s, p, r)

    row_sum = jnp.zeros((rows, 1), F32)
    for s in range(pn.streams):
        wg = acc[s, u]
        row_sum = row_sum + jnp.sum(wg * wg, axis=1, keepdims=True)
    diag = lax.broadcasted_iota(jnp.int32, (rows, rows), 0) == lax.broadcasted_iota(
        jnp.int32, (rows, rows), 1)
    row_old = jnp.sum(jnp.where(diag, rs_ref[...], 0.0), axis=1, keepdims=True)
    row_mix = DECAY_RATE * row_old + (1.0 - DECAY_RATE) * (row_sum / pn.width)
    row_mean = jnp.sum(row_mix) / rows
    scaled_sum = jnp.float32(0.0)
    for s in range(pn.streams):
        wg = acc[s, u]
        here = cols(xor(c, s), part) if split == gather else slice(0, part)
        col_new = jnp.sum(wg * wg, axis=0, keepdims=True) / rows
        col_mix = DECAY_RATE * cs_ref[:, here] + (1.0 - DECAY_RATE) * col_new
        scaled = wg / jnp.sqrt(row_mix * col_mix / row_mean)
        sc_ref[:, here] = scaled
        scaled_sum = scaled_sum + jnp.sum(scaled * scaled)

    outs.append(local_out(sc_ref, sc_out, 2 + gather))
    outs[-1].start()
    row = lax.broadcasted_iota(jnp.int32, (8, 128), 0)
    xs[0] = jnp.where(row < 4, scaled_sum, weight_sum)

    if pn.flat:
        levels = [[
            {"tok": xor(u, i) * gather + xor(c, j), "head": xor(hd, h)}
            for i in range(upper) for j in range(gather) for h in range(n_head) if i or j or h
        ]]
    else:
        levels = [near_ids, far_ids]

    def share(level, i, partner):
        slot = i + (len(near) if level else 0)
        return Link(ledger, ("share", slot), xs.at[level], xr.at[slot], (x_s, x_r), (slot,), partner)

    for level, ids in enumerate(levels):
        for i, partner in enumerate(ids):
            share(level, i, partner).start()
        total = xs[level]
        for i, partner in enumerate(ids):
            share(level, i, partner).wait_recv()
            total = total + xr[i + (len(near) if level else 0)]
        xs[level + 1] = total
    sums = xs[len(levels)]
    size = float(rows * n * pn.width * n_head)
    rms_scaled = jnp.sqrt(sums[0:1] / size)
    rms_weight = jnp.sqrt(sums[4:5] / size)
    fac_ref[...] = jnp.broadcast_to(rms_weight / jnp.maximum(1.0, rms_scaled), fac_ref.shape)

    outs.append(local_out(fac_ref, fac_out, 3 + gather))
    outs[-1].start()
    for copy in outs:
        copy.wait()
    for wait in ledger.values():
        wait()


def fused(pn, limits, query, grad, keys, values, norm, delta, act, weight, row_state, col_state):
    kw, qw = pn.kv * HD, pn.kv * pn.group * HD
    whole = WINDOW + pn.tokens
    hbm = pl.BlockSpec(memory_space=pl.ANY)
    dma = pltpu.SemaphoreType.DMA
    half, cuts = pn.half, len(pn.parts)
    peers = pn.n * pn.n_head - 1 if pn.flat else pn.gather * pn.n_head - 1 + pn.upper - 1
    reach, gather, split = pn.reach, pn.gather, pn.split
    piece = (pn.tokens, kw) if split == gather else (pn.tok_len, kw)
    return pl.pallas_call(
        functools.partial(fused_kernel, pn),
        out_shape=[
            jax.ShapeDtypeStruct(query.shape, BF16),
            jax.ShapeDtypeStruct(keys.shape, BF16),
            jax.ShapeDtypeStruct(keys.shape, BF16),
            jax.ShapeDtypeStruct((pn.rows, pn.width), F32),
            jax.ShapeDtypeStruct((8, 128), F32),
        ],
        in_specs=[hbm] * 11,
        out_specs=[hbm] * 5,
        scratch_shapes=[
            pltpu.SMEM(limits.shape, jnp.int32),
            pltpu.VMEM(norm.shape, F32),
            pltpu.VMEM(delta.shape, F32),
            pltpu.VMEM(row_state.shape, F32),
            pltpu.VMEM(col_state.shape, F32),
            pltpu.VMEM((pn.rows, pn.width), F32),
            pltpu.VMEM((8, 128), F32),
            pltpu.VMEM((pn.kv_local, 2 * pn.group, pn.tok_len), F32),
            pltpu.VMEM((pn.rows, pn.width), BF16),
            pltpu.VMEM((pn.tok_len, pn.wide) if pn.inside else act.shape[1:], BF16),
            pltpu.VMEM((pn.wide, pn.tok_len) if pn.inside else (16, 128), BF16),
            pltpu.VMEM((pn.tokens, qw), BF16),
            pltpu.VMEM((pn.tokens, qw), BF16),
            pltpu.VMEM((whole, kw), BF16),
            pltpu.VMEM((whole, kw), BF16),
            pltpu.VMEM((split, pn.kv, 2 * pn.group, pn.tok_len), F32),
            pltpu.VMEM((whole, kw), F32),
            pltpu.VMEM((whole, kw), F32),
            pltpu.VMEM((pn.tokens, qw), BF16),
            pltpu.VMEM((pn.tokens, kw), BF16),
            pltpu.VMEM((WINDOW, kw), BF16),
            pltpu.VMEM((WINDOW, kw), BF16),
            pltpu.VMEM((reach, min(pn.tokens, WINDOW), kw), BF16),
            pltpu.VMEM((reach, min(pn.tokens, WINDOW), kw), BF16),
            pltpu.VMEM((pn.upper, pn.rows, gather * pn.tok_len), BF16),
            pltpu.VMEM((gather,) + piece, BF16),
            pltpu.VMEM((pn.streams, pn.upper, pn.rows, pn.part), F32),
            pltpu.VMEM((pn.streams, pn.upper - 1, pn.rows, pn.part), BF16),
            pltpu.VMEM((pn.streams, pn.upper - 1, pn.rows, pn.part), BF16),
            pltpu.VMEM((3, 8, 128), F32),
            pltpu.VMEM((peers, 8, 128), F32),
            dma((7,)), dma((5,)), dma((5, split)), dma((5, split)), dma((2, reach)), dma((2, reach)),
            dma((2, reach)), dma((2, reach)), dma((half, cuts)),
            dma((gather, half, cuts)), dma((gather, half, cuts)),
            dma((gather, half, cuts)), dma((gather, half, cuts)),
            dma((gather, len(pn.pieces))), dma((gather, len(pn.pieces))), dma((split,)), dma((split,)),
            dma((split,)), dma((split,)), dma((4 + gather,)),
            dma((pn.streams, pn.bits, cuts)), dma((pn.streams, pn.bits, cuts)), dma((peers,)), dma((peers,)),
        ],
        compiler_params=pltpu.CompilerParams(
            collective_id=0, has_side_effects=True, vmem_limit_bytes=56 * 1024 * 1024
        ),
        name="fused",
    )(limits, query, grad, keys, values, norm, delta, act, weight, row_state, col_state)


def finish_kernel(
    dq_in, dk_in, dv_in, w_in, sc_in, fac_in, dq, dk, dv, new, upd,
    dq_v, dk_v, dv_v, w_v, sc_v, new_v, upd_v, fac_ref, in_sem, out_sem,
):
    pairs = [(dq_in, dq_v, dq), (dk_in, dk_v, dk), (dv_in, dv_v, dv)]
    loads = [pltpu.make_async_copy(fac_in, fac_ref, in_sem.at[5]), pltpu.make_async_copy(sc_in, sc_v, in_sem.at[3]), pltpu.make_async_copy(w_in, w_v, in_sem.at[4])]
    for copy in loads:
        copy.start()
    ins = [pltpu.make_async_copy(a, b, in_sem.at[i]) for i, (a, b, _) in enumerate(pairs)]
    outs = [pltpu.make_async_copy(b, d, out_sem.at[i]) for i, (_, b, d) in enumerate(pairs)]
    outs += [pltpu.make_async_copy(new_v, new, out_sem.at[3]), pltpu.make_async_copy(upd_v, upd, out_sem.at[4])]
    for copy in ins:
        copy.start()
    for copy in loads:
        copy.wait()
    update = sc_v[...] * fac_ref[0:1, 0:1]
    upd_v[...] = update
    outs[4].start()
    new_v[...] = (w_v[...].astype(F32) - LEARN_RATE * update).astype(BF16)
    outs[3].start()
    for i in range(3):
        ins[i].wait()
        outs[i].start()
    for copy in outs:
        copy.wait()


def finish(dq, dk, dv, weight, scaled, factor):
    hbm = pl.BlockSpec(memory_space=pl.ANY)
    arrays = [dq, dk, dv, weight, scaled]
    outs = [dq, dk, dv, weight, scaled]
    return pl.pallas_call(
        finish_kernel,
        out_shape=[jax.ShapeDtypeStruct(x.shape, x.dtype) for x in outs],
        in_specs=[hbm] * 6,
        out_specs=[hbm] * 5,
        scratch_shapes=[pltpu.VMEM(x.shape, x.dtype) for x in arrays + [weight, scaled, factor]]
        + [pltpu.SemaphoreType.DMA((6,)), pltpu.SemaphoreType.DMA((5,))],
        name="finish",
    )(*arrays, factor)


def shards(
    query_rows, key_rows, value_rows, out_grad, log_norm, delta_rows, window_len,
    activations, value_weight, row_state, col_state, *, n, n_head,
):
    tok_len = query_rows.shape[0]
    kv_local = key_rows.shape[1] // HD
    group = query_rows.shape[1] // key_rows.shape[1]
    rows, width = value_weight.shape
    pn = Plan(n, n_head, tok_len, kv_local, group, width, rows)

    act = activations if pn.inside else activations.T.reshape(n, rows, tok_len)
    query_grad, key_grad, value_grad, scaled, factor = fused(
        pn, window_len, query_rows, out_grad, key_rows, value_rows, log_norm.T, delta_rows.T, act,
        value_weight, row_state, col_state,
    )
    return finish(query_grad, key_grad, value_grad, value_weight, scaled, factor)


def solution(mesh):
    both = P("tok", "head")
    return jax.shard_map(
        functools.partial(shards, n=mesh.shape["tok"], n_head=mesh.shape["head"]),
        mesh=mesh,
        in_specs=(
            both, both, both, both, both, both, P("head"), P("tok", None),
            both, P("head", "tok"), both,
        ),
        out_specs=(both,) * 5,
        check_vma=False,
    )
```

```python
import functools
import math

import jax
import jax.numpy as jnp
from jax import lax
from jax.experimental import pallas as pl
from jax.experimental.pallas import tpu as pltpu
from jax.sharding import PartitionSpec as P

HD = 128
WINDOW = 1024
WINDOW_MIN = 896
SUB = 128
QUERY_SCALE = 1.0 / 12.0
LOG2E = math.log2(math.e)
DECAY_RATE = 0.9
LEARN_RATE = 0.05
F32 = jnp.float32
BF16 = jnp.bfloat16
MESH = pl.DeviceIdType.MESH


def xor(index, j):
    k = 0
    while (1 << k) <= j:
        if (j >> k) & 1:
            index = index + (1 << k) * (1 - 2 * lax.rem(index // (1 << k), 2))
        k += 1
    return index


class Plan:
    def __init__(self, n, n_head, tok_len, kv_local, group, width, rows):
        self.n, self.n_head, self.tok_len = n, n_head, tok_len
        self.kv_local, self.group = kv_local, group
        self.width, self.rows = width, rows
        self.gather = 4 if n % 4 == 0 else 1
        self.upper = n // self.gather
        self.split = self.gather if kv_local % self.gather == 0 else 1
        self.kv = kv_local // self.split
        self.tokens = self.split * tok_len
        self.blocks = n // self.split
        self.reach = min(-(-WINDOW // self.tokens), self.blocks - 1)
        self.subs = tok_len // SUB
        self.streams = self.split
        self.part = width // self.streams
        self.bits = int(math.log2(self.upper))
        self.share = 2 if n_head % 2 == 0 and self.upper % 2 == 0 else 1
        self.half = self.upper // self.share
        self.wide = self.half * self.gather * rows
        self.inside = rows % 16 == 0 and self.wide % SUB == 0
        first = rows * 5 // 7 // 16 * 16
        cut = self.inside and self.split == self.gather and first
        self.parts = [(0, first), (first, rows - first)] if cut else [(0, rows)]
        self.flat = n * n_head <= 64
        length = self.tokens if self.split == self.gather else tok_len
        first, middle = self.tokens - WINDOW, length // 2
        self.ahead = self.split == self.gather and 0 < first < middle and first % 16 == 0
        if self.ahead:
            self.pieces = [(0, first), (first, middle - first), (middle, length - middle)]
        else:
            self.pieces = [(0, middle), (middle, length - middle)]
        self.tail = len(self.pieces) - 1

    def halo_count(self, o):
        return min(self.tokens, WINDOW - (o - 1) * self.tokens)

    def halo_first(self, o):
        return max(0, WINDOW - o * self.tokens)


class Link:
    def __init__(self, ledger, key, src, dst, sems, at, device, send_if=None, recv_if=None):
        self.ledger, self.key = ledger, key
        self.send_if, self.recv_if = send_if, recv_if
        self.copy = pltpu.make_async_remote_copy(
            src_ref=src, dst_ref=dst, send_sem=sems[0].at[at], recv_sem=sems[1].at[at],
            device_id=device, device_id_type=MESH,
        )

    def guarded(self, condition, action):
        if condition is None:
            action()
        else:
            pl.when(condition)(action)

    def start(self):
        self.guarded(self.send_if, self.copy.start)
        self.ledger[self.key + ("send",)] = lambda: self.guarded(self.send_if, self.copy.wait_send)
        self.ledger[self.key + ("recv",)] = lambda: self.guarded(self.recv_if, self.copy.wait_recv)

    def wait_recv(self):
        self.ledger.pop(self.key + ("recv",))
        self.guarded(self.recv_if, self.copy.wait_recv)


def fused_kernel(
    pn,
    lim_in, q_ref, g_ref, k_ref, v_ref, ln_in, de_in, at_ref, w_ref, rs_in, cs_in,
    dq_ref, dk_ref, dv_ref, sc_out, fac_out,
    lim_ref, ln_ref, de_ref, rs_ref, cs_ref, sc_ref, fac_ref, st, wv, abuf, turned, qb, gb, kb, vb, stb, dva, dka, dqb, dkb, hsv, hsk, hrv, hrk, act, vga, acc, sbuf, rbuf,
    xs, xr,
    own_sem, small_sem, in_s, in_r, halo_s, halo_r, back_s, back_r, act_own, act_s, act_r, fwd_s, fwd_r,
    vg_s, vg_r, dq_s, dq_r, dk_s, dk_r, out_sem, rs_s, rs_r, x_s, x_r,
):
    n, n_head, gather, upper = pn.n, pn.n_head, pn.gather, pn.upper
    split, kv, length, tokens = pn.split, pn.kv, pn.tok_len, pn.tokens
    group, subs = pn.group, pn.subs
    me, hd = lax.axis_index("tok"), lax.axis_index("head")
    c, u = lax.rem(me, gather), me // gather
    place, block = lax.rem(me, split), me // split
    kw, qw = kv * HD, kv * group * HD
    rows = pn.rows
    ledger = {}

    def at_plane(j):
        return {"tok": me - c + xor(c, j)}

    near = [(j, h) for j in range(gather) for h in range(n_head) if j or h]
    far = list(range(1, upper))
    near_ids = [{"tok": me - c + xor(c, j), "head": xor(hd, h)} for j, h in near]
    far_ids = [{"tok": xor(u, i) * gather + c} for i in far]
    barrier = pltpu.get_barrier_semaphore()
    for partner in near_ids + far_ids:
        pl.semaphore_signal(barrier, inc=1, device_id=partner, device_id_type=MESH)
    lone = []
    if split == 1:
        for o in range(1, pn.reach + 1):
            lone.append(o)
            @pl.when(block + o < pn.blocks)
            def _(o=o):
                pl.semaphore_signal(barrier, inc=1, device_id={"tok": me + o}, device_id_type=MESH)

            @pl.when(block >= o)
            def _(o=o):
                pl.semaphore_signal(barrier, inc=1, device_id={"tok": me - o}, device_id_type=MESH)

    def cols(index, size):
        return pl.ds(pl.multiple_of(index * size, 128), size)

    own = [
        pltpu.make_async_copy(k_ref.at[:, cols(place, kw)], kb.at[pl.ds(WINDOW + place * length, length)], own_sem.at[0]),
        pltpu.make_async_copy(v_ref.at[:, cols(place, kw)], vb.at[pl.ds(WINDOW + place * length, length)], own_sem.at[1]),
        pltpu.make_async_copy(q_ref.at[:, cols(place, qw)], qb.at[pl.ds(place * length, length)], own_sem.at[2]),
        pltpu.make_async_copy(g_ref.at[:, cols(place, qw)], gb.at[pl.ds(place * length, length)], own_sem.at[3]),
        pltpu.make_async_copy(st.at[pl.ds(place * kv, kv)], stb.at[place], own_sem.at[4]),
    ]
    half = pn.half
    low = lax.rem(hd, pn.share) * half
    if pn.inside:
        load = pltpu.make_async_copy(
            at_ref.at[:, cols(lax.rem(hd, pn.share), pn.wide)], abuf, own_sem.at[5]
        )
        load.start()
    for copy in own[:4]:
        copy.start()
    small = [
        pltpu.make_async_copy(src, dst, small_sem.at[i])
        for i, (src, dst) in enumerate(
            [(ln_in, ln_ref), (de_in, de_ref), (lim_in, lim_ref), (rs_in, rs_ref), (cs_in, cs_ref)])
    ]
    for copy in small:
        copy.start()
    weight_in = pltpu.make_async_copy(w_ref, wv, own_sem.at[6])
    weight_in.start()

    pl.semaphore_wait(barrier, len(near_ids) + len(far_ids))
    for o in lone:
        @pl.when(block + o < pn.blocks)
        def _():
            pl.semaphore_wait(barrier, 1)

        @pl.when(block >= o)
        def _():
            pl.semaphore_wait(barrier, 1)

    def exchange(a, j):
        other = xor(place, j)
        src, dst = [
            (k_ref.at[:, cols(other, kw)], kb.at[pl.ds(WINDOW + place * length, length)]),
            (v_ref.at[:, cols(other, kw)], vb.at[pl.ds(WINDOW + place * length, length)]),
            (q_ref.at[:, cols(other, qw)], qb.at[pl.ds(place * length, length)]),
            (g_ref.at[:, cols(other, qw)], gb.at[pl.ds(place * length, length)]),
            (st.at[pl.ds(other * kv, kv)], stb.at[place]),
        ][a]
        return Link(ledger, ("in", a, j), src, dst, (in_s, in_r), (a, j), at_plane(j))

    for a in (0, 1, 2, 3):
        for j in range(1, split):
            exchange(a, j).start()
    for copy in small:
        copy.wait()
    for i, ref in enumerate((ln_ref, de_ref)):
        stat = ref[...]
        if i == 0:
            stat = stat * LOG2E
        for k in range(pn.kv_local):
            st[k, i * group : (i + 1) * group] = stat[k * group : (k + 1) * group]
    own[4].start()
    for j in range(1, split):
        exchange(4, j).start()
    dva[...] = jnp.zeros_like(dva)
    dka[...] = jnp.zeros_like(dka)

    def turn(first, last):
        @pl.loop(first, last)
        def _(i):
            here = pl.ds(pl.multiple_of(i * SUB, SUB), SUB)
            turned[here, :] = abuf[:, here].T

    steps = pn.wide // SUB
    if pn.inside:
        load.wait()

    def halo(a, o):
        count, first = pn.halo_count(o), pn.halo_first(o)
        buf = (kb, vb)[a]
        return Link(
            ledger, ("halo", a, o), buf.at[pl.ds(WINDOW + tokens - count, count)],
            buf.at[pl.ds(first, count)], (halo_s, halo_r), (a, o - 1), {"tok": me + o * split},
            block + o < pn.blocks, block >= o,
        )

    for a in (0, 1):
        own[a].wait()
        for j in range(1, split):
            exchange(a, j).wait_recv()
        for o in range(1, pn.reach + 1):
            halo(a, o).start()

            @pl.when(block < o)
            def _(a=a, o=o):
                buf = (kb, vb)[a]
                here = pl.ds(pn.halo_first(o), pn.halo_count(o))
                buf[here] = jnp.zeros((pn.halo_count(o), kw), BF16)
    if pn.reach * tokens < WINDOW:
        rest = WINDOW - pn.reach * tokens
        for buf in (kb, vb):
            buf[pl.ds(0, rest)] = jnp.zeros((rest, kw), BF16)

    if pn.inside:
        turn(0, steps)

    parts = pn.parts

    def act_piece(i, owner, r):
        first, size = parts[r]
        if pn.inside:
            here = pl.multiple_of((i * gather + owner) * rows + first, 16)
            return turned.at[pl.ds(here, size)]
        return at_ref.at[(low + i) * gather + owner]

    act_mine = [
        pltpu.make_async_copy(
            act_piece(i, c, r), act.at[low + i, pl.ds(*parts[r]), cols(c, length)], act_own.at[i, r])
        for i in range(half) for r in range(len(parts))
    ]
    for copy in act_mine:
        copy.start()

    def act_send(j, i, r):
        return Link(
            ledger, ("act", j, i, r), act_piece(i, xor(c, j), r),
            act.at[low + i, pl.ds(*parts[r]), cols(c, length)],
            (act_s, act_r), (j, i, r), at_plane(j),
        )

    def act_forward(j, i, r, start=low):
        piece = act.at[start + i, pl.ds(*parts[r]), cols(xor(c, j), length)]
        return Link(
            ledger, ("forward", j, i, r), piece, piece, (fwd_s, fwd_r), (j, i, r),
            {"head": xor(hd, 1)})

    order = [(j, i) for i in range(half) for j in (1, 2, 3)]
    if gather == 1:
        order = []

    def act_out(r):
        for j, i in order:
            act_send(j, i, r).start()

    def act_pass(r):
        for j, i in order:
            act_send(j, i, r).wait_recv()
            if pn.share == 2:
                act_forward(j, i, r).start()

    def act_ready(r):
        if pn.share == 2:
            for j, i in [(0, i) for i in range(half)] + order:
                act_forward(j, i, r, half - low).wait_recv()

    act_out(0)
    for a in (0, 1):
        for o in range(1, pn.reach + 1):
            halo(a, o).wait_recv()

    seen = WINDOW + SUB
    chunk = seen // 3
    lanes = group * SUB

    def unit(b, kh, sub):
        start = pl.multiple_of(b * length + sub * SUB, SUB)
        rows_q = pl.ds(start, SUB)
        head = kh * group * HD
        query = jnp.concatenate(
            [qb[rows_q, head + m * HD : head + (m + 1) * HD] for m in range(group)], axis=0
        )
        grad = jnp.concatenate(
            [gb[rows_q, head + m * HD : head + (m + 1) * HD] for m in range(group)], axis=0
        )
        lane_q = pl.ds(pl.multiple_of(sub * SUB, SUB), SUB)
        norm, delta = [
            jnp.concatenate([stb[b, kh, i * group + m : i * group + m + 1, lane_q] for m in range(group)], axis=1)
            for i in range(2)
        ]
        total = jnp.zeros((lanes, HD), F32)
        for piece in range(3):
            here = pl.ds(pl.multiple_of(start + piece * chunk, SUB), chunk)
            keys = kb[here, kh * HD : (kh + 1) * HD]
            values = vb[here, kh * HD : (kh + 1) * HD]
            scores = lax.dot_general(
                keys, query, (((1,), (1,)), ((), ())), preferred_element_type=F32
            )
            prob = jnp.exp2(scores * (QUERY_SCALE * LOG2E) - norm)
            if piece == 0:
                edge = WINDOW - WINDOW_MIN + SUB
                row = lax.broadcasted_iota(jnp.int32, (edge, lanes), 0)
                lane = lax.broadcasted_iota(jnp.int32, (edge, lanes), 1)
                limit = jnp.full((edge, lanes), 0, jnp.int32)
                for m in range(group):
                    limit = jnp.where(
                        lane // SUB == m, lim_ref[(place * kv + kh) * group + m], limit
                    )
                visible = WINDOW + lax.rem(lane, SUB) - row < limit
                prob = jnp.concatenate(
                    [jnp.where(visible, prob[:edge], 0.0), prob[edge:]], axis=0
                )
            if piece == 2:
                row = lax.broadcasted_iota(jnp.int32, (SUB, lanes), 0)
                lane = lax.broadcasted_iota(jnp.int32, (SUB, lanes), 1)
                visible = row <= lax.rem(lane, SUB)
                prob = jnp.concatenate(
                    [prob[: chunk - SUB], jnp.where(visible, prob[chunk - SUB :], 0.0)], axis=0
                )
            dva[here, kh * HD : (kh + 1) * HD] += jnp.dot(
                prob.astype(BF16), grad, preferred_element_type=F32
            )
            dprob = lax.dot_general(
                values, grad, (((1,), (1,)), ((), ())), preferred_element_type=F32
            )
            dscore = (QUERY_SCALE * prob * (dprob - delta)).astype(BF16)
            dka[here, kh * HD : (kh + 1) * HD] += jnp.dot(
                dscore, query, preferred_element_type=F32
            )
            total = total + lax.dot_general(
                dscore, keys, (((0,), (0,)), ((), ())), preferred_element_type=F32
            )
        low_q = total.astype(BF16)
        for m in range(group):
            dqb[rows_q, head + m * HD : head + (m + 1) * HD] = low_q[m * SUB : (m + 1) * SUB]

    def dq_send(j):
        other = xor(place, j)
        src = dqb.at[pl.ds(other * length, length)]
        return Link(
            ledger, ("dq", j), src, dq_ref.at[:, cols(place, qw)], (dq_s, dq_r), (j,), at_plane(j))

    def local_out(src, dst, i):
        return pltpu.make_async_copy(src, dst, out_sem.at[i])

    for j in range(split):
        b = xor(place, j)
        for a in (2, 3, 4):
            if j:
                exchange(a, j).wait_recv()
            else:
                own[a].wait()
        for kh in range(kv):
            @pl.loop(0, subs)
            def _(sub, b=b, kh=kh):
                unit(b, kh, sub)

        if j == 0:
            for copy in act_mine:
                copy.wait()
            if pn.share == 2:
                for r in range(len(parts)):
                    for i in range(half):
                        act_forward(0, i, r).start()

    def back(a, o):
        count, first = pn.halo_count(o), pn.halo_first(o)
        return Link(
            ledger, ("back", a, o), (hsv, hsk)[a].at[pl.ds(first, count)],
            (hrv, hrk)[a].at[o - 1, pl.ds(0, count)], (back_s, back_r), (a, o - 1),
            {"tok": me - o * split}, block >= o, block + o < pn.blocks,
        )

    tail = pn.tail

    def vg_copy(j, owner, h):
        piece = vga.at[owner, pl.ds(*pn.pieces[h])]
        return Link(
            ledger, ("vg", j, h), piece, piece, (vg_s, vg_r), (j, h),
            at_plane(j if j < 3 else (1 if h == tail else 2)),
        )

    def vg_send(j, h):
        return vg_copy(j, c if j < 3 else xor(c, 2 if h == tail else 1), h)

    def vg_wait(j, h):
        vg_copy(j, xor(c, j), h).wait_recv()

    for a in (0, 1):
        (hsv, hsk)[a][...] = (dva, dka)[a][pl.ds(0, WINDOW)].astype(BF16)
        for o in range(1, pn.reach + 1):
            back(a, o).start()
        if a == 0 and pn.ahead:
            first = pn.pieces[0][1]
            vga[c, pl.ds(0, first)] = dva[pl.ds(WINDOW, first)].astype(BF16)
            for j in (1, 2):
                vg_send(j, 0).start()

    def add_back(a):
        for o in range(1, pn.reach + 1):
            back(a, o).wait_recv()

            @pl.when(block + o < pn.blocks)
            def _(o=o):
                count = pn.halo_count(o)
                here = pl.ds(WINDOW + tokens - count, count)
                total = (dva, dka)[a]
                total[here] = total[here] + (hrv, hrk)[a][o - 1, pl.ds(0, count)].astype(F32)

    act_pass(0)
    add_back(0)
    ready = pn.pieces[0][1] if pn.ahead else 0
    vga[c, pl.ds(ready, tokens - ready)] = dva[pl.ds(WINDOW + ready, tokens - ready)].astype(BF16)
    rest = list(range(1 if pn.ahead else 0, len(pn.pieces)))
    if gather > 1:
        for h, g in zip(rest, rest[::-1]):
            vg_send(1, h).start()
            vg_send(2, g).start()
    act_ready(0)
    bits, part = pn.bits, pn.part
    counts = [upper >> (p + 1) for p in range(bits)]
    starts = [sum(counts[:p]) for p in range(bits)]
    partners = [{"tok": xor(u, 1 << p) * gather + c} for p in range(bits)]

    def bit_of(index, k):
        return lax.rem(index // (1 << k), 2)

    def block_at(phase, j, other):
        index = 0
        for k in range(phase):
            index = index + (1 << k) * bit_of(u, k)
        mine = bit_of(u, phase)
        index = index + (1 << phase) * ((1 - mine) if other else mine)
        return index + (1 << (phase + 1)) * j

    def copy_of(s, p, r):
        here, there = pl.ds(starts[p], counts[p]), pl.ds(*parts[r])
        return Link(
            ledger, ("sum", s, p, r), sbuf.at[s, here, there], rbuf.at[s, here, there],
            (rs_s, rs_r), (s, p, r), partners[p],
        )

    def product(s, index, r):
        left = act[index, pl.ds(*parts[r]), :]
        if split == gather:
            return jnp.dot(left, vga[xor(c, s)], preferred_element_type=F32)
        whole = vga[...].reshape(gather * length, part)
        return jnp.dot(left, whole, preferred_element_type=F32)

    def products(s, r):
        there = pl.ds(*parts[r])

        @pl.loop(0, counts[0])
        def _(j):
            sbuf[s, j, there] = product(s, block_at(0, j, True), r).astype(BF16)

        copy_of(s, 0, r).start()

        @pl.loop(0, counts[0])
        def _(j):
            index = block_at(0, j, False)
            acc[s, index, there] = product(s, index, r)

    def arrived(s, p, r):
        there = pl.ds(*parts[r])
        copy_of(s, p, r).wait_recv()

        @pl.loop(0, counts[p])
        def _(j):
            index = block_at(p, j, False)
            acc[s, index, there] = acc[s, index, there] + rbuf[s, starts[p] + j, there].astype(F32)

        if p + 1 < bits:
            @pl.loop(0, counts[p + 1])
            def _(j):
                index = block_at(p + 1, j, True)
                sbuf[s, starts[p + 1] + j, there] = acc[s, index, there].astype(BF16)

            copy_of(s, p + 1, r).start()

    def pass_on():
        for h in range(tail - 1):
            vg_wait(1, h)
            vg_send(3, h).start()
        vg_wait(2, tail)
        vg_send(3, tail).start()
        vg_wait(1, tail - 1)
        vg_send(3, tail - 1).start()

    def vg_rest(j):
        for h in range(tail + 1):
            if j == 3 or (j == 1 and h == tail) or (j == 2 and h != tail):
                vg_wait(j, h)

    last = len(parts) - 1
    if split == 1 and gather > 1:
        pass_on()
        for j in (1, 2, 3):
            vg_rest(j)
    products(0, 0)
    if split > 1:
        pass_on()
        if last:
            act_out(1)
            arrived(0, 0, 0)
        for s in (1, 2):
            vg_rest(s)
            products(s, 0)

    outs = []
    outs.append(local_out(dqb.at[pl.ds(place * length, length)], dq_ref.at[:, cols(place, qw)], 0))
    outs[-1].start()

    add_back(1)
    dkb[...] = dka[pl.ds(WINDOW, tokens)].astype(BF16)

    def dk_send(j):
        other = xor(place, j)
        return Link(
            ledger, ("dk", j), dkb.at[pl.ds(other * length, length)], dk_ref.at[:, cols(place, kw)],
            (dk_s, dk_r), (j,), at_plane(j),
        )

    outs.append(local_out(dkb.at[pl.ds(place * length, length)], dk_ref.at[:, cols(place, kw)], 1))
    outs[-1].start()
    if last:
        vg_rest(3)
        products(3, 0)
        arrived(1, 0, 0)
        arrived(2, 0, 0)
        act_pass(1)
        act_ready(1)
        for s in range(4):
            products(s, 1)
            if s:
                dq_send(s).start()
                dk_send(s).start()
    elif split > 1:
        vg_rest(3)
        products(3, 0)
    if not last:
        for j in range(1, split):
            dq_send(j).start()
            dk_send(j).start()
    if split == gather:
        for j in range(gather):
            src = xor(c, j)
            outs.append(local_out(
                vga.at[src, pl.ds(c * length, length)], dv_ref.at[:, cols(src, kw)], 2 + j))
            outs[-1].start()
    else:
        outs.append(local_out(vga.at[c], dv_ref, 2))
        outs[-1].start()

    weight_in.wait()
    weight_f = wv[...].astype(F32)
    weight_sum = jnp.sum(weight_f * weight_f)

    early, late = list(range(min(3, pn.streams))), list(range(3, pn.streams))
    steps = [(s, 0, last) for s in early]
    if last:
        steps += [(s, 1, 0) for s in early] if bits > 1 else []
    steps = ([(s, 0, 0) for s in late] if last else []) + steps + [(s, 0, last) for s in late]
    for p in range(1, bits):
        steps += [(s, p, r) for r in range(len(parts)) for s in early if p > 1 or r == last]
        steps += [(s, p, r) for r in range(len(parts)) for s in late]
    for s, p, r in steps:
        arrived(s, p, r)

    row_sum = jnp.zeros((rows, 1), F32)
    for s in range(pn.streams):
        wg = acc[s, u]
        row_sum = row_sum + jnp.sum(wg * wg, axis=1, keepdims=True)
    diag = lax.broadcasted_iota(jnp.int32, (rows, rows), 0) == lax.broadcasted_iota(
        jnp.int32, (rows, rows), 1)
    row_old = jnp.sum(jnp.where(diag, rs_ref[...], 0.0), axis=1, keepdims=True)
    row_mix = DECAY_RATE * row_old + (1.0 - DECAY_RATE) * (row_sum / pn.width)
    row_mean = jnp.sum(row_mix) / rows
    scaled_sum = jnp.float32(0.0)
    for s in range(pn.streams):
        wg = acc[s, u]
        here = cols(xor(c, s), part) if split == gather else slice(0, part)
        col_new = jnp.sum(wg * wg, axis=0, keepdims=True) / rows
        col_mix = DECAY_RATE * cs_ref[:, here] + (1.0 - DECAY_RATE) * col_new
        scaled = wg / jnp.sqrt(row_mix * col_mix / row_mean)
        sc_ref[:, here] = scaled
        scaled_sum = scaled_sum + jnp.sum(scaled * scaled)

    outs.append(local_out(sc_ref, sc_out, 2 + gather))
    outs[-1].start()
    row = lax.broadcasted_iota(jnp.int32, (8, 128), 0)
    xs[0] = jnp.where(row < 1, scaled_sum, weight_sum)

    if pn.flat:
        levels = [[
            {"tok": xor(u, i) * gather + xor(c, j), "head": xor(hd, h)}
            for i in range(upper) for j in range(gather) for h in range(n_head) if i or j or h
        ]]
    else:
        levels = [near_ids, far_ids]

    def share(level, i, partner):
        slot = i + (len(near) if level else 0)
        return Link(ledger, ("share", slot), xs.at[level, pl.ds(0, 2)], xr.at[slot, pl.ds(0, 2)], (x_s, x_r), (slot,), partner)

    for level, ids in enumerate(levels):
        for i, partner in enumerate(ids):
            share(level, i, partner).start()
        total = xs[level, pl.ds(0, 2)]
        for i, partner in enumerate(ids):
            share(level, i, partner).wait_recv()
            total = total + xr[i + (len(near) if level else 0), pl.ds(0, 2)]
        xs[level + 1, pl.ds(0, 2)] = total
    sums = xs[len(levels)]
    size = float(rows * n * pn.width * n_head)
    rms_scaled = jnp.sqrt(sums[0:1] / size)
    rms_weight = jnp.sqrt(sums[1:2] / size)
    fac_ref[...] = jnp.broadcast_to(rms_weight / jnp.maximum(1.0, rms_scaled), fac_ref.shape)

    outs.append(local_out(fac_ref, fac_out, 3 + gather))
    outs[-1].start()
    for copy in outs:
        copy.wait()
    for wait in ledger.values():
        wait()


def fused(pn, limits, query, grad, keys, values, norm, delta, act, weight, row_state, col_state):
    kw, qw = pn.kv * HD, pn.kv * pn.group * HD
    whole = WINDOW + pn.tokens
    hbm = pl.BlockSpec(memory_space=pl.ANY)
    dma = pltpu.SemaphoreType.DMA
    half, cuts = pn.half, len(pn.parts)
    peers = pn.n * pn.n_head - 1 if pn.flat else pn.gather * pn.n_head - 1 + pn.upper - 1
    reach, gather, split = pn.reach, pn.gather, pn.split
    piece = (pn.tokens, kw) if split == gather else (pn.tok_len, kw)
    return pl.pallas_call(
        functools.partial(fused_kernel, pn),
        out_shape=[
            jax.ShapeDtypeStruct(query.shape, BF16),
            jax.ShapeDtypeStruct(keys.shape, BF16),
            jax.ShapeDtypeStruct(keys.shape, BF16),
            jax.ShapeDtypeStruct((pn.rows, pn.width), F32),
            jax.ShapeDtypeStruct((8, 128), F32),
        ],
        in_specs=[hbm] * 11,
        out_specs=[hbm] * 5,
        scratch_shapes=[
            pltpu.SMEM(limits.shape, jnp.int32),
            pltpu.VMEM(norm.shape, F32),
            pltpu.VMEM(delta.shape, F32),
            pltpu.VMEM(row_state.shape, F32),
            pltpu.VMEM(col_state.shape, F32),
            pltpu.VMEM((pn.rows, pn.width), F32),
            pltpu.VMEM((8, 128), F32),
            pltpu.VMEM((pn.kv_local, 2 * pn.group, pn.tok_len), F32),
            pltpu.VMEM((pn.rows, pn.width), BF16),
            pltpu.VMEM((pn.tok_len, pn.wide) if pn.inside else act.shape[1:], BF16),
            pltpu.VMEM((pn.wide, pn.tok_len) if pn.inside else (16, 128), BF16),
            pltpu.VMEM((pn.tokens, qw), BF16),
            pltpu.VMEM((pn.tokens, qw), BF16),
            pltpu.VMEM((whole, kw), BF16),
            pltpu.VMEM((whole, kw), BF16),
            pltpu.VMEM((split, pn.kv, 2 * pn.group, pn.tok_len), F32),
            pltpu.VMEM((whole, kw), F32),
            pltpu.VMEM((whole, kw), F32),
            pltpu.VMEM((pn.tokens, qw), BF16),
            pltpu.VMEM((pn.tokens, kw), BF16),
            pltpu.VMEM((WINDOW, kw), BF16),
            pltpu.VMEM((WINDOW, kw), BF16),
            pltpu.VMEM((reach, min(pn.tokens, WINDOW), kw), BF16),
            pltpu.VMEM((reach, min(pn.tokens, WINDOW), kw), BF16),
            pltpu.VMEM((pn.upper, pn.rows, gather * pn.tok_len), BF16),
            pltpu.VMEM((gather,) + piece, BF16),
            pltpu.VMEM((pn.streams, pn.upper, pn.rows, pn.part), F32),
            pltpu.VMEM((pn.streams, pn.upper - 1, pn.rows, pn.part), BF16),
            pltpu.VMEM((pn.streams, pn.upper - 1, pn.rows, pn.part), BF16),
            pltpu.VMEM((3, 8, 128), F32),
            pltpu.VMEM((peers, 8, 128), F32),
            dma((7,)), dma((5,)), dma((5, split)), dma((5, split)), dma((2, reach)), dma((2, reach)),
            dma((2, reach)), dma((2, reach)), dma((half, cuts)),
            dma((gather, half, cuts)), dma((gather, half, cuts)),
            dma((gather, half, cuts)), dma((gather, half, cuts)),
            dma((gather, len(pn.pieces))), dma((gather, len(pn.pieces))), dma((split,)), dma((split,)),
            dma((split,)), dma((split,)), dma((4 + gather,)),
            dma((pn.streams, pn.bits, cuts)), dma((pn.streams, pn.bits, cuts)), dma((peers,)), dma((peers,)),
        ],
        compiler_params=pltpu.CompilerParams(
            collective_id=0, has_side_effects=True, vmem_limit_bytes=56 * 1024 * 1024
        ),
        name="fused",
    )(limits, query, grad, keys, values, norm, delta, act, weight, row_state, col_state)


def finish_kernel(
    dq_in, dk_in, dv_in, w_in, sc_in, fac_in, dq, dk, dv, new, upd,
    dq_v, dk_v, dv_v, w_v, sc_v, new_v, upd_v, fac_ref, in_sem, out_sem,
):
    pairs = [(dq_in, dq_v, dq), (dk_in, dk_v, dk), (dv_in, dv_v, dv)]
    loads = [pltpu.make_async_copy(fac_in, fac_ref, in_sem.at[5]), pltpu.make_async_copy(sc_in, sc_v, in_sem.at[3]), pltpu.make_async_copy(w_in, w_v, in_sem.at[4])]
    for copy in loads:
        copy.start()
    ins = [pltpu.make_async_copy(a, b, in_sem.at[i]) for i, (a, b, _) in enumerate(pairs)]
    outs = [pltpu.make_async_copy(b, d, out_sem.at[i]) for i, (_, b, d) in enumerate(pairs)]
    outs += [pltpu.make_async_copy(new_v, new, out_sem.at[3]), pltpu.make_async_copy(upd_v, upd, out_sem.at[4])]
    for copy in ins:
        copy.start()
    for copy in loads:
        copy.wait()
    update = sc_v[...] * fac_ref[0:1, 0:1]
    upd_v[...] = update
    outs[4].start()
    new_v[...] = (w_v[...].astype(F32) - LEARN_RATE * update).astype(BF16)
    outs[3].start()
    for i in range(3):
        ins[i].wait()
        outs[i].start()
    for copy in outs:
        copy.wait()


def finish(dq, dk, dv, weight, scaled, factor):
    hbm = pl.BlockSpec(memory_space=pl.ANY)
    arrays = [dq, dk, dv, weight, scaled]
    outs = [dq, dk, dv, weight, scaled]
    return pl.pallas_call(
        finish_kernel,
        out_shape=[jax.ShapeDtypeStruct(x.shape, x.dtype) for x in outs],
        in_specs=[hbm] * 6,
        out_specs=[hbm] * 5,
        scratch_shapes=[pltpu.VMEM(x.shape, x.dtype) for x in arrays + [weight, scaled, factor]]
        + [pltpu.SemaphoreType.DMA((6,)), pltpu.SemaphoreType.DMA((5,))],
        name="finish",
    )(*arrays, factor)


def shards(
    query_rows, key_rows, value_rows, out_grad, log_norm, delta_rows, window_len,
    activations, value_weight, row_state, col_state, *, n, n_head,
):
    tok_len = query_rows.shape[0]
    kv_local = key_rows.shape[1] // HD
    group = query_rows.shape[1] // key_rows.shape[1]
    rows, width = value_weight.shape
    pn = Plan(n, n_head, tok_len, kv_local, group, width, rows)

    act = activations if pn.inside else activations.T.reshape(n, rows, tok_len)
    query_grad, key_grad, value_grad, scaled, factor = fused(
        pn, window_len, query_rows, out_grad, key_rows, value_rows, log_norm.T, delta_rows.T, act,
        value_weight, row_state, col_state,
    )
    return finish(query_grad, key_grad, value_grad, value_weight, scaled, factor)


def solution(mesh):
    both = P("tok", "head")
    return jax.shard_map(
        functools.partial(shards, n=mesh.shape["tok"], n_head=mesh.shape["head"]),
        mesh=mesh,
        in_specs=(
            both, both, both, both, both, both, P("head"), P("tok", None),
            both, P("head", "tok"), both,
        ),
        out_specs=(both,) * 5,
        check_vma=False,
    )
```

```python
import functools
import math

import jax
import jax.numpy as jnp
from jax import lax
from jax.experimental import pallas as pl
from jax.experimental.pallas import tpu as pltpu
from jax.sharding import PartitionSpec as P

HD = 128
WINDOW = 1024
WINDOW_MIN = 896
SUB = 128
QUERY_SCALE = 1.0 / 12.0
LOG2E = math.log2(math.e)
DECAY_RATE = 0.9
LEARN_RATE = 0.05
F32 = jnp.float32
BF16 = jnp.bfloat16
MESH = pl.DeviceIdType.MESH


def xor(index, j):
    k = 0
    while (1 << k) <= j:
        if (j >> k) & 1:
            index = index + (1 << k) * (1 - 2 * lax.rem(index // (1 << k), 2))
        k += 1
    return index


class Plan:
    def __init__(self, n, n_head, tok_len, kv_local, group, width, rows):
        self.n, self.n_head, self.tok_len = n, n_head, tok_len
        self.kv_local, self.group = kv_local, group
        self.width, self.rows = width, rows
        self.gather = 4 if n % 4 == 0 else 1
        self.upper = n // self.gather
        self.split = self.gather if kv_local % self.gather == 0 else 1
        self.kv = kv_local // self.split
        self.tokens = self.split * tok_len
        self.blocks = n // self.split
        self.reach = min(-(-WINDOW // self.tokens), self.blocks - 1)
        self.subs = tok_len // SUB
        self.streams = self.split
        self.part = width // self.streams
        self.bits = int(math.log2(self.upper))
        self.share = 2 if n_head % 2 == 0 and self.upper % 2 == 0 else 1
        self.half = self.upper // self.share
        self.wide = self.half * self.gather * rows
        self.inside = rows % 16 == 0 and self.wide % SUB == 0
        first = rows * 5 // 7 // 16 * 16
        cut = self.inside and self.split == self.gather and first
        self.parts = [(0, first), (first, rows - first)] if cut else [(0, rows)]
        self.flat = n * n_head <= 64
        length = self.tokens if self.split == self.gather else tok_len
        first, middle = self.tokens - WINDOW, length // 2
        self.ahead = self.split == self.gather and 0 < first < middle and first % 16 == 0
        if self.ahead:
            self.pieces = [(0, first), (first, middle - first), (middle, length - middle)]
        else:
            self.pieces = [(0, middle), (middle, length - middle)]
        self.tail = len(self.pieces) - 1

    def halo_count(self, o):
        return min(self.tokens, WINDOW - (o - 1) * self.tokens)

    def halo_first(self, o):
        return max(0, WINDOW - o * self.tokens)


class Link:
    def __init__(self, ledger, key, src, dst, sems, at, device, send_if=None, recv_if=None):
        self.ledger, self.key = ledger, key
        self.send_if, self.recv_if = send_if, recv_if
        self.copy = pltpu.make_async_remote_copy(
            src_ref=src, dst_ref=dst, send_sem=sems[0].at[at], recv_sem=sems[1].at[at],
            device_id=device, device_id_type=MESH,
        )

    def guarded(self, condition, action):
        if condition is None:
            action()
        else:
            pl.when(condition)(action)

    def start(self):
        self.guarded(self.send_if, self.copy.start)
        self.ledger[self.key + ("send",)] = lambda: self.guarded(self.send_if, self.copy.wait_send)
        self.ledger[self.key + ("recv",)] = lambda: self.guarded(self.recv_if, self.copy.wait_recv)

    def wait_recv(self):
        self.ledger.pop(self.key + ("recv",))
        self.guarded(self.recv_if, self.copy.wait_recv)


def fused_kernel(
    pn,
    lim_in, q_ref, g_ref, k_ref, v_ref, ln_in, de_in, at_ref, w_ref, rs_in, cs_in,
    dq_ref, dk_ref, dv_ref, sc_out, fac_out,
    lim_ref, ln_ref, de_ref, rs_ref, cs_ref, sc_ref, fac_ref, st, wv, abuf, turned, qb, gb, kb, vb, stb, dva, dka, dqb, dkb, hsv, hsk, hrv, hrk, act, vga, acc, sbuf, rbuf,
    xs, xr,
    own_sem, small_sem, in_s, in_r, halo_s, halo_r, back_s, back_r, act_own, act_s, act_r, fwd_s, fwd_r,
    vg_s, vg_r, dq_s, dq_r, dk_s, dk_r, out_sem, rs_s, rs_r, x_s, x_r,
):
    n, n_head, gather, upper = pn.n, pn.n_head, pn.gather, pn.upper
    split, kv, length, tokens = pn.split, pn.kv, pn.tok_len, pn.tokens
    group, subs = pn.group, pn.subs
    me, hd = lax.axis_index("tok"), lax.axis_index("head")
    c, u = lax.rem(me, gather), me // gather
    place, block = lax.rem(me, split), me // split
    kw, qw = kv * HD, kv * group * HD
    rows = pn.rows
    ledger = {}

    def at_plane(j):
        return {"tok": me - c + xor(c, j)}

    near = [(j, h) for j in range(gather) for h in range(n_head) if j or h]
    far = list(range(1, upper))
    near_ids = [{"tok": me - c + xor(c, j), "head": xor(hd, h)} for j, h in near]
    far_ids = [{"tok": xor(u, i) * gather + c} for i in far]
    barrier = pltpu.get_barrier_semaphore()
    for partner in near_ids + far_ids:
        pl.semaphore_signal(barrier, inc=1, device_id=partner, device_id_type=MESH)
    lone = []
    if split == 1:
        for o in range(1, pn.reach + 1):
            lone.append(o)
            @pl.when(block + o < pn.blocks)
            def _(o=o):
                pl.semaphore_signal(barrier, inc=1, device_id={"tok": me + o}, device_id_type=MESH)

            @pl.when(block >= o)
            def _(o=o):
                pl.semaphore_signal(barrier, inc=1, device_id={"tok": me - o}, device_id_type=MESH)

    def cols(index, size):
        return pl.ds(pl.multiple_of(index * size, 128), size)

    own = [
        pltpu.make_async_copy(k_ref.at[:, cols(place, kw)], kb.at[pl.ds(WINDOW + place * length, length)], own_sem.at[0]),
        pltpu.make_async_copy(v_ref.at[:, cols(place, kw)], vb.at[pl.ds(WINDOW + place * length, length)], own_sem.at[1]),
        pltpu.make_async_copy(q_ref.at[:, cols(place, qw)], qb.at[pl.ds(place * length, length)], own_sem.at[2]),
        pltpu.make_async_copy(g_ref.at[:, cols(place, qw)], gb.at[pl.ds(place * length, length)], own_sem.at[3]),
        pltpu.make_async_copy(st.at[pl.ds(place * kv, kv)], stb.at[place], own_sem.at[4]),
    ]
    half = pn.half
    low = lax.rem(hd, pn.share) * half
    if pn.inside:
        load = pltpu.make_async_copy(
            at_ref.at[:, cols(lax.rem(hd, pn.share), pn.wide)], abuf, own_sem.at[5]
        )
        load.start()
    for copy in own[:4]:
        copy.start()
    small = [
        pltpu.make_async_copy(src, dst, small_sem.at[i])
        for i, (src, dst) in enumerate(
            [(ln_in, ln_ref), (de_in, de_ref), (lim_in, lim_ref), (rs_in, rs_ref), (cs_in, cs_ref)])
    ]
    for copy in small:
        copy.start()
    weight_in = pltpu.make_async_copy(w_ref, wv, own_sem.at[6])
    weight_in.start()

    pl.semaphore_wait(barrier, len(near_ids) + len(far_ids))
    for o in lone:
        @pl.when(block + o < pn.blocks)
        def _():
            pl.semaphore_wait(barrier, 1)

        @pl.when(block >= o)
        def _():
            pl.semaphore_wait(barrier, 1)

    def exchange(a, j):
        other = xor(place, j)
        src, dst = [
            (k_ref.at[:, cols(other, kw)], kb.at[pl.ds(WINDOW + place * length, length)]),
            (v_ref.at[:, cols(other, kw)], vb.at[pl.ds(WINDOW + place * length, length)]),
            (q_ref.at[:, cols(other, qw)], qb.at[pl.ds(place * length, length)]),
            (g_ref.at[:, cols(other, qw)], gb.at[pl.ds(place * length, length)]),
            (st.at[pl.ds(other * kv, kv)], stb.at[place]),
        ][a]
        return Link(ledger, ("in", a, j), src, dst, (in_s, in_r), (a, j), at_plane(j))

    for a in (0, 1, 2, 3):
        for j in range(1, split):
            exchange(a, j).start()
    for copy in small:
        copy.wait()
    for i, ref in enumerate((ln_ref, de_ref)):
        stat = ref[...]
        if i == 0:
            stat = stat * LOG2E
        for k in range(pn.kv_local):
            st[k, i * group : (i + 1) * group] = stat[k * group : (k + 1) * group]
    own[4].start()
    for j in range(1, split):
        exchange(4, j).start()
    dva[...] = jnp.zeros_like(dva)
    dka[...] = jnp.zeros_like(dka)

    def turn(first, last):
        @pl.loop(first, last)
        def _(i):
            here = pl.ds(pl.multiple_of(i * SUB, SUB), SUB)
            turned[here, :] = abuf[:, here].T

    steps = pn.wide // SUB
    if pn.inside:
        load.wait()

    def halo(a, o):
        count, first = pn.halo_count(o), pn.halo_first(o)
        buf = (kb, vb)[a]
        return Link(
            ledger, ("halo", a, o), buf.at[pl.ds(WINDOW + tokens - count, count)],
            buf.at[pl.ds(first, count)], (halo_s, halo_r), (a, o - 1), {"tok": me + o * split},
            block + o < pn.blocks, block >= o,
        )

    for a in (0, 1):
        own[a].wait()
        for j in range(1, split):
            exchange(a, j).wait_recv()
        for o in range(1, pn.reach + 1):
            halo(a, o).start()

            @pl.when(block < o)
            def _(a=a, o=o):
                buf = (kb, vb)[a]
                here = pl.ds(pn.halo_first(o), pn.halo_count(o))
                buf[here] = jnp.zeros((pn.halo_count(o), kw), BF16)
    if pn.reach * tokens < WINDOW:
        rest = WINDOW - pn.reach * tokens
        for buf in (kb, vb):
            buf[pl.ds(0, rest)] = jnp.zeros((rest, kw), BF16)

    if pn.inside:
        turn(0, steps)

    parts = pn.parts

    def act_piece(i, owner, r):
        first, size = parts[r]
        if pn.inside:
            here = pl.multiple_of((i * gather + owner) * rows + first, 16)
            return turned.at[pl.ds(here, size)]
        return at_ref.at[(low + i) * gather + owner]

    act_mine = [
        pltpu.make_async_copy(
            act_piece(i, c, r), act.at[low + i, pl.ds(*parts[r]), cols(c, length)], act_own.at[i, r])
        for i in range(half) for r in range(len(parts))
    ]
    for copy in act_mine:
        copy.start()

    def act_send(j, i, r):
        return Link(
            ledger, ("act", j, i, r), act_piece(i, xor(c, j), r),
            act.at[low + i, pl.ds(*parts[r]), cols(c, length)],
            (act_s, act_r), (j, i, r), at_plane(j),
        )

    def act_forward(j, i, r, start=low):
        piece = act.at[start + i, pl.ds(*parts[r]), cols(xor(c, j), length)]
        return Link(
            ledger, ("forward", j, i, r), piece, piece, (fwd_s, fwd_r), (j, i, r),
            {"head": xor(hd, 1)})

    order = [(j, i) for i in range(half) for j in (1, 2, 3)]
    if gather == 1:
        order = []

    def act_out(r):
        for j, i in order:
            act_send(j, i, r).start()

    def act_pass(r):
        for j, i in order:
            act_send(j, i, r).wait_recv()
            if pn.share == 2:
                act_forward(j, i, r).start()

    def act_ready(r):
        if pn.share == 2:
            for j, i in [(0, i) for i in range(half)] + order:
                act_forward(j, i, r, half - low).wait_recv()

    act_out(0)
    for a in (0, 1):
        for o in range(1, pn.reach + 1):
            halo(a, o).wait_recv()

    seen = WINDOW + SUB
    chunk = seen // 3
    lanes = group * SUB

    def unit(b, kh, sub):
        start = pl.multiple_of(b * length + sub * SUB, SUB)
        rows_q = pl.ds(start, SUB)
        head = kh * group * HD
        query = jnp.concatenate(
            [qb[rows_q, head + m * HD : head + (m + 1) * HD] for m in range(group)], axis=0
        )
        grad = jnp.concatenate(
            [gb[rows_q, head + m * HD : head + (m + 1) * HD] for m in range(group)], axis=0
        )
        lane_q = pl.ds(pl.multiple_of(sub * SUB, SUB), SUB)
        norm, delta = [
            jnp.concatenate([stb[b, kh, i * group + m : i * group + m + 1, lane_q] for m in range(group)], axis=1)
            for i in range(2)
        ]
        total = jnp.zeros((lanes, HD), F32)
        for piece in range(3):
            here = pl.ds(pl.multiple_of(start + piece * chunk, SUB), chunk)
            keys = kb[here, kh * HD : (kh + 1) * HD]
            values = vb[here, kh * HD : (kh + 1) * HD]
            scores = lax.dot_general(
                keys, query, (((1,), (1,)), ((), ())), preferred_element_type=F32
            )
            prob = jnp.exp2(scores * (QUERY_SCALE * LOG2E) - norm)
            if piece == 0:
                edge = WINDOW - WINDOW_MIN + SUB
                row = lax.broadcasted_iota(jnp.int32, (edge, lanes), 0)
                lane = lax.broadcasted_iota(jnp.int32, (edge, lanes), 1)
                limit = jnp.full((edge, lanes), 0, jnp.int32)
                for m in range(group):
                    limit = jnp.where(
                        lane // SUB == m, lim_ref[(place * kv + kh) * group + m], limit
                    )
                visible = WINDOW + lax.rem(lane, SUB) - row < limit
                prob = jnp.concatenate(
                    [jnp.where(visible, prob[:edge], 0.0), prob[edge:]], axis=0
                )
            if piece == 2:
                row = lax.broadcasted_iota(jnp.int32, (SUB, lanes), 0)
                lane = lax.broadcasted_iota(jnp.int32, (SUB, lanes), 1)
                visible = row <= lax.rem(lane, SUB)
                prob = jnp.concatenate(
                    [prob[: chunk - SUB], jnp.where(visible, prob[chunk - SUB :], 0.0)], axis=0
                )
            dva[here, kh * HD : (kh + 1) * HD] += jnp.dot(
                prob.astype(BF16), grad, preferred_element_type=F32
            )
            dprob = lax.dot_general(
                values, grad, (((1,), (1,)), ((), ())), preferred_element_type=F32
            )
            dscore = (QUERY_SCALE * prob * (dprob - delta)).astype(BF16)
            dka[here, kh * HD : (kh + 1) * HD] += jnp.dot(
                dscore, query, preferred_element_type=F32
            )
            total = total + lax.dot_general(
                dscore, keys, (((0,), (0,)), ((), ())), preferred_element_type=F32
            )
        low_q = total.astype(BF16)
        for m in range(group):
            dqb[rows_q, head + m * HD : head + (m + 1) * HD] = low_q[m * SUB : (m + 1) * SUB]

    def dq_send(j):
        other = xor(place, j)
        src = dqb.at[pl.ds(other * length, length)]
        return Link(
            ledger, ("dq", j), src, dq_ref.at[:, cols(place, qw)], (dq_s, dq_r), (j,), at_plane(j))

    def local_out(src, dst, i):
        return pltpu.make_async_copy(src, dst, out_sem.at[i])

    for j in range(split):
        b = xor(place, j)
        for a in (2, 3, 4):
            if j:
                exchange(a, j).wait_recv()
            else:
                own[a].wait()
        for kh in range(kv):
            @pl.loop(0, subs)
            def _(sub, b=b, kh=kh):
                unit(b, kh, sub)

        if j == 0:
            for copy in act_mine:
                copy.wait()
            if pn.share == 2:
                for r in range(len(parts)):
                    for i in range(half):
                        act_forward(0, i, r).start()

    def back(a, o):
        count, first = pn.halo_count(o), pn.halo_first(o)
        return Link(
            ledger, ("back", a, o), (hsv, hsk)[a].at[pl.ds(first, count)],
            (hrv, hrk)[a].at[o - 1, pl.ds(0, count)], (back_s, back_r), (a, o - 1),
            {"tok": me - o * split}, block >= o, block + o < pn.blocks,
        )

    tail = pn.tail

    def vg_copy(j, owner, h):
        piece = vga.at[owner, pl.ds(*pn.pieces[h])]
        return Link(
            ledger, ("vg", j, h), piece, piece, (vg_s, vg_r), (j, h),
            at_plane(j if j < 3 else (1 if h == tail else 2)),
        )

    def vg_send(j, h):
        return vg_copy(j, c if j < 3 else xor(c, 2 if h == tail else 1), h)

    def vg_wait(j, h):
        vg_copy(j, xor(c, j), h).wait_recv()

    for a in (0, 1):
        (hsv, hsk)[a][...] = (dva, dka)[a][pl.ds(0, WINDOW)].astype(BF16)
        for o in range(1, pn.reach + 1):
            back(a, o).start()
        if a == 0 and pn.ahead:
            first = pn.pieces[0][1]
            vga[c, pl.ds(0, first)] = dva[pl.ds(WINDOW, first)].astype(BF16)
            for j in (1, 2):
                vg_send(j, 0).start()

    def add_back(a):
        for o in range(1, pn.reach + 1):
            back(a, o).wait_recv()

            @pl.when(block + o < pn.blocks)
            def _(o=o):
                count = pn.halo_count(o)
                here = pl.ds(WINDOW + tokens - count, count)
                total = (dva, dka)[a]
                total[here] = total[here] + (hrv, hrk)[a][o - 1, pl.ds(0, count)].astype(F32)

    act_pass(0)
    add_back(0)
    ready = pn.pieces[0][1] if pn.ahead else 0
    vga[c, pl.ds(ready, tokens - ready)] = dva[pl.ds(WINDOW + ready, tokens - ready)].astype(BF16)
    rest = list(range(1 if pn.ahead else 0, len(pn.pieces)))
    if gather > 1:
        for h, g in zip(rest, rest[::-1]):
            vg_send(1, h).start()
            vg_send(2, g).start()
    act_ready(0)
    bits, part = pn.bits, pn.part
    counts = [upper >> (p + 1) for p in range(bits)]
    starts = [sum(counts[:p]) for p in range(bits)]
    partners = [{"tok": xor(u, 1 << p) * gather + c} for p in range(bits)]

    def bit_of(index, k):
        return lax.rem(index // (1 << k), 2)

    def block_at(phase, j, other):
        index = 0
        for k in range(phase):
            index = index + (1 << k) * bit_of(u, k)
        mine = bit_of(u, phase)
        index = index + (1 << phase) * ((1 - mine) if other else mine)
        return index + (1 << (phase + 1)) * j

    def copy_of(s, p, r):
        here, there = pl.ds(starts[p], counts[p]), pl.ds(*parts[r])
        return Link(
            ledger, ("sum", s, p, r), sbuf.at[s, here, there], rbuf.at[s, here, there],
            (rs_s, rs_r), (s, p, r), partners[p],
        )

    def product(s, index, r):
        left = act[index, pl.ds(*parts[r]), :]
        if split == gather:
            return jnp.dot(left, vga[xor(c, s)], preferred_element_type=F32)
        whole = vga[...].reshape(gather * length, part)
        return jnp.dot(left, whole, preferred_element_type=F32)

    def products(s, r):
        there = pl.ds(*parts[r])

        @pl.loop(0, counts[0])
        def _(j):
            sbuf[s, j, there] = product(s, block_at(0, j, True), r).astype(BF16)

        copy_of(s, 0, r).start()

        @pl.loop(0, counts[0])
        def _(j):
            index = block_at(0, j, False)
            acc[s, index, there] = product(s, index, r)

    def arrived(s, p, r):
        there = pl.ds(*parts[r])
        copy_of(s, p, r).wait_recv()

        @pl.loop(0, counts[p])
        def _(j):
            index = block_at(p, j, False)
            acc[s, index, there] = acc[s, index, there] + rbuf[s, starts[p] + j, there].astype(F32)

        if p + 1 < bits:
            @pl.loop(0, counts[p + 1])
            def _(j):
                index = block_at(p + 1, j, True)
                sbuf[s, starts[p + 1] + j, there] = acc[s, index, there].astype(BF16)

            copy_of(s, p + 1, r).start()

    def pass_on():
        for h in range(tail - 1):
            vg_wait(1, h)
            vg_send(3, h).start()
        vg_wait(2, tail)
        vg_send(3, tail).start()
        vg_wait(1, tail - 1)
        vg_send(3, tail - 1).start()

    def vg_rest(j):
        for h in range(tail + 1):
            if j == 3 or (j == 1 and h == tail) or (j == 2 and h != tail):
                vg_wait(j, h)

    last = len(parts) - 1
    if split == 1 and gather > 1:
        pass_on()
        for j in (1, 2, 3):
            vg_rest(j)
    products(0, 0)
    if split > 1:
        pass_on()
        if last:
            act_out(1)
            arrived(0, 0, 0)
        for s in (1, 2):
            vg_rest(s)
            products(s, 0)

    outs = []
    outs.append(local_out(dqb.at[pl.ds(place * length, length)], dq_ref.at[:, cols(place, qw)], 0))
    outs[-1].start()

    add_back(1)
    dkb[...] = dka[pl.ds(WINDOW, tokens)].astype(BF16)

    def dk_send(j):
        other = xor(place, j)
        return Link(
            ledger, ("dk", j), dkb.at[pl.ds(other * length, length)], dk_ref.at[:, cols(place, kw)],
            (dk_s, dk_r), (j,), at_plane(j),
        )

    outs.append(local_out(dkb.at[pl.ds(place * length, length)], dk_ref.at[:, cols(place, kw)], 1))
    outs[-1].start()
    if last:
        vg_rest(3)
        products(3, 0)
        arrived(1, 0, 0)
        arrived(2, 0, 0)
        act_pass(1)
        act_ready(1)
        for s in range(4):
            if s < 3:
                dq_send(3 - s).start()
                dk_send(3 - s).start()
            products(s, 1)
    elif split > 1:
        vg_rest(3)
        products(3, 0)
    if not last:
        for j in range(1, split):
            dq_send(j).start()
            dk_send(j).start()
    if split == gather:
        for j in range(gather):
            src = xor(c, j)
            outs.append(local_out(
                vga.at[src, pl.ds(c * length, length)], dv_ref.at[:, cols(src, kw)], 2 + j))
            outs[-1].start()
    else:
        outs.append(local_out(vga.at[c], dv_ref, 2))
        outs[-1].start()

    weight_in.wait()
    weight_f = wv[...].astype(F32)
    weight_sum = jnp.sum(weight_f * weight_f)

    early, late = list(range(min(3, pn.streams))), list(range(3, pn.streams))
    steps = [(s, 0, last) for s in early]
    if last:
        steps += [(s, 1, 0) for s in early] if bits > 1 else []
    steps = ([(s, 0, 0) for s in late] if last else []) + steps + [(s, 0, last) for s in late]
    for p in range(1, bits):
        steps += [(s, p, r) for r in range(len(parts)) for s in early if p > 1 or r == last]
        steps += [(s, p, r) for r in range(len(parts)) for s in late]
    for s, p, r in steps:
        arrived(s, p, r)

    row_sum = jnp.zeros((rows, 1), F32)
    for s in range(pn.streams):
        wg = acc[s, u]
        row_sum = row_sum + jnp.sum(wg * wg, axis=1, keepdims=True)
    diag = lax.broadcasted_iota(jnp.int32, (rows, rows), 0) == lax.broadcasted_iota(
        jnp.int32, (rows, rows), 1)
    row_old = jnp.sum(jnp.where(diag, rs_ref[...], 0.0), axis=1, keepdims=True)
    row_mix = DECAY_RATE * row_old + (1.0 - DECAY_RATE) * (row_sum / pn.width)
    row_mean = jnp.sum(row_mix) / rows
    scaled_sum = jnp.float32(0.0)
    for s in range(pn.streams):
        wg = acc[s, u]
        here = cols(xor(c, s), part) if split == gather else slice(0, part)
        col_new = jnp.sum(wg * wg, axis=0, keepdims=True) / rows
        col_mix = DECAY_RATE * cs_ref[:, here] + (1.0 - DECAY_RATE) * col_new
        scaled = wg / jnp.sqrt(row_mix * col_mix / row_mean)
        sc_ref[:, here] = scaled
        scaled_sum = scaled_sum + jnp.sum(scaled * scaled)

    outs.append(local_out(sc_ref, sc_out, 2 + gather))
    outs[-1].start()
    row = lax.broadcasted_iota(jnp.int32, (8, 128), 0)
    xs[0] = jnp.where(row < 1, scaled_sum, weight_sum)

    if pn.flat:
        levels = [[
            {"tok": xor(u, i) * gather + xor(c, j), "head": xor(hd, h)}
            for i in range(upper) for j in range(gather) for h in range(n_head) if i or j or h
        ]]
    else:
        levels = [near_ids, far_ids]

    def share(level, i, partner):
        slot = i + (len(near) if level else 0)
        return Link(ledger, ("share", slot), xs.at[level, pl.ds(0, 2)], xr.at[slot, pl.ds(0, 2)], (x_s, x_r), (slot,), partner)

    for level, ids in enumerate(levels):
        for i, partner in enumerate(ids):
            share(level, i, partner).start()
        total = xs[level, pl.ds(0, 2)]
        for i, partner in enumerate(ids):
            share(level, i, partner).wait_recv()
            total = total + xr[i + (len(near) if level else 0), pl.ds(0, 2)]
        xs[level + 1, pl.ds(0, 2)] = total
    sums = xs[len(levels)]
    size = float(rows * n * pn.width * n_head)
    rms_scaled = jnp.sqrt(sums[0:1] / size)
    rms_weight = jnp.sqrt(sums[1:2] / size)
    fac_ref[...] = jnp.broadcast_to(rms_weight / jnp.maximum(1.0, rms_scaled), fac_ref.shape)

    outs.append(local_out(fac_ref, fac_out, 3 + gather))
    outs[-1].start()
    for copy in outs:
        copy.wait()
    for wait in ledger.values():
        wait()


def fused(pn, limits, query, grad, keys, values, norm, delta, act, weight, row_state, col_state):
    kw, qw = pn.kv * HD, pn.kv * pn.group * HD
    whole = WINDOW + pn.tokens
    hbm = pl.BlockSpec(memory_space=pl.ANY)
    dma = pltpu.SemaphoreType.DMA
    half, cuts = pn.half, len(pn.parts)
    peers = pn.n * pn.n_head - 1 if pn.flat else pn.gather * pn.n_head - 1 + pn.upper - 1
    reach, gather, split = pn.reach, pn.gather, pn.split
    piece = (pn.tokens, kw) if split == gather else (pn.tok_len, kw)
    return pl.pallas_call(
        functools.partial(fused_kernel, pn),
        out_shape=[
            jax.ShapeDtypeStruct(query.shape, BF16),
            jax.ShapeDtypeStruct(keys.shape, BF16),
            jax.ShapeDtypeStruct(keys.shape, BF16),
            jax.ShapeDtypeStruct((pn.rows, pn.width), F32),
            jax.ShapeDtypeStruct((8, 128), F32),
        ],
        in_specs=[hbm] * 11,
        out_specs=[hbm] * 5,
        scratch_shapes=[
            pltpu.SMEM(limits.shape, jnp.int32),
            pltpu.VMEM(norm.shape, F32),
            pltpu.VMEM(delta.shape, F32),
            pltpu.VMEM(row_state.shape, F32),
            pltpu.VMEM(col_state.shape, F32),
            pltpu.VMEM((pn.rows, pn.width), F32),
            pltpu.VMEM((8, 128), F32),
            pltpu.VMEM((pn.kv_local, 2 * pn.group, pn.tok_len), F32),
            pltpu.VMEM((pn.rows, pn.width), BF16),
            pltpu.VMEM((pn.tok_len, pn.wide) if pn.inside else act.shape[1:], BF16),
            pltpu.VMEM((pn.wide, pn.tok_len) if pn.inside else (16, 128), BF16),
            pltpu.VMEM((pn.tokens, qw), BF16),
            pltpu.VMEM((pn.tokens, qw), BF16),
            pltpu.VMEM((whole, kw), BF16),
            pltpu.VMEM((whole, kw), BF16),
            pltpu.VMEM((split, pn.kv, 2 * pn.group, pn.tok_len), F32),
            pltpu.VMEM((whole, kw), F32),
            pltpu.VMEM((whole, kw), F32),
            pltpu.VMEM((pn.tokens, qw), BF16),
            pltpu.VMEM((pn.tokens, kw), BF16),
            pltpu.VMEM((WINDOW, kw), BF16),
            pltpu.VMEM((WINDOW, kw), BF16),
            pltpu.VMEM((reach, min(pn.tokens, WINDOW), kw), BF16),
            pltpu.VMEM((reach, min(pn.tokens, WINDOW), kw), BF16),
            pltpu.VMEM((pn.upper, pn.rows, gather * pn.tok_len), BF16),
            pltpu.VMEM((gather,) + piece, BF16),
            pltpu.VMEM((pn.streams, pn.upper, pn.rows, pn.part), F32),
            pltpu.VMEM((pn.streams, pn.upper - 1, pn.rows, pn.part), BF16),
            pltpu.VMEM((pn.streams, pn.upper - 1, pn.rows, pn.part), BF16),
            pltpu.VMEM((3, 8, 128), F32),
            pltpu.VMEM((peers, 8, 128), F32),
            dma((7,)), dma((5,)), dma((5, split)), dma((5, split)), dma((2, reach)), dma((2, reach)),
            dma((2, reach)), dma((2, reach)), dma((half, cuts)),
            dma((gather, half, cuts)), dma((gather, half, cuts)),
            dma((gather, half, cuts)), dma((gather, half, cuts)),
            dma((gather, len(pn.pieces))), dma((gather, len(pn.pieces))), dma((split,)), dma((split,)),
            dma((split,)), dma((split,)), dma((4 + gather,)),
            dma((pn.streams, pn.bits, cuts)), dma((pn.streams, pn.bits, cuts)), dma((peers,)), dma((peers,)),
        ],
        compiler_params=pltpu.CompilerParams(
            collective_id=0, has_side_effects=True, vmem_limit_bytes=56 * 1024 * 1024
        ),
        name="fused",
    )(limits, query, grad, keys, values, norm, delta, act, weight, row_state, col_state)


def finish_kernel(
    dq_in, dk_in, dv_in, w_in, sc_in, fac_in, dq, dk, dv, new, upd,
    dq_v, dk_v, dv_v, w_v, sc_v, new_v, upd_v, fac_ref, in_sem, out_sem,
):
    pairs = [(dq_in, dq_v, dq), (dk_in, dk_v, dk), (dv_in, dv_v, dv)]
    loads = [pltpu.make_async_copy(fac_in, fac_ref, in_sem.at[5]), pltpu.make_async_copy(sc_in, sc_v, in_sem.at[3]), pltpu.make_async_copy(w_in, w_v, in_sem.at[4])]
    ins = [pltpu.make_async_copy(a, b, in_sem.at[i]) for i, (a, b, _) in enumerate(pairs)]
    outs = [pltpu.make_async_copy(b, d, out_sem.at[i]) for i, (_, b, d) in enumerate(pairs)]
    outs += [pltpu.make_async_copy(new_v, new, out_sem.at[3]), pltpu.make_async_copy(upd_v, upd, out_sem.at[4])]
    for copy in ins + loads:
        copy.start()
    for i in range(3):
        ins[i].wait()
        outs[i].start()
    for copy in loads:
        copy.wait()
    update = sc_v[...] * fac_ref[0:1, 0:1]
    upd_v[...] = update
    outs[4].start()
    new_v[...] = (w_v[...].astype(F32) - LEARN_RATE * update).astype(BF16)
    outs[3].start()
    for copy in outs:
        copy.wait()


def finish(dq, dk, dv, weight, scaled, factor):
    hbm = pl.BlockSpec(memory_space=pl.ANY)
    arrays = [dq, dk, dv, weight, scaled]
    outs = [dq, dk, dv, weight, scaled]
    return pl.pallas_call(
        finish_kernel,
        out_shape=[jax.ShapeDtypeStruct(x.shape, x.dtype) for x in outs],
        in_specs=[hbm] * 6,
        out_specs=[hbm] * 5,
        scratch_shapes=[pltpu.VMEM(x.shape, x.dtype) for x in arrays + [weight, scaled, factor]]
        + [pltpu.SemaphoreType.DMA((6,)), pltpu.SemaphoreType.DMA((5,))],
        name="finish",
    )(*arrays, factor)


def shards(
    query_rows, key_rows, value_rows, out_grad, log_norm, delta_rows, window_len,
    activations, value_weight, row_state, col_state, *, n, n_head,
):
    tok_len = query_rows.shape[0]
    kv_local = key_rows.shape[1] // HD
    group = query_rows.shape[1] // key_rows.shape[1]
    rows, width = value_weight.shape
    pn = Plan(n, n_head, tok_len, kv_local, group, width, rows)

    act = activations if pn.inside else activations.T.reshape(n, rows, tok_len)
    query_grad, key_grad, value_grad, scaled, factor = fused(
        pn, window_len, query_rows, out_grad, key_rows, value_rows, log_norm.T, delta_rows.T, act,
        value_weight, row_state, col_state,
    )
    return finish(query_grad, key_grad, value_grad, value_weight, scaled, factor)


def solution(mesh):
    both = P("tok", "head")
    return jax.shard_map(
        functools.partial(shards, n=mesh.shape["tok"], n_head=mesh.shape["head"]),
        mesh=mesh,
        in_specs=(
            both, both, both, both, both, both, P("head"), P("tok", None),
            both, P("head", "tok"), both,
        ),
        out_specs=(both,) * 5,
        check_vma=False,
    )
```

```python
import functools
import math

import jax
import jax.numpy as jnp
from jax import lax
from jax.experimental import pallas as pl
from jax.experimental.pallas import tpu as pltpu
from jax.sharding import PartitionSpec as P

HD = 128
WINDOW = 1024
WINDOW_MIN = 896
SUB = 128
QUERY_SCALE = 1.0 / 12.0
LOG2E = math.log2(math.e)
DECAY_RATE = 0.9
LEARN_RATE = 0.05
F32 = jnp.float32
BF16 = jnp.bfloat16
MESH = pl.DeviceIdType.MESH


def xor(index, j):
    k = 0
    while (1 << k) <= j:
        if (j >> k) & 1:
            index = index + (1 << k) * (1 - 2 * lax.rem(index // (1 << k), 2))
        k += 1
    return index


class Plan:
    def __init__(self, n, n_head, tok_len, kv_local, group, width, rows):
        self.n, self.n_head, self.tok_len = n, n_head, tok_len
        self.kv_local, self.group = kv_local, group
        self.width, self.rows = width, rows
        self.gather = 4 if n % 4 == 0 else 1
        self.upper = n // self.gather
        self.split = self.gather if kv_local % self.gather == 0 else 1
        self.kv = kv_local // self.split
        self.tokens = self.split * tok_len
        self.blocks = n // self.split
        self.reach = min(-(-WINDOW // self.tokens), self.blocks - 1)
        self.subs = tok_len // SUB
        self.streams = self.split
        self.part = width // self.streams
        self.bits = int(math.log2(self.upper))
        self.share = 2 if n_head % 2 == 0 and self.upper % 2 == 0 else 1
        self.half = self.upper // self.share
        self.wide = self.half * self.gather * rows
        self.inside = rows % 16 == 0 and self.wide % SUB == 0
        first = rows * 5 // 7 // 16 * 16
        cut = self.inside and self.split == self.gather and first
        self.parts = [(0, first), (first, rows - first)] if cut else [(0, rows)]
        self.flat = n * n_head <= 64
        length = self.tokens if self.split == self.gather else tok_len
        first, middle = self.tokens - WINDOW, length // 2
        self.ahead = self.split == self.gather and 0 < first < middle and first % 16 == 0
        if self.ahead:
            self.pieces = [(0, first), (first, middle - first), (middle, length - middle)]
        else:
            self.pieces = [(0, middle), (middle, length - middle)]
        self.tail = len(self.pieces) - 1

    def halo_count(self, o):
        return min(self.tokens, WINDOW - (o - 1) * self.tokens)

    def halo_first(self, o):
        return max(0, WINDOW - o * self.tokens)


class Link:
    def __init__(self, ledger, key, src, dst, sems, at, device, send_if=None, recv_if=None):
        self.ledger, self.key = ledger, key
        self.send_if, self.recv_if = send_if, recv_if
        self.copy = pltpu.make_async_remote_copy(
            src_ref=src, dst_ref=dst, send_sem=sems[0].at[at], recv_sem=sems[1].at[at],
            device_id=device, device_id_type=MESH,
        )

    def guarded(self, condition, action):
        if condition is None:
            action()
        else:
            pl.when(condition)(action)

    def start(self):
        self.guarded(self.send_if, self.copy.start)
        self.ledger[self.key + ("send",)] = lambda: self.guarded(self.send_if, self.copy.wait_send)
        self.ledger[self.key + ("recv",)] = lambda: self.guarded(self.recv_if, self.copy.wait_recv)

    def wait_recv(self):
        self.ledger.pop(self.key + ("recv",))
        self.guarded(self.recv_if, self.copy.wait_recv)


def fused_kernel(
    pn,
    lim_in, q_ref, g_ref, k_ref, v_ref, ln_in, de_in, at_ref, w_ref, rs_in, cs_in,
    dq_ref, dk_ref, dv_ref, sc_out, fac_out,
    lim_ref, ln_ref, de_ref, rs_ref, cs_ref, sc_ref, fac_ref, st, wv, abuf, turned, qb, gb, kb, vb, stb, dva, dka, dqb, dkb, hsv, hsk, hrv, hrk, act, vga, acc, sbuf, rbuf,
    xs, xr,
    own_sem, small_sem, in_s, in_r, halo_s, halo_r, back_s, back_r, act_own, act_s, act_r, fwd_s, fwd_r,
    vg_s, vg_r, dq_s, dq_r, dk_s, dk_r, out_sem, rs_s, rs_r, x_s, x_r,
):
    n, n_head, gather, upper = pn.n, pn.n_head, pn.gather, pn.upper
    split, kv, length, tokens = pn.split, pn.kv, pn.tok_len, pn.tokens
    group, subs = pn.group, pn.subs
    me, hd = lax.axis_index("tok"), lax.axis_index("head")
    c, u = lax.rem(me, gather), me // gather
    place, block = lax.rem(me, split), me // split
    kw, qw = kv * HD, kv * group * HD
    rows = pn.rows
    ledger = {}

    def at_plane(j):
        return {"tok": me - c + xor(c, j)}

    near = [(j, h) for j in range(gather) for h in range(n_head) if j or h]
    far = list(range(1, upper))
    near_ids = [{"tok": me - c + xor(c, j), "head": xor(hd, h)} for j, h in near]
    far_ids = [{"tok": xor(u, i) * gather + c} for i in far]
    barrier = pltpu.get_barrier_semaphore()
    for partner in near_ids + far_ids:
        pl.semaphore_signal(barrier, inc=1, device_id=partner, device_id_type=MESH)
    lone = []
    if split == 1:
        for o in range(1, pn.reach + 1):
            lone.append(o)
            @pl.when(block + o < pn.blocks)
            def _(o=o):
                pl.semaphore_signal(barrier, inc=1, device_id={"tok": me + o}, device_id_type=MESH)

            @pl.when(block >= o)
            def _(o=o):
                pl.semaphore_signal(barrier, inc=1, device_id={"tok": me - o}, device_id_type=MESH)

    def cols(index, size):
        return pl.ds(pl.multiple_of(index * size, 128), size)

    own = [
        pltpu.make_async_copy(k_ref.at[:, cols(place, kw)], kb.at[pl.ds(WINDOW + place * length, length)], own_sem.at[0]),
        pltpu.make_async_copy(v_ref.at[:, cols(place, kw)], vb.at[pl.ds(WINDOW + place * length, length)], own_sem.at[1]),
        pltpu.make_async_copy(q_ref.at[:, cols(place, qw)], qb.at[pl.ds(place * length, length)], own_sem.at[2]),
        pltpu.make_async_copy(g_ref.at[:, cols(place, qw)], gb.at[pl.ds(place * length, length)], own_sem.at[3]),
        pltpu.make_async_copy(st.at[pl.ds(place * kv, kv)], stb.at[place], own_sem.at[4]),
    ]
    half = pn.half
    low = lax.rem(hd, pn.share) * half
    if pn.inside:
        load = pltpu.make_async_copy(
            at_ref.at[:, cols(lax.rem(hd, pn.share), pn.wide)], abuf, own_sem.at[5]
        )
        load.start()
    for copy in own[:4]:
        copy.start()
    small = [
        pltpu.make_async_copy(src, dst, small_sem.at[i])
        for i, (src, dst) in enumerate(
            [(ln_in, ln_ref), (de_in, de_ref), (lim_in, lim_ref), (rs_in, rs_ref), (cs_in, cs_ref)])
    ]
    for copy in small:
        copy.start()
    weight_in = pltpu.make_async_copy(w_ref, wv, own_sem.at[6])
    weight_in.start()

    pl.semaphore_wait(barrier, len(near_ids) + len(far_ids))
    for o in lone:
        @pl.when(block + o < pn.blocks)
        def _():
            pl.semaphore_wait(barrier, 1)

        @pl.when(block >= o)
        def _():
            pl.semaphore_wait(barrier, 1)

    def exchange(a, j):
        other = xor(place, j)
        src, dst = [
            (k_ref.at[:, cols(other, kw)], kb.at[pl.ds(WINDOW + place * length, length)]),
            (v_ref.at[:, cols(other, kw)], vb.at[pl.ds(WINDOW + place * length, length)]),
            (q_ref.at[:, cols(other, qw)], qb.at[pl.ds(place * length, length)]),
            (g_ref.at[:, cols(other, qw)], gb.at[pl.ds(place * length, length)]),
            (st.at[pl.ds(other * kv, kv)], stb.at[place]),
        ][a]
        return Link(ledger, ("in", a, j), src, dst, (in_s, in_r), (a, j), at_plane(j))

    for a in (0, 1, 2, 3):
        for j in range(1, split):
            exchange(a, j).start()
    for copy in small:
        copy.wait()
    for i, ref in enumerate((ln_ref, de_ref)):
        stat = ref[...]
        if i == 0:
            stat = stat * LOG2E
        for k in range(pn.kv_local):
            st[k, i * group : (i + 1) * group] = stat[k * group : (k + 1) * group]
    own[4].start()
    for j in range(1, split):
        exchange(4, j).start()
    dva[...] = jnp.zeros_like(dva)
    dka[...] = jnp.zeros_like(dka)

    def turn(first, last):
        @pl.loop(first, last)
        def _(i):
            here = pl.ds(pl.multiple_of(i * SUB, SUB), SUB)
            turned[here, :] = abuf[:, here].T

    steps = pn.wide // SUB
    if pn.inside:
        load.wait()

    def halo(a, o):
        count, first = pn.halo_count(o), pn.halo_first(o)
        buf = (kb, vb)[a]
        return Link(
            ledger, ("halo", a, o), buf.at[pl.ds(WINDOW + tokens - count, count)],
            buf.at[pl.ds(first, count)], (halo_s, halo_r), (a, o - 1), {"tok": me + o * split},
            block + o < pn.blocks, block >= o,
        )

    for a in (0, 1):
        own[a].wait()
        for j in range(1, split):
            exchange(a, j).wait_recv()
        for o in range(1, pn.reach + 1):
            halo(a, o).start()

            @pl.when(block < o)
            def _(a=a, o=o):
                buf = (kb, vb)[a]
                here = pl.ds(pn.halo_first(o), pn.halo_count(o))
                buf[here] = jnp.zeros((pn.halo_count(o), kw), BF16)
    if pn.reach * tokens < WINDOW:
        rest = WINDOW - pn.reach * tokens
        for buf in (kb, vb):
            buf[pl.ds(0, rest)] = jnp.zeros((rest, kw), BF16)

    if pn.inside:
        turn(0, steps)

    parts = pn.parts

    def act_piece(i, owner, r):
        first, size = parts[r]
        if pn.inside:
            here = pl.multiple_of((i * gather + owner) * rows + first, 16)
            return turned.at[pl.ds(here, size)]
        return at_ref.at[(low + i) * gather + owner]

    act_mine = [
        pltpu.make_async_copy(
            act_piece(i, c, r), act.at[low + i, pl.ds(*parts[r]), cols(c, length)], act_own.at[i, r])
        for i in range(half) for r in range(len(parts))
    ]
    for copy in act_mine:
        copy.start()

    def act_send(j, i, r):
        return Link(
            ledger, ("act", j, i, r), act_piece(i, xor(c, j), r),
            act.at[low + i, pl.ds(*parts[r]), cols(c, length)],
            (act_s, act_r), (j, i, r), at_plane(j),
        )

    def act_forward(j, i, r, start=low):
        piece = act.at[start + i, pl.ds(*parts[r]), cols(xor(c, j), length)]
        return Link(
            ledger, ("forward", j, i, r), piece, piece, (fwd_s, fwd_r), (j, i, r),
            {"head": xor(hd, 1)})

    order = [(j, i) for i in range(half) for j in (1, 2, 3)]
    if gather == 1:
        order = []

    def act_out(r):
        for j, i in order:
            act_send(j, i, r).start()

    def act_pass(r):
        for j, i in order:
            act_send(j, i, r).wait_recv()
            if pn.share == 2:
                act_forward(j, i, r).start()

    def act_ready(r):
        if pn.share == 2:
            for j, i in [(0, i) for i in range(half)] + order:
                act_forward(j, i, r, half - low).wait_recv()

    act_out(0)
    for a in (0, 1):
        for o in range(1, pn.reach + 1):
            halo(a, o).wait_recv()

    seen = WINDOW + SUB
    chunk = seen // 3
    lanes = group * SUB

    def unit(b, kh, sub):
        start = pl.multiple_of(b * length + sub * SUB, SUB)
        rows_q = pl.ds(start, SUB)
        head = kh * group * HD
        query = jnp.concatenate(
            [qb[rows_q, head + m * HD : head + (m + 1) * HD] for m in range(group)], axis=0
        )
        grad = jnp.concatenate(
            [gb[rows_q, head + m * HD : head + (m + 1) * HD] for m in range(group)], axis=0
        )
        lane_q = pl.ds(pl.multiple_of(sub * SUB, SUB), SUB)
        norm, delta = [
            jnp.concatenate([stb[b, kh, i * group + m : i * group + m + 1, lane_q] for m in range(group)], axis=1)
            for i in range(2)
        ]
        total = jnp.zeros((lanes, HD), F32)
        for piece in range(3):
            here = pl.ds(pl.multiple_of(start + piece * chunk, SUB), chunk)
            keys = kb[here, kh * HD : (kh + 1) * HD]
            values = vb[here, kh * HD : (kh + 1) * HD]
            scores = lax.dot_general(
                keys, query, (((1,), (1,)), ((), ())), preferred_element_type=F32
            )
            prob = jnp.exp2(scores * (QUERY_SCALE * LOG2E) - norm)
            if piece == 0:
                edge = WINDOW - WINDOW_MIN + SUB
                row = lax.broadcasted_iota(jnp.int32, (edge, lanes), 0)
                lane = lax.broadcasted_iota(jnp.int32, (edge, lanes), 1)
                limit = jnp.full((edge, lanes), 0, jnp.int32)
                for m in range(group):
                    limit = jnp.where(
                        lane // SUB == m, lim_ref[(place * kv + kh) * group + m], limit
                    )
                visible = WINDOW + lax.rem(lane, SUB) - row < limit
                prob = jnp.concatenate(
                    [jnp.where(visible, prob[:edge], 0.0), prob[edge:]], axis=0
                )
            if piece == 2:
                row = lax.broadcasted_iota(jnp.int32, (SUB, lanes), 0)
                lane = lax.broadcasted_iota(jnp.int32, (SUB, lanes), 1)
                visible = row <= lax.rem(lane, SUB)
                prob = jnp.concatenate(
                    [prob[: chunk - SUB], jnp.where(visible, prob[chunk - SUB :], 0.0)], axis=0
                )
            dva[here, kh * HD : (kh + 1) * HD] += jnp.dot(
                prob.astype(BF16), grad, preferred_element_type=F32
            )
            dprob = lax.dot_general(
                values, grad, (((1,), (1,)), ((), ())), preferred_element_type=F32
            )
            dscore = (QUERY_SCALE * prob * (dprob - delta)).astype(BF16)
            dka[here, kh * HD : (kh + 1) * HD] += jnp.dot(
                dscore, query, preferred_element_type=F32
            )
            total = total + lax.dot_general(
                dscore, keys, (((0,), (0,)), ((), ())), preferred_element_type=F32
            )
        low_q = total.astype(BF16)
        for m in range(group):
            dqb[rows_q, head + m * HD : head + (m + 1) * HD] = low_q[m * SUB : (m + 1) * SUB]

    def dq_send(j):
        other = xor(place, j)
        src = dqb.at[pl.ds(other * length, length)]
        return Link(
            ledger, ("dq", j), src, dq_ref.at[:, cols(place, qw)], (dq_s, dq_r), (j,), at_plane(j))

    def local_out(src, dst, i):
        return pltpu.make_async_copy(src, dst, out_sem.at[i])

    for j in range(split):
        b = xor(place, j)
        for a in (2, 3, 4):
            if j:
                exchange(a, j).wait_recv()
            else:
                own[a].wait()
        for kh in range(kv):
            @pl.loop(0, subs)
            def _(sub, b=b, kh=kh):
                unit(b, kh, sub)

        if j == 0:
            for copy in act_mine:
                copy.wait()
            if pn.share == 2:
                for r in range(len(parts)):
                    for i in range(half):
                        act_forward(0, i, r).start()

    def back(a, o):
        count, first = pn.halo_count(o), pn.halo_first(o)
        return Link(
            ledger, ("back", a, o), (hsv, hsk)[a].at[pl.ds(first, count)],
            (hrv, hrk)[a].at[o - 1, pl.ds(0, count)], (back_s, back_r), (a, o - 1),
            {"tok": me - o * split}, block >= o, block + o < pn.blocks,
        )

    tail = pn.tail

    def vg_copy(j, owner, h):
        piece = vga.at[owner, pl.ds(*pn.pieces[h])]
        return Link(
            ledger, ("vg", j, h), piece, piece, (vg_s, vg_r), (j, h),
            at_plane(j if j < 3 else (1 if h == tail else 2)),
        )

    def vg_send(j, h):
        return vg_copy(j, c if j < 3 else xor(c, 2 if h == tail else 1), h)

    def vg_wait(j, h):
        vg_copy(j, xor(c, j), h).wait_recv()

    for a in (0, 1):
        (hsv, hsk)[a][...] = (dva, dka)[a][pl.ds(0, WINDOW)].astype(BF16)
        for o in range(1, pn.reach + 1):
            back(a, o).start()
        if a == 0 and pn.ahead:
            first = pn.pieces[0][1]
            vga[c, pl.ds(0, first)] = dva[pl.ds(WINDOW, first)].astype(BF16)
            for j in (1, 2):
                vg_send(j, 0).start()

    def add_back(a):
        for o in range(1, pn.reach + 1):
            back(a, o).wait_recv()

            @pl.when(block + o < pn.blocks)
            def _(o=o):
                count = pn.halo_count(o)
                here = pl.ds(WINDOW + tokens - count, count)
                total = (dva, dka)[a]
                total[here] = total[here] + (hrv, hrk)[a][o - 1, pl.ds(0, count)].astype(F32)

    act_pass(0)
    add_back(0)
    ready = pn.pieces[0][1] if pn.ahead else 0
    vga[c, pl.ds(ready, tokens - ready)] = dva[pl.ds(WINDOW + ready, tokens - ready)].astype(BF16)
    rest = list(range(1 if pn.ahead else 0, len(pn.pieces)))
    if gather > 1:
        for h, g in zip(rest, rest[::-1]):
            vg_send(1, h).start()
            vg_send(2, g).start()
    act_ready(0)
    bits, part = pn.bits, pn.part
    counts = [upper >> (p + 1) for p in range(bits)]
    starts = [sum(counts[:p]) for p in range(bits)]
    partners = [{"tok": xor(u, 1 << p) * gather + c} for p in range(bits)]

    def bit_of(index, k):
        return lax.rem(index // (1 << k), 2)

    def block_at(phase, j, other):
        index = 0
        for k in range(phase):
            index = index + (1 << k) * bit_of(u, k)
        mine = bit_of(u, phase)
        index = index + (1 << phase) * ((1 - mine) if other else mine)
        return index + (1 << (phase + 1)) * j

    def copy_of(s, p, r):
        here, there = pl.ds(starts[p], counts[p]), pl.ds(*parts[r])
        return Link(
            ledger, ("sum", s, p, r), sbuf.at[s, here, there], rbuf.at[s, here, there],
            (rs_s, rs_r), (s, p, r), partners[p],
        )

    def product(s, index, r):
        left = act[index, pl.ds(*parts[r]), :]
        if split == gather:
            return jnp.dot(left, vga[xor(c, s)], preferred_element_type=F32)
        whole = vga[...].reshape(gather * length, part)
        return jnp.dot(left, whole, preferred_element_type=F32)

    def products(s, r):
        there = pl.ds(*parts[r])

        @pl.loop(0, counts[0])
        def _(j):
            sbuf[s, j, there] = product(s, block_at(0, j, True), r).astype(BF16)

        copy_of(s, 0, r).start()

        @pl.loop(0, counts[0])
        def _(j):
            index = block_at(0, j, False)
            acc[s, index, there] = product(s, index, r)

    def arrived(s, p, r):
        there = pl.ds(*parts[r])
        copy_of(s, p, r).wait_recv()

        @pl.loop(0, counts[p])
        def _(j):
            index = block_at(p, j, False)
            acc[s, index, there] = acc[s, index, there] + rbuf[s, starts[p] + j, there].astype(F32)

        if p + 1 < bits:
            @pl.loop(0, counts[p + 1])
            def _(j):
                index = block_at(p + 1, j, True)
                sbuf[s, starts[p + 1] + j, there] = acc[s, index, there].astype(BF16)

            copy_of(s, p + 1, r).start()

    def pass_on():
        for h in range(tail - 1):
            vg_wait(1, h)
            vg_send(3, h).start()
        vg_wait(2, tail)
        vg_send(3, tail).start()
        vg_wait(1, tail - 1)
        vg_send(3, tail - 1).start()

    def vg_rest(j):
        for h in range(tail + 1):
            if j == 3 or (j == 1 and h == tail) or (j == 2 and h != tail):
                vg_wait(j, h)

    last = len(parts) - 1
    if split == 1 and gather > 1:
        pass_on()
        for j in (1, 2, 3):
            vg_rest(j)
    products(0, 0)
    weight_in.wait()
    weight_f = wv[...].astype(F32)
    weight_sum = jnp.sum(weight_f * weight_f)
    if split > 1:
        pass_on()
        if last:
            act_out(1)
            arrived(0, 0, 0)
        for s in (1, 2):
            vg_rest(s)
            products(s, 0)

    outs = []
    outs.append(local_out(dqb.at[pl.ds(place * length, length)], dq_ref.at[:, cols(place, qw)], 0))
    outs[-1].start()

    add_back(1)
    dkb[...] = dka[pl.ds(WINDOW, tokens)].astype(BF16)

    def dk_send(j):
        other = xor(place, j)
        return Link(
            ledger, ("dk", j), dkb.at[pl.ds(other * length, length)], dk_ref.at[:, cols(place, kw)],
            (dk_s, dk_r), (j,), at_plane(j),
        )

    outs.append(local_out(dkb.at[pl.ds(place * length, length)], dk_ref.at[:, cols(place, kw)], 1))
    outs[-1].start()
    if last:
        vg_rest(3)
        products(3, 0)
        arrived(1, 0, 0)
        arrived(2, 0, 0)
        act_pass(1)
        act_ready(1)
        for s in range(4):
            if s < 3:
                dq_send(3 - s).start()
                dk_send(3 - s).start()
            products(s, 1)
    elif split > 1:
        vg_rest(3)
        products(3, 0)
    if not last:
        for j in range(1, split):
            dq_send(j).start()
            dk_send(j).start()
    if split == gather:
        for j in range(gather):
            src = xor(c, j)
            outs.append(local_out(
                vga.at[src, pl.ds(c * length, length)], dv_ref.at[:, cols(src, kw)], 2 + j))
            outs[-1].start()
    else:
        outs.append(local_out(vga.at[c], dv_ref, 2))
        outs[-1].start()


    early, late = list(range(min(3, pn.streams))), list(range(3, pn.streams))
    steps = [(s, 0, last) for s in early]
    if last:
        steps += [(s, 1, 0) for s in early] if bits > 1 else []
    steps = ([(s, 0, 0) for s in late] if last else []) + steps + [(s, 0, last) for s in late]
    for p in range(1, bits):
        steps += [(s, p, r) for r in range(len(parts)) for s in early if p > 1 or r == last]
        steps += [(s, p, r) for r in range(len(parts)) for s in late]
    for s, p, r in steps:
        arrived(s, p, r)

    row_sum = jnp.zeros((rows, 1), F32)
    for s in range(pn.streams):
        wg = acc[s, u]
        row_sum = row_sum + jnp.sum(wg * wg, axis=1, keepdims=True)
    diag = lax.broadcasted_iota(jnp.int32, (rows, rows), 0) == lax.broadcasted_iota(
        jnp.int32, (rows, rows), 1)
    row_old = jnp.sum(jnp.where(diag, rs_ref[...], 0.0), axis=1, keepdims=True)
    row_mix = DECAY_RATE * row_old + (1.0 - DECAY_RATE) * (row_sum / pn.width)
    row_mean = jnp.sum(row_mix) / rows
    scaled_sum = jnp.float32(0.0)
    for s in range(pn.streams):
        wg = acc[s, u]
        here = cols(xor(c, s), part) if split == gather else slice(0, part)
        col_new = jnp.sum(wg * wg, axis=0, keepdims=True) / rows
        col_mix = DECAY_RATE * cs_ref[:, here] + (1.0 - DECAY_RATE) * col_new
        scaled = wg / jnp.sqrt(row_mix * col_mix / row_mean)
        sc_ref[:, here] = scaled
        scaled_sum = scaled_sum + jnp.sum(scaled * scaled)

    outs.append(local_out(sc_ref, sc_out, 2 + gather))
    outs[-1].start()
    row = lax.broadcasted_iota(jnp.int32, (8, 128), 0)
    xs[0] = jnp.where(row < 1, scaled_sum, weight_sum)

    if pn.flat:
        levels = [[
            {"tok": xor(u, i) * gather + xor(c, j), "head": xor(hd, h)}
            for i in range(upper) for j in range(gather) for h in range(n_head) if i or j or h
        ]]
    else:
        levels = [near_ids, far_ids]

    def share(level, i, partner):
        slot = i + (len(near) if level else 0)
        return Link(ledger, ("share", slot), xs.at[level, pl.ds(0, 2)], xr.at[slot, pl.ds(0, 2)], (x_s, x_r), (slot,), partner)

    for level, ids in enumerate(levels):
        for i, partner in enumerate(ids):
            share(level, i, partner).start()
        total = xs[level, pl.ds(0, 2)]
        for i, partner in enumerate(ids):
            share(level, i, partner).wait_recv()
            total = total + xr[i + (len(near) if level else 0), pl.ds(0, 2)]
        xs[level + 1, pl.ds(0, 2)] = total
    sums = xs[len(levels)]
    size = float(rows * n * pn.width * n_head)
    rms_scaled = jnp.sqrt(sums[0:1] / size)
    rms_weight = jnp.sqrt(sums[1:2] / size)
    fac_ref[...] = jnp.broadcast_to(rms_weight / jnp.maximum(1.0, rms_scaled), fac_ref.shape)

    outs.append(local_out(fac_ref, fac_out, 3 + gather))
    outs[-1].start()
    for copy in outs:
        copy.wait()
    for wait in ledger.values():
        wait()


def fused(pn, limits, query, grad, keys, values, norm, delta, act, weight, row_state, col_state):
    kw, qw = pn.kv * HD, pn.kv * pn.group * HD
    whole = WINDOW + pn.tokens
    hbm = pl.BlockSpec(memory_space=pl.ANY)
    dma = pltpu.SemaphoreType.DMA
    half, cuts = pn.half, len(pn.parts)
    peers = pn.n * pn.n_head - 1 if pn.flat else pn.gather * pn.n_head - 1 + pn.upper - 1
    reach, gather, split = pn.reach, pn.gather, pn.split
    piece = (pn.tokens, kw) if split == gather else (pn.tok_len, kw)
    return pl.pallas_call(
        functools.partial(fused_kernel, pn),
        out_shape=[
            jax.ShapeDtypeStruct(query.shape, BF16),
            jax.ShapeDtypeStruct(keys.shape, BF16),
            jax.ShapeDtypeStruct(keys.shape, BF16),
            jax.ShapeDtypeStruct((pn.rows, pn.width), F32),
            jax.ShapeDtypeStruct((8, 128), F32),
        ],
        in_specs=[hbm] * 11,
        out_specs=[hbm] * 5,
        scratch_shapes=[
            pltpu.SMEM(limits.shape, jnp.int32),
            pltpu.VMEM(norm.shape, F32),
            pltpu.VMEM(delta.shape, F32),
            pltpu.VMEM(row_state.shape, F32),
            pltpu.VMEM(col_state.shape, F32),
            pltpu.VMEM((pn.rows, pn.width), F32),
            pltpu.VMEM((8, 128), F32),
            pltpu.VMEM((pn.kv_local, 2 * pn.group, pn.tok_len), F32),
            pltpu.VMEM((pn.rows, pn.width), BF16),
            pltpu.VMEM((pn.tok_len, pn.wide) if pn.inside else act.shape[1:], BF16),
            pltpu.VMEM((pn.wide, pn.tok_len) if pn.inside else (16, 128), BF16),
            pltpu.VMEM((pn.tokens, qw), BF16),
            pltpu.VMEM((pn.tokens, qw), BF16),
            pltpu.VMEM((whole, kw), BF16),
            pltpu.VMEM((whole, kw), BF16),
            pltpu.VMEM((split, pn.kv, 2 * pn.group, pn.tok_len), F32),
            pltpu.VMEM((whole, kw), F32),
            pltpu.VMEM((whole, kw), F32),
            pltpu.VMEM((pn.tokens, qw), BF16),
            pltpu.VMEM((pn.tokens, kw), BF16),
            pltpu.VMEM((WINDOW, kw), BF16),
            pltpu.VMEM((WINDOW, kw), BF16),
            pltpu.VMEM((reach, min(pn.tokens, WINDOW), kw), BF16),
            pltpu.VMEM((reach, min(pn.tokens, WINDOW), kw), BF16),
            pltpu.VMEM((pn.upper, pn.rows, gather * pn.tok_len), BF16),
            pltpu.VMEM((gather,) + piece, BF16),
            pltpu.VMEM((pn.streams, pn.upper, pn.rows, pn.part), F32),
            pltpu.VMEM((pn.streams, pn.upper - 1, pn.rows, pn.part), BF16),
            pltpu.VMEM((pn.streams, pn.upper - 1, pn.rows, pn.part), BF16),
            pltpu.VMEM((3, 8, 128), F32),
            pltpu.VMEM((peers, 8, 128), F32),
            dma((7,)), dma((5,)), dma((5, split)), dma((5, split)), dma((2, reach)), dma((2, reach)),
            dma((2, reach)), dma((2, reach)), dma((half, cuts)),
            dma((gather, half, cuts)), dma((gather, half, cuts)),
            dma((gather, half, cuts)), dma((gather, half, cuts)),
            dma((gather, len(pn.pieces))), dma((gather, len(pn.pieces))), dma((split,)), dma((split,)),
            dma((split,)), dma((split,)), dma((4 + gather,)),
            dma((pn.streams, pn.bits, cuts)), dma((pn.streams, pn.bits, cuts)), dma((peers,)), dma((peers,)),
        ],
        compiler_params=pltpu.CompilerParams(
            collective_id=0, has_side_effects=True, vmem_limit_bytes=56 * 1024 * 1024
        ),
        name="fused",
    )(limits, query, grad, keys, values, norm, delta, act, weight, row_state, col_state)


def finish_kernel(
    dq_in, dk_in, dv_in, w_in, sc_in, fac_in, dq, dk, dv, new, upd,
    dq_v, dk_v, dv_v, w_v, sc_v, new_v, upd_v, fac_ref, in_sem, out_sem,
):
    pairs = [(dq_in, dq_v, dq), (dk_in, dk_v, dk), (dv_in, dv_v, dv)]
    loads = [pltpu.make_async_copy(fac_in, fac_ref, in_sem.at[5]), pltpu.make_async_copy(sc_in, sc_v, in_sem.at[3]), pltpu.make_async_copy(w_in, w_v, in_sem.at[4])]
    ins = [pltpu.make_async_copy(a, b, in_sem.at[i]) for i, (a, b, _) in enumerate(pairs)]
    outs = [pltpu.make_async_copy(b, d, out_sem.at[i]) for i, (_, b, d) in enumerate(pairs)]
    outs += [pltpu.make_async_copy(new_v, new, out_sem.at[3]), pltpu.make_async_copy(upd_v, upd, out_sem.at[4])]
    for copy in ins + loads:
        copy.start()
    for i in range(3):
        ins[i].wait()
        outs[i].start()
    for copy in loads:
        copy.wait()
    update = sc_v[...] * fac_ref[0:1, 0:1]
    upd_v[...] = update
    outs[4].start()
    new_v[...] = (w_v[...].astype(F32) - LEARN_RATE * update).astype(BF16)
    outs[3].start()
    for copy in outs:
        copy.wait()


def finish(dq, dk, dv, weight, scaled, factor):
    hbm = pl.BlockSpec(memory_space=pl.ANY)
    arrays = [dq, dk, dv, weight, scaled]
    outs = [dq, dk, dv, weight, scaled]
    return pl.pallas_call(
        finish_kernel,
        out_shape=[jax.ShapeDtypeStruct(x.shape, x.dtype) for x in outs],
        in_specs=[hbm] * 6,
        out_specs=[hbm] * 5,
        scratch_shapes=[pltpu.VMEM(x.shape, x.dtype) for x in arrays + [weight, scaled, factor]]
        + [pltpu.SemaphoreType.DMA((6,)), pltpu.SemaphoreType.DMA((5,))],
        name="finish",
    )(*arrays, factor)


def shards(
    query_rows, key_rows, value_rows, out_grad, log_norm, delta_rows, window_len,
    activations, value_weight, row_state, col_state, *, n, n_head,
):
    tok_len = query_rows.shape[0]
    kv_local = key_rows.shape[1] // HD
    group = query_rows.shape[1] // key_rows.shape[1]
    rows, width = value_weight.shape
    pn = Plan(n, n_head, tok_len, kv_local, group, width, rows)

    act = activations if pn.inside else activations.T.reshape(n, rows, tok_len)
    query_grad, key_grad, value_grad, scaled, factor = fused(
        pn, window_len, query_rows, out_grad, key_rows, value_rows, log_norm.T, delta_rows.T, act,
        value_weight, row_state, col_state,
    )
    return finish(query_grad, key_grad, value_grad, value_weight, scaled, factor)


def solution(mesh):
    both = P("tok", "head")
    return jax.shard_map(
        functools.partial(shards, n=mesh.shape["tok"], n_head=mesh.shape["head"]),
        mesh=mesh,
        in_specs=(
            both, both, both, both, both, both, P("head"), P("tok", None),
            both, P("head", "tok"), both,
        ),
        out_specs=(both,) * 5,
        check_vma=False,
    )
```
